32 devices in a mesh: slab: 16 (over z, y, x), pencil: 2 (over core).
Axes of the slice: x: 2, y: 2, z: 4, core: 2. Of those that a mesh axis runs over, the one named last changes fastest.
Arguments:
- owner_map: int32 [16], replicated, may hold values from 0 to 15
- window_start: int32 [1], replicated, may hold values from 0 to 8
- child_maps: float32 [8, 20, 20], replicated, may hold values from -1 to 1
- innovation: float32 [20, 20], replicated, may hold values from -1.25 to 1.25
- coarse_bank: float32 [16, 20, 74898], P('slab'), may hold values from -6 to 6
- noise_middle: float32 [20, 64, 64, 128], P(None, 'slab', 'pencil'), may hold values from -6 to 6
- noise_finest: float32 [20, 128, 128, 256], P(None, 'slab', 'pencil'), may hold values from -6 to 6
Outputs:
- field_values: float32 [256, 256, 512], P('slab', 'pencil')
- zface_mean: float32 [128, 256, 512], P('slab', 'pencil')
- yface_mean: float32 [256, 128, 512], P('slab', 'pencil')
The draws below stay inside these ranges and needn't reach their ends.
All inputs are finite; a program needn't handle non-finite values.
Results may differ from the reference program's by a relative error of at most 0.0001.
Values sent between devices are 32-bit elements; how exact they have to be, the bound alone decides.
A program may use at most 448 MiB of HBM per device.

```python
import math
import jax
import jax.numpy as jnp
import numpy as np
from jax import lax

K = 20
LEVELS = 8
ROOTS = 2
ROOTS_Z = 1
ROOTS_Y = 1
DEPTH = 16
COARSE = 74898
FZ = 128
FY = 128
FX = 256
N_SLAB = 16


def touch_ends(result, rng, least, top_value):
    spot = [jax.random.randint(jax.random.fold_in(rng, axis), (), 0, length) for axis, length in enumerate(result.shape)]
    widest = result.shape.index(max(result.shape))
    beside = spot[:widest] + [(spot[widest] + 1) % result.shape[widest]] + spot[widest + 1:]
    return result.at[tuple(spot)].set(least).at[tuple(beside)].set(top_value)


def steps_of(rng, dims, split, least, largest):
    level = 1.0
    for dim, shards_of in split:
        heights = jax.random.uniform(jax.random.fold_in(jax.random.fold_in(rng, 6), dim), (shards_of,), jnp.float32, least / len(split), largest / len(split))
        level = level * jnp.repeat(jnp.exp(heights), dims[dim] // shards_of).reshape((-1,) + (1,) * (len(dims) - 1 - dim))
    return level


def bell_draw(rng, shape, width, bound, cuts=(), kind=jnp.bfloat16):
    entries = width * jax.random.normal(rng, shape, jnp.float32)
    if cuts:
        entries = entries * steps_of(rng, shape, cuts, -0.22, 0.18)
    return jnp.clip(entries, -bound, bound).astype(kind)


def setup_inputs(seed: int = 0) -> dict:
    seeds = jax.random.split(jax.random.key(seed), 8)
    owner_map = touch_ends(jax.random.randint(seeds[0], (DEPTH,), 0, N_SLAB), jax.random.fold_in(seeds[0], 1), 0, N_SLAB - 1).astype(jnp.int32)
    window_start = jax.random.randint(seeds[1], (1,), 0, DEPTH - LEVELS + 1).astype(jnp.int32)
    child_maps = bell_draw(seeds[2], (8, K, K), (2 * K) ** -0.5, 1.0, (), jnp.float32)
    innovation = bell_draw(seeds[3], (K, K), K ** -0.5, 1.25, (), jnp.float32)
    coarse_bank = bell_draw(seeds[4], (N_SLAB, K, COARSE), 1.0, 6.0, ((0, 16),), jnp.float32)
    noise_middle = bell_draw(seeds[5], (K, FZ // 2, FY // 2, FX // 2), 1.0, 6.0, ((1, 16), (2, 2)), jnp.float32)
    noise_finest = bell_draw(seeds[6], (K, FZ, FY, FX), 1.0, 6.0, ((1, 16), (2, 2)), jnp.float32)
    return {"owner_map": owner_map, "window_start": window_start, "child_maps": child_maps, "innovation": innovation, "coarse_bank": coarse_bank, "noise_middle": noise_middle, "noise_finest": noise_finest}


def legendre(order, point):
    values = [1.0, point, 1.5 * point * point - 0.5, 2.5 * point * point * point - 1.5 * point]
    return values[order]

def basis_table(points):
    table_rows = []
    for point in points:
        w_coord, v_coord, u_coord = point
        entry = []
        for deg_x in range(4):
            for deg_y in range(4):
                for deg_z in range(4):
                    if deg_x + deg_y + deg_z <= 3:
                        factor = math.sqrt((2 * deg_x + 1) * (2 * deg_y + 1) * (2 * deg_z + 1))
                        entry.append(factor * legendre(deg_x, u_coord) * legendre(deg_y, v_coord) * legendre(deg_z, w_coord))
        table_rows.append(entry)
    return jnp.asarray(np.array(table_rows), jnp.float32)

def level_block(flat, level):
    scale = 2 ** level
    first = ROOTS_Z * ROOTS_Y * ROOTS
    offset = first * (8 ** level - 1) // 7
    length = first * 8 ** level
    return flat[:, offset:offset + length].reshape(flat.shape[0], ROOTS_Z * scale, ROOTS_Y * scale, ROOTS * scale)

def descend(parent, child_maps):
    kids = jnp.einsum('okn,nzyx->okzyx', child_maps, parent, precision=lax.Precision.HIGHEST)
    count, planes, rows_y, cols_x = parent.shape
    kids = kids.reshape(2, 2, 2, count, planes, rows_y, cols_x).transpose(3, 4, 0, 5, 1, 6, 2)
    return kids.reshape(count, 2 * planes, 2 * rows_y, 2 * cols_x)

def innovate(innovation, noise):
    return jnp.einsum('kn,nzyx->kzyx', innovation, noise, precision=lax.Precision.HIGHEST)

def expand(table, coeffs):
    return jnp.einsum('pk,kzyx->pzyx', table, coeffs, precision=lax.Precision.HIGHEST)

def reference(owner_map, window_start, child_maps, innovation, coarse_bank, noise_middle, noise_finest):
    coeffs = None
    for level in range(LEVELS - 2):
        owner = owner_map[window_start[0] + level].astype(jnp.int32)
        chosen = lax.dynamic_index_in_dim(coarse_bank, owner, 0, keepdims=False)
        fresh = innovate(innovation, level_block(chosen, level))
        coeffs = fresh if level == 0 else descend(coeffs, child_maps) + fresh
    coeffs = descend(coeffs, child_maps) + innovate(innovation, noise_middle)
    fine = descend(coeffs, child_maps) + innovate(innovation, noise_finest)
    count, planes, rows_y, cols_x = fine.shape
    halves = [-0.5, 0.5]
    inner = basis_table([(pz, py, px) for pz in halves for py in halves for px in halves])
    top = basis_table([(1.0, py, px) for py in halves for px in halves])
    bottom = basis_table([(-1.0, py, px) for py in halves for px in halves])
    north = basis_table([(pz, 1.0, px) for pz in halves for px in halves])
    south = basis_table([(pz, -1.0, px) for pz in halves for px in halves])
    values = expand(inner, fine).reshape(2, 2, 2, planes, rows_y, cols_x).transpose(3, 0, 4, 1, 5, 2)
    field_values = values.reshape(2 * planes, 2 * rows_y, 2 * cols_x)
    zsum = expand(top, fine) + jnp.roll(expand(bottom, fine), -1, axis=1)
    zface = (0.5 * zsum).reshape(2, 2, planes, rows_y, cols_x).transpose(2, 3, 0, 4, 1)
    zface_mean = zface.reshape(planes, 2 * rows_y, 2 * cols_x)
    ysum = expand(north, fine) + jnp.roll(expand(south, fine), -1, axis=2)
    yface = (0.5 * ysum).reshape(2, 2, planes, rows_y, cols_x).transpose(2, 0, 3, 4, 1)
    yface_mean = yface.reshape(2 * planes, rows_y, 2 * cols_x)
    return (field_values, zface_mean, yface_mean)
```

```python
import functools
import math

import jax
import jax.numpy as jnp
import numpy as np
from jax import lax
from jax.experimental import pallas as pl
from jax.experimental.pallas import tpu as pltpu
from jax.sharding import PartitionSpec as P

LEVELS = 8
ROOTS = 2
BANKS = LEVELS - 2
LAST = BANKS - 1
LANES = 128
TILE = 8
F32 = jnp.float32
BF16 = jnp.bfloat16
MESH = pl.DeviceIdType.MESH


def legendre(order, point):
    values = [1.0, point, 1.5 * point * point - 0.5, 2.5 * point * point * point - 1.5 * point]
    return values[order]


def basis_row(point):
    w_coord, v_coord, u_coord = point
    entry = []
    for deg_x in range(4):
        for deg_y in range(4):
            for deg_z in range(4):
                if deg_x + deg_y + deg_z <= 3:
                    factor = math.sqrt((2 * deg_x + 1) * (2 * deg_y + 1) * (2 * deg_z + 1))
                    entry.append(
                        factor
                        * legendre(deg_x, u_coord)
                        * legendre(deg_y, v_coord)
                        * legendre(deg_z, w_coord)
                    )
    return np.array(entry)


def shifted(block, axis, distance):
    devices = range(lax.axis_size(axis))
    route = [((i - distance) % len(devices), i) for i in devices]
    return lax.ppermute(block, axis, route)


def offset_of(level):
    return ROOTS * (8**level - 1) // 7


def round_up(size, unit):
    return -(-size // unit) * unit


def log2(n):
    return n.bit_length() - 1


class Region:
    def __init__(self, level, n_slab, n_pencil):
        side = 2**level
        self.level = level
        self.side = side
        self.nx = ROOTS * side
        self.ny = side // n_pencil
        self.nz = max(1, side // n_slab)
        self.plane = side * self.nx
        self.part = self.ny * self.nx
        self.n_slab = n_slab

    def first_plane(self, slab):
        return (slab * self.side) // self.n_slab


def split2(value):
    high = value.astype(BF16)
    low = (value - high.astype(F32)).astype(BF16)
    return high, low


def split3(value):
    high, low = split2(value)
    rest = value - high.astype(F32) - low.astype(F32)
    return jnp.concatenate([high.astype(F32), low.astype(F32), rest], axis=0).astype(BF16)


def dot(left, right):
    return jnp.dot(left, right, preferred_element_type=F32)


def pieces_of(value):
    high, low = split2(value)
    return high, low, (value - high.astype(F32) - low.astype(F32)).astype(BF16)


def exact(left, right, terms=3):
    total = 0.0
    for i, a in reversed(list(enumerate(pieces_of(left)))):
        for j, b in reversed(list(enumerate(pieces_of(right)))):
            if i + j < terms:
                total = total + dot(a, b)
    return total


def chosen(pick, value):
    high, low, rest = pieces_of(value)
    return dot(pick, high) + (dot(pick, low) + dot(pick, rest))


def placed_at(value, place):
    high, low, rest = pieces_of(value)
    return dot(high, place) + (dot(low, place) + dot(rest, place))


def stacked(value):
    high, low = split2(value)
    return jnp.concatenate([high, low, high], axis=0)


def picked(parent, pick):
    rows = parent.shape[0]
    up = dot(split3(parent), pick)
    return up[:rows] + up[rows : 2 * rows] + up[2 * rows :]


def spread(up, octant, names):
    return [jnp.where(octant == o, up, 0.0) for o in names]


def iota(shape, dim):
    return lax.broadcasted_iota(jnp.int32, shape, dim)


def deepened(value, rows):
    return jnp.concatenate(
        [value, jnp.zeros((rows - value.shape[0], value.shape[1]), F32)], axis=0
    )


def weave(table_terms, mask, place, table, innovation, maps, octz):
    both = []
    for octy in range(2):
        o = 4 * octz + 2 * octy
        wide = placed_at(jnp.concatenate([innovation, maps[o], maps[o + 1]], axis=1), place[...])
        if table is not None:
            wide = exact(table, deepened(wide, LANES))
        both.append(deepened(wide, LANES // 2))
    both = jnp.concatenate(both, axis=0)
    total = 0.0
    for term in range(table_terms.shape[0]):
        total = total + chosen(table_terms[term], both) * mask[term].astype(F32)
    high, low = split2(total)
    return jnp.concatenate([high, high, low], axis=1)


def head_kernel(n_slab, n_pencil, info, head, end, flat, maps, innovation, table,
                fine_rows, fine_mask, fine_place, mid_rows, mid_mask, mid_place,
                partial, tail, fine_w, mid_w, chain_w):
    rows = head.shape[0]
    pencil = info[0]
    tail[...] = end[...]
    w_high, w_low = split2(flat[...])
    w_all = jnp.concatenate([w_high, w_high, w_low], axis=1)
    lane = iota((rows, LANES), 1)
    last = LAST - 1

    def unshifted(at, shift):
        if shift == 0:
            return head[:, pl.ds(at, LANES)]
        left = pltpu.roll(head[:, pl.ds(at, LANES)], LANES - shift, 1)
        right = pltpu.roll(head[:, pl.ds(at + LANES, LANES)], LANES - shift, 1)
        return jnp.where(lane < LANES - shift, left, right)

    parent = None
    for level in range(last):
        side, nx = 2**level, ROOTS * 2**level
        cells = side * side * nx
        padded = round_up(cells, LANES)
        first = offset_of(level)
        shift = first % LANES
        noise = jnp.concatenate(
            [unshifted(first - shift + t * LANES, shift) for t in range(padded // LANES)], axis=1
        )
        noise = jnp.where(info[1 + level] > 0, noise, 0.0)
        if cells < padded:
            noise = jnp.where(iota((rows, padded), 1) < cells, noise, 0.0)
        if parent is None:
            up = jnp.zeros((rows, padded), F32)
        else:
            q = parent.shape[1]
            half = nx // 2

            def source_of(shape):
                cell = iota(shape, 1)
                x = cell & (nx - 1)
                y = (cell >> log2(nx)) & (side - 1)
                z = cell >> log2(nx * side)
                return x, y, z

            x, y, z = source_of((q, padded))
            source = ((z >> 1) * (side // 2) + (y >> 1)) * half + (x >> 1)
            pick = jnp.where(iota((q, padded), 0) == source, 1.0, 0.0).astype(BF16)
            up = picked(parent, pick)
        cell = iota((rows, padded), 1)
        octant = (
            4 * ((cell >> log2(nx * side)) & 1) + 2 * ((cell >> log2(nx)) & 1) + (cell & 1)
        )
        stack = jnp.concatenate(spread(up, octant, range(8)) + [noise], axis=0)
        parent = dot(w_all, stacked(stack))[:rows]

    r = Region(last, n_slab, n_pencil)
    half = r.nx // 2
    plane = (r.side // 2) * half
    cell = iota((plane, r.part), 1)
    y = (cell >> log2(r.nx)) + pencil * r.ny
    source = (y >> 1) * half + ((cell & (r.nx - 1)) >> 1)
    pick = jnp.where(iota((plane, r.part), 0) == source, 1.0, 0.0).astype(BF16)
    pieces = [split3(parent[:, z * plane : (z + 1) * plane]) for z in range(r.side // 2)]
    ups = dot(jnp.concatenate(pieces, axis=0), pick)
    cell = iota((rows, r.part), 1)
    octant = 2 * ((cell >> log2(r.nx)) & 1) + (cell & 1)
    first = offset_of(last)
    shift = first % LANES
    quad = 4 * rows
    w_z = []
    for octz in range(2):
        w = jnp.concatenate(
            [flat[:, octz * quad : (octz + 1) * quad], flat[:, 2 * quad :]], axis=1
        )
        high, low = split2(w)
        chain_w[octz] = jnp.concatenate([high, high, low], axis=1)
    for z in range(r.side):
        at = (z // 2) * 3 * rows
        up = ups[at : at + rows] + ups[at + rows : at + 2 * rows] + ups[at + 2 * rows : at + 3 * rows]
        start = first - shift + z * r.plane
        noise = jnp.concatenate(
            [
                unshifted(pl.multiple_of(start + pencil * r.part + t * LANES, LANES), shift)
                for t in range(r.part // LANES)
            ],
            axis=1,
        )
        noise = jnp.where(info[1 + last] > 0, noise, 0.0)
        stack = jnp.concatenate(spread(up, octant, range(4)) + [noise], axis=0)
        partial[z] = dot(chain_w[z % 2], stacked(stack))[:rows]

    for octz in range(2):
        fine_w[octz] = weave(fine_rows, fine_mask, fine_place, table[...], innovation[...], maps, octz)
        mid_w[octz] = weave(mid_rows, mid_mask, mid_place, None, innovation[...], maps, octz)


def routes(owner, n_slab):
    inner = 4
    others = [d for d in range(n_slab) if d != owner]
    if n_slab != inner * inner:
        return {d: None for d in others}
    own_z, own_p = divmod(owner, inner)

    def link(dest):
        z, p = divmod(dest, inner)
        if z != own_z:
            return "up" if z > own_z else "down"
        return "x" if (p ^ own_p) & 1 else "y"

    def options(dest):
        p = dest % inner
        found = [(None, link(dest))]
        for bit, name in ((1, "x"), (2, "y")):
            relay = own_z * inner + (own_p ^ bit)
            if relay != dest and (p ^ own_p) & bit:
                found.append((relay, name))
        return found

    load, via = {}, {}
    for d in sorted(others, key=lambda d: (len(options(d)), d)):
        relay, name = min(
            options(d), key=lambda t: load.get(t[1], 0) + (0 if t[0] is None else 0.01)
        )
        load[name] = load.get(name, 0) + 1
        via[d] = relay
    return via


def share_kernel(owner, n_slab, n_pencil, bank, tail, partial, fresh, gathered, relay,
                 send, recv, own, to_relay, onward, give, take, keep):
    r = Region(LAST, n_slab, n_pencil)
    r4 = Region(LAST - 1, n_slab, n_pencil)
    me, pencil = lax.axis_index("slab"), lax.axis_index("pencil")
    base = offset_of(LAST) // LANES * LANES
    via = routes(owner, n_slab)
    relayed = [d for d in via if via[d] is not None]
    direct = [d for d in via if via[d] is None]
    slots = {}
    for d in relayed:
        slots[d] = sum(1 for e in slots if via[e] == via[d])

    def at(d):
        return {"slab": d}

    barrier = pltpu.get_barrier_semaphore()

    def greet(i, _):
        pl.semaphore_signal(
            barrier, inc=1, device_id=at(lax.rem(me + i, n_slab)), device_id_type=MESH
        )
        return 0

    lax.fori_loop(1, n_slab, greet, 0)
    pl.semaphore_wait(barrier, n_slab - 1)

    def source(d, z):
        start = base + (r.first_plane(d) + z) * r.plane + pencil * r.part
        return bank.at[:, :, pl.ds(pl.multiple_of(start, LANES), r.part)]

    def beyond(d, z, act):
        plane = r.first_plane(d) + z
        start = base + plane * r.plane + (pencil + 1) * r.part
        inside = bank.at[:, :, pl.ds(pl.multiple_of(start, LANES), LANES)]
        if isinstance(d, int) and plane < r.side - 1:
            act(inside)
            return
        ends = jnp.logical_and(plane == r.side - 1, pencil == n_pencil - 1)
        pl.when(ends)(lambda: act(tail))
        pl.when(jnp.logical_not(ends))(lambda: act(inside))

    def body(ref):
        return ref.at[:, :, pl.ds(0, r.part)]

    def rest(ref):
        return ref.at[:, :, pl.ds(r.part, LANES)]

    def remote(src, dst, ssem, rsem, d):
        return pltpu.make_async_remote_copy(
            src, dst, ssem, rsem, device_id=at(d), device_id_type=MESH
        )

    def start_block(d, z):
        if isinstance(d, int) and via[d] is not None:
            dst, rsem, to = relay.at[slots[d], z], to_relay.at[slots[d], z], via[d]
        else:
            dst, rsem, to = fresh.at[z], recv.at[z], d
        remote(source(d, z), body(dst), send.at[d, z, 0], rsem.at[0], to).start()
        beyond(d, z, lambda src: remote(src, rest(dst), send.at[d, z, 1], rsem.at[1], to).start())

    def drain_block(d, z):
        remote(source(d, z), body(fresh.at[z]), send.at[d, z, 0], recv.at[z, 0], d).wait_send()
        remote(tail, rest(fresh.at[z]), send.at[d, z, 1], recv.at[z, 1], d).wait_send()

    def landed(dst, rsem, d):
        remote(source(0, 0), body(dst), send.at[0, 0, 0], rsem.at[0], d).wait_recv()
        remote(tail, rest(dst), send.at[0, 0, 1], rsem.at[1], d).wait_recv()

    def forward(d, z):
        return remote(relay.at[slots[d], z], fresh.at[z], onward.at[slots[d], z], recv.at[z, 2], d)

    @pl.when(me == owner)
    def _():
        if relayed:
            for d in relayed + direct:
                for z in range(r.nz):
                    start_block(d, z)
        else:

            def step(i, _):
                for z in range(r.nz):
                    start_block(lax.rem(owner + i, n_slab), z)
                return 0

            lax.fori_loop(1, n_slab, step, 0)
        for z in range(r.nz):
            pltpu.make_async_copy(source(owner, z), body(fresh.at[z]), own.at[z, 0]).start()
            beyond(
                owner,
                z,
                lambda src: pltpu.make_async_copy(src, rest(fresh.at[z]), own.at[z, 1]).start(),
            )

    def piece(d):
        return partial.at[r4.first_plane(d)]

    def give_one(i, _):
        d = lax.rem(me + i, n_slab)
        remote(piece(d), gathered.at[me], give.at[d], take.at[me], d).start()
        return 0

    lax.fori_loop(1, n_slab, give_one, 0)
    mine = pltpu.make_async_copy(piece(me), gathered.at[me], keep)
    mine.start()

    for hub in sorted({via[d] for d in relayed}):

        @pl.when(me == hub)
        def _():
            group = [d for d in relayed if via[d] == hub]
            for d in group:
                for z in range(r.nz):
                    landed(relay.at[slots[d], z], to_relay.at[slots[d], z], owner)
                    forward(d, z).start()
            for d in group:
                for z in range(r.nz):
                    forward(d, z).wait_send()

    through = functools.reduce(jnp.logical_or, [me == d for d in relayed], False)

    @pl.when(jnp.logical_and(me != owner, jnp.logical_not(through)))
    def _():
        for z in range(r.nz):
            landed(fresh.at[z], recv.at[z], owner)

    if relayed:

        @pl.when(through)
        def _():
            for z in range(r.nz):
                remote(relay.at[0, z], fresh.at[z], onward.at[0, z], recv.at[z, 2], owner).wait_recv()

    @pl.when(me == owner)
    def _():
        if relayed:
            for d in relayed + direct:
                for z in range(r.nz):
                    drain_block(d, z)
        else:

            def step(i, _):
                for z in range(r.nz):
                    drain_block(lax.rem(owner + i, n_slab), z)
                return 0

            lax.fori_loop(1, n_slab, step, 0)
        for z in range(r.nz):
            pltpu.make_async_copy(source(owner, z), body(fresh.at[z]), own.at[z, 0]).wait()
            pltpu.make_async_copy(tail, rest(fresh.at[z]), own.at[z, 1]).wait()

    def take_one(i, _):
        d = lax.rem(me + i, n_slab)
        remote(piece(d), gathered.at[d], give.at[d], take.at[d], d).wait()
        return 0

    lax.fori_loop(1, n_slab, take_one, 0)
    mine.wait()


def share(owner, n_slab, n_pencil, count, bank, tail, partial):
    r = Region(LAST, n_slab, n_pencil)
    block = (r.nz, count, 1, r.part + LANES)
    via = routes(owner, n_slab)
    hubs = [v for v in via.values() if v is not None]
    slots = max([hubs.count(h) for h in hubs], default=1)
    dma = pltpu.SemaphoreType.DMA
    anywhere = pl.BlockSpec(memory_space=pl.ANY)
    return pl.pallas_call(
        functools.partial(share_kernel, owner, n_slab, n_pencil),
        in_specs=[anywhere] * 3,
        out_specs=[anywhere] * 2,
        out_shape=[
            jax.ShapeDtypeStruct(block, F32),
            jax.ShapeDtypeStruct((n_slab, *partial.shape[1:]), F32),
        ],
        scratch_shapes=[
            pltpu.VMEM((slots, *block), F32),
            dma((n_slab, r.nz, 2)),
            dma((r.nz, 3)),
            dma((r.nz, 2)),
            dma((slots, r.nz, 2)),
            dma((slots, r.nz)),
            dma((n_slab,)),
            dma((n_slab,)),
            dma,
        ],
        compiler_params=pltpu.CompilerParams(collective_id=owner, has_side_effects=True),
        name="share",
    )(bank, tail, partial)


def middle_kernel(n_slab, n_pencil, per, info, gathered, fresh, noise, chain_w, weights, out,
                  last_coarse):
    r = Region(LAST, n_slab, n_pencil)
    q = Region(LAST - 1, n_slab, n_pencil)
    rows = gathered.shape[1]
    count = noise.shape[0]
    step = pl.program_id(0)
    pencil = info[0]

    @pl.when(step == 0)
    def _():
        parent = gathered[0]
        for d in range(1, gathered.shape[0]):
            parent = parent + gathered[d]
        cell = iota((q.part, r.part), 1)
        source = (cell >> (log2(r.nx) + 1)) * q.nx + ((cell & (r.nx - 1)) >> 1)
        pick = jnp.where(iota((q.part, r.part), 0) == source, 1.0, 0.0).astype(BF16)
        up = picked(parent, pick)
        cell = iota((rows, r.part), 1)
        octant = 2 * ((cell >> log2(r.nx)) & 1) + (cell & 1)
        spreads = spread(up, octant, range(4))
        shift = offset_of(LAST) % LANES
        lane = iota((count, LANES), 1)
        for z in range(r.nz):
            raw = fresh[z, :, 0, :]
            rolled = [
                pltpu.roll(raw[:, t * LANES : (t + 1) * LANES], LANES - shift, 1)
                for t in range(r.part // LANES + 1)
            ]
            block = jnp.concatenate(
                [
                    jnp.where(lane < LANES - shift, rolled[t], rolled[t + 1])
                    for t in range(r.part // LANES)
                ],
                axis=1,
            )
            last_coarse[z] = jnp.zeros_like(last_coarse[z])
            last_coarse[z, :count, :] = block
            stack = jnp.concatenate(spreads + [last_coarse[z]], axis=0)
            octz = (info[1] + z) & 1
            last_coarse[z] = dot(chain_w[octz], stacked(stack))[:rows]

    octz = lax.rem(step, per) if per == 2 else info[2]
    at = step // per
    wide = noise.shape[3]
    lane = iota((rows, LANES), 1)
    even = (lane & 1) == 0
    half = TILE // 2
    across = LANES // r.nx

    def parents(t):
        pieces = []
        for yy in range(half):
            y = t * half + yy
            cells = last_coarse[at, :, (y // across) * LANES : (y // across + 1) * LANES]
            index = (y % across) * r.nx + (lane >> 1)
            pieces.append(jnp.take_along_axis(cells, index, axis=1))
        return [jnp.where(even, p, 0.0) for p in pieces] + [jnp.where(even, 0.0, p) for p in pieces]

    group = 2
    for j in range(noise.shape[2] // (TILE * group)):
        columns = []
        for g in range(group):
            t = j * group + g
            fresh_part = noise[:, 0, t * TILE : (t + 1) * TILE, :].reshape(count * TILE, wide)
            columns.append(jnp.concatenate([fresh_part] + parents(t), axis=0))
        result = dot(weights[octz], stacked(jnp.concatenate(columns, axis=1)))
        size = count * half
        for g in range(group):
            for h in range(2):
                out[0, (j * group + g) * 2 + h] = result[
                    h * size : (h + 1) * size, g * wide : (g + 1) * wide
                ]


def interleave(even, odd):
    rows, cols = even.shape
    lane = iota((rows, LANES), 1)
    half = lane >> 1
    first = (lane & 1) == 0
    parts = []
    for j in range(2 * cols // LANES):
        at = (j // 2) * LANES
        index = half + (j % 2) * (LANES // 2)
        a = jnp.take_along_axis(even[:, at : at + LANES], index, axis=1)
        b = jnp.take_along_axis(odd[:, at : at + LANES], index, axis=1)
        parts.append(jnp.where(first, a, b))
    return jnp.concatenate(parts, axis=1)


def fine_kernel(middle, noise, weights, field, zface, yface, lower, south, carry_z, carry_y):
    count = noise.shape[0]
    cols = noise.shape[3]
    tiles = noise.shape[2] // TILE
    depth_step, row_step = pl.program_id(0), pl.program_id(1)
    small = middle.shape[2]

    @pl.when(depth_step == 0)
    def _():
        carry_z[row_step] = jnp.zeros(carry_z.shape[1:], F32)

    @pl.when(row_step == 0)
    def _():
        carry_y[...] = jnp.zeros_like(carry_y)

    lane = iota((small, LANES), 1)
    even = (iota((small, cols), 1) & 1) == 0
    end_row = iota((TILE, cols), 0) == TILE - 1
    for j in reversed(range(tiles)):
        parts = []
        for c in range(cols // LANES):
            index = (c % 2) * (LANES // 2) + (lane >> 1)
            from_lanes = middle[0, j, :, (c // 2) * LANES : (c // 2 + 1) * LANES]
            parts.append(jnp.take_along_axis(from_lanes, index, axis=1))
        up = jnp.concatenate(parts, axis=1)
        up = jnp.concatenate([jnp.where(even, up, 0.0), jnp.where(even, 0.0, up)], axis=0)
        up_high, up_low = split2(up)
        above = carry_z[row_step, j]
        for octz in (1, 0):
            fresh = noise[:, octz, j * TILE : (j + 1) * TILE, :].reshape(count * TILE, cols)
            high, low = split2(fresh)
            result = dot(
                weights[octz],
                jnp.concatenate([high, up_high, low, up_low, high, up_high], axis=0),
            )
            at = 0

            def take(size):
                nonlocal at
                at += size
                return result[at - size : at]

            rows = slice(2 * TILE * j, 2 * TILE * (j + 1))
            for half in range(2):
                field[2 * octz + half, rows] = interleave(take(2 * TILE), take(2 * TILE))
            top = take(4 * TILE) + above
            zface[octz, rows] = interleave(top[: 2 * TILE], top[2 * TILE :])
            above = take(4 * TILE)
            for half in range(2):
                pair = []
                for side in range(2):
                    k = TILE * side + half
                    edge = carry_y[octz, k : k + 1, :]
                    pair.append(take(TILE) + jnp.where(end_row, edge, 0.0))
                yface[2 * octz + half, TILE * j : TILE * (j + 1)] = interleave(*pair)
            carry_y[octz] = take(2 * TILE)
        carry_z[row_step, j] = above

    @pl.when(depth_step == pl.num_programs(0) - 1)
    def _():
        for j in range(tiles):
            above = carry_z[row_step, j]
            lower[2 * TILE * j : 2 * TILE * (j + 1)] = interleave(
                above[: 2 * TILE], above[2 * TILE :]
            )

    @pl.when(row_step == pl.num_programs(1) - 1)
    def _():
        for octz in range(2):
            edge = carry_y[octz]
            south[0, octz] = interleave(edge[:TILE], edge[TILE:])


def fine_rows():
    table, index = [], {}

    def entry(point, scale):
        key = (point, scale)
        if key not in index:
            index[key] = len(table)
            table.append(scale * basis_row(point))
        return index[key]

    halves = [-0.5, 0.5]
    rows = []
    for pz in halves:
        for px in halves:
            for y in range(TILE):
                for py in halves:
                    rows.append([(entry((pz, py, px), 1.0), y)])
    for w in (1.0, -1.0):
        for px in halves:
            for y in range(TILE):
                for py in halves:
                    rows.append([(entry((w, py, px), 0.5), y)])
    for pz in halves:
        for px in halves:
            for y in range(TILE):
                terms = [(entry((pz, 1.0, px), 0.5), y)]
                if y + 1 < TILE:
                    terms.append((entry((pz, -1.0, px), 0.5), y + 1))
                rows.append(terms)
    for px in halves:
        for pz in halves:
            rows.append([(entry((pz, -1.0, px), 0.5), 0)])
        rows.extend([[]] * (TILE - 2))
    return np.array(table), rows


def layout_of(rows, count, parent_columns):
    columns = count * TILE + 2 * len(parent_columns)
    place = np.zeros((3, LANES, columns), np.float32)
    at_y = np.zeros((columns,), np.int64)
    for k in range(count):
        for y in range(TILE):
            place[0, k, k * TILE + y] = 1
            at_y[k * TILE + y] = y
    for block in (1, 2):
        for i, (k, y) in enumerate(parent_columns):
            c = count * TILE + (block - 1) * len(parent_columns) + i
            at_y[c] = y
            if k < count:
                place[block, k, c] = 1
    noise = np.arange(columns) < count * TILE
    terms = max(len(r) for r in rows)
    pick = np.zeros((terms, len(rows), LANES), np.float32)
    mask = np.zeros((terms, len(rows), columns), np.float32)
    for term in range(terms):
        for i, row in enumerate(rows):
            if term < len(row):
                q, y = row[term]
                pick[term, i, (y % 2) * (LANES // 2) + q] = 1
                mask[term, i] = np.where(noise, at_y == y, at_y == y // 2)
    return tuple(jnp.asarray(a, BF16) for a in (pick, mask, place.reshape(3 * LANES, columns)))


def shards(n_slab, n_pencil, owner_map, window_start, child_maps, innovation, bank,
           noise_middle, noise_finest):
    slab = lax.axis_index("slab").astype(jnp.int32)
    pencil = lax.axis_index("pencil").astype(jnp.int32)
    count = innovation.shape[0]
    padded = round_up(count, 8)
    total = bank.shape[2]
    owners = lax.dynamic_slice(owner_map, (window_start[0],), (BANKS,)).astype(jnp.int32)
    info = jnp.concatenate([pencil[None], (owners == slab).astype(jnp.int32)])
    smem = pl.BlockSpec(memory_space=pltpu.SMEM)
    vmem = pl.BlockSpec(memory_space=pltpu.VMEM)
    top = Region(LAST, n_slab, n_pencil)
    under = Region(LAST - 1, n_slab, n_pencil)

    rows3 = bank.reshape(count, 1, total)
    head_width = offset_of(LAST) // LANES * LANES + LANES
    head = jnp.pad(bank[0, :, :head_width], ((0, padded - count), (0, 0)))
    wide_maps = jnp.pad(child_maps, ((0, 0), (0, padded - count), (0, LANES - count)))
    wide_innovation = jnp.pad(innovation, ((0, padded - count), (0, LANES - count)))
    flat = jnp.concatenate(
        [wide_maps[o, :, :padded] for o in range(8)] + [wide_innovation[:, :padded]], axis=1
    )

    table, row_list = fine_rows()
    half = TILE // 2
    fine_columns = [(k, y) for k in range(count) for y in range(half)]
    fine_parts = layout_of(row_list, count, fine_columns)
    mid_columns = [(k, y) for y in range(half) for k in range(padded)]
    mid_list = [[(k, h * half + y)] for h in range(2) for k in range(count) for y in range(half)]
    mid_parts = layout_of(mid_list, count, mid_columns)
    fine_k, mid_k = fine_parts[1].shape[2], mid_parts[1].shape[2]

    partial, tail, fine_weights, mid_weights, chain_weights = pl.pallas_call(
        functools.partial(head_kernel, n_slab, n_pencil),
        grid=(1,),
        in_specs=[
            smem,
            vmem,
            pl.BlockSpec((count, 1, LANES), lambda i: (0, 0, total // LANES)),
        ]
        + [vmem] * 10,
        out_specs=[vmem] * 5,
        out_shape=[
            jax.ShapeDtypeStruct((under.side, padded, under.part), F32),
            jax.ShapeDtypeStruct((count, 1, LANES), F32),
            jax.ShapeDtypeStruct((2, len(row_list), 3 * fine_k), BF16),
            jax.ShapeDtypeStruct((2, len(mid_list), 3 * mid_k), BF16),
            jax.ShapeDtypeStruct((2, padded, 15 * padded), BF16),
        ],
        name="head",
    )(info, head, rows3, flat, wide_maps, wide_innovation,
      jnp.asarray(np.pad(table, ((0, 0), (0, LANES - count))), F32), *fine_parts, *mid_parts)

    fresh, gathered = lax.switch(
        owners[LAST],
        [functools.partial(share, o, n_slab, n_pencil, count) for o in range(n_slab)],
        rows3, tail, partial,
    )

    _, planes, rows, cols = noise_middle.shape
    per = planes // top.nz
    tiles = 2 * rows // TILE
    place = jnp.stack([pencil, top.first_plane(slab), (slab * planes) % 2])
    middle = pl.pallas_call(
        functools.partial(middle_kernel, n_slab, n_pencil, per),
        grid=(planes,),
        in_specs=[
            smem,
            pl.BlockSpec(gathered.shape, lambda z: (0, 0, 0)),
            pl.BlockSpec(fresh.shape, lambda z: (0, 0, 0, 0)),
            pl.BlockSpec((count, 1, rows, cols), lambda z: (0, z, 0, 0)),
            vmem,
            vmem,
        ],
        out_specs=pl.BlockSpec((1, tiles, count * half, cols), lambda z: (z, 0, 0, 0)),
        out_shape=jax.ShapeDtypeStruct((planes, tiles, count * half, cols), F32),
        scratch_shapes=[pltpu.VMEM((top.nz, padded, top.part), F32)],
        name="middle",
    )(place, gathered, fresh, noise_middle, chain_weights, mid_weights)

    _, fine_planes, fine_y, fine_x = noise_finest.shape
    deep = 16
    nz, ny = planes, fine_y // deep
    out_x = 2 * fine_x
    each = deep // TILE

    def block(*where):
        def index(z, y):
            at = {"z": nz - 1 - z, "y": ny - 1 - y}
            return tuple(at.get(w, 0) for w in where)

        return index

    field, zface, yface, lower, south = pl.pallas_call(
        fine_kernel,
        grid=(nz, ny),
        in_specs=[
            pl.BlockSpec((1, each, count * half, cols), block("z", "y", 0, 0)),
            pl.BlockSpec((count, 2, deep, fine_x), block(0, "z", "y", 0)),
            vmem,
        ],
        out_specs=[
            pl.BlockSpec((4, 2 * deep, out_x), block("z", "y", 0)),
            pl.BlockSpec((2, 2 * deep, out_x), block("z", "y", 0)),
            pl.BlockSpec((4, deep, out_x), block("z", "y", 0)),
            pl.BlockSpec((2 * deep, out_x), block("y", 0)),
            pl.BlockSpec((1, 2, 8, out_x), block("z", 0, 0, 0)),
        ],
        out_shape=[
            jax.ShapeDtypeStruct((2 * fine_planes, 2 * fine_y, out_x), F32),
            jax.ShapeDtypeStruct((fine_planes, 2 * fine_y, out_x), F32),
            jax.ShapeDtypeStruct((2 * fine_planes, fine_y, out_x), F32),
            jax.ShapeDtypeStruct((2 * fine_y, out_x), F32),
            jax.ShapeDtypeStruct((nz, 2, 8, out_x), F32),
        ],
        scratch_shapes=[
            pltpu.VMEM((ny, each, 4 * TILE, fine_x), F32),
            pltpu.VMEM((2, 2 * TILE, fine_x), F32),
        ],
        name="fine",
    )(middle, noise_finest, fine_weights)
    above = shifted(lower, "slab", -1)
    beside = shifted(south[:, :, :2].reshape(2 * fine_planes, out_x), "pencil", -1)
    zface = zface.at[-1].add(above)
    yface = yface.at[:, -1].add(beside)
    return field, zface, yface


def solution(mesh):
    placed = (
        P(),
        P(),
        P(),
        P(),
        P("slab", None, None),
        P(None, "slab", "pencil", None),
        P(None, "slab", "pencil", None),
    )
    return jax.shard_map(
        functools.partial(shards, mesh.shape["slab"], mesh.shape["pencil"]),
        mesh=mesh,
        in_specs=placed,
        out_specs=(P("slab", "pencil", None), P("slab", "pencil", None), P("slab", "pencil", None)),
        check_vma=False,
    )
```

```python
import functools
import math

import jax
import jax.numpy as jnp
import numpy as np
from jax import lax
from jax.experimental import pallas as pl
from jax.experimental.pallas import tpu as pltpu
from jax.sharding import PartitionSpec as P

LEVELS = 8
ROOTS = 2
BANKS = LEVELS - 2
LAST = BANKS - 1
LANES = 128
TILE = 8
BOTTOM = 12
F32 = jnp.float32
BF16 = jnp.bfloat16
MESH = pl.DeviceIdType.MESH


def legendre(order, point):
    values = [1.0, point, 1.5 * point * point - 0.5, 2.5 * point * point * point - 1.5 * point]
    return values[order]


def basis_row(point):
    w_coord, v_coord, u_coord = point
    entry = []
    for deg_x in range(4):
        for deg_y in range(4):
            for deg_z in range(4):
                if deg_x + deg_y + deg_z <= 3:
                    factor = math.sqrt((2 * deg_x + 1) * (2 * deg_y + 1) * (2 * deg_z + 1))
                    entry.append(
                        factor
                        * legendre(deg_x, u_coord)
                        * legendre(deg_y, v_coord)
                        * legendre(deg_z, w_coord)
                    )
    return np.array(entry)


def shifted(block, axis, distance):
    devices = range(lax.axis_size(axis))
    route = [((i - distance) % len(devices), i) for i in devices]
    return lax.ppermute(block, axis, route)


def offset_of(level):
    return ROOTS * (8**level - 1) // 7


def round_up(size, unit):
    return -(-size // unit) * unit


def log2(n):
    return n.bit_length() - 1


class Region:
    def __init__(self, level, n_slab, n_pencil):
        side = 2**level
        self.level = level
        self.side = side
        self.nx = ROOTS * side
        self.ny = side // n_pencil
        self.nz = max(1, side // n_slab)
        self.plane = side * self.nx
        self.part = self.ny * self.nx
        self.n_slab = n_slab

    def first_plane(self, slab):
        return (slab * self.side) // self.n_slab


def split2(value):
    high = value.astype(BF16)
    low = (value - high.astype(F32)).astype(BF16)
    return high, low


def split3(value):
    high, low = split2(value)
    rest = value - high.astype(F32) - low.astype(F32)
    return jnp.concatenate([high.astype(F32), low.astype(F32), rest], axis=0).astype(BF16)


def dot(left, right):
    return jnp.dot(left, right, preferred_element_type=F32)


def exact(left, right):
    left_high, left_low = split2(left)
    right_high, right_low = split2(right)
    return dot(left_high, right_high) + (dot(left_low, right_high) + dot(left_high, right_low))


def chosen(pick, value):
    high, low = split2(value)
    return dot(pick, high) + dot(pick, low)


def placed_at(value, place):
    high, low = split2(value)
    return dot(high, place) + dot(low, place)


def stacked(value):
    high, low = split2(value)
    return jnp.concatenate([high, low, high], axis=0)


def picked(parent, pick):
    rows = parent.shape[0]
    up = dot(split3(parent), pick)
    return up[:rows] + up[rows : 2 * rows] + up[2 * rows :]


def spread(up, octant, names):
    return [jnp.where(octant == o, up, 0.0) for o in names]


def iota(shape, dim):
    return lax.broadcasted_iota(jnp.int32, shape, dim)


def deepened(value, rows):
    return jnp.concatenate(
        [value, jnp.zeros((rows - value.shape[0], value.shape[1]), F32)], axis=0
    )


def weave(table_terms, mask, place, table, innovation, maps, octz):
    both = []
    for octy in range(2):
        o = 4 * octz + 2 * octy
        wide = placed_at(jnp.concatenate([innovation, maps[o], maps[o + 1]], axis=1), place[...])
        if table is not None:
            wide = exact(table, deepened(wide, LANES))
        both.append(deepened(wide, LANES // 2))
    both = jnp.concatenate(both, axis=0)
    total = 0.0
    for term in range(table_terms.shape[0]):
        total = total + chosen(table_terms[term], both) * mask[term].astype(F32)
    high, low = split2(total)
    return jnp.concatenate([high, high, low], axis=1)


def head_kernel(n_slab, n_pencil, owner_map, window_start, head, end, child_maps, innovation,
                table, fine_rows, fine_mask, fine_place, mid_rows, mid_mask, mid_place,
                partial, tail, fine_w, mid_w, chain_w, maps, inner):
    rows = head.shape[0]
    count = innovation.shape[0]
    slab, pencil = lax.axis_index("slab"), lax.axis_index("pencil")

    def owned(level):
        return owner_map[window_start[0] + level] == slab

    tail[...] = end[...]
    maps[...] = jnp.zeros_like(maps)
    inner[...] = jnp.zeros_like(inner)
    maps[:, :count, :count] = child_maps[...]
    inner[:count, :count] = innovation[...]
    quad = 4 * rows
    blocks = []
    for octz in range(2):
        block = 0.0
        for o in range(4):
            block = block + pltpu.roll(maps[4 * octz + o], o * rows, 1)
        blocks.append(block[:, :quad])
    flat = jnp.concatenate(blocks + [inner[:, :rows]], axis=1)
    w_high, w_low = split2(flat)
    w_all = jnp.concatenate([w_high, w_high, w_low], axis=1)
    lane = iota((rows, LANES), 1)
    last = LAST - 1

    def unshifted(at, shift):
        if shift == 0:
            return head[:, pl.ds(at, LANES)]
        left = pltpu.roll(head[:, pl.ds(at, LANES)], LANES - shift, 1)
        right = pltpu.roll(head[:, pl.ds(at + LANES, LANES)], LANES - shift, 1)
        return jnp.where(lane < LANES - shift, left, right)

    parent = None
    for level in range(last):
        side, nx = 2**level, ROOTS * 2**level
        cells = side * side * nx
        padded = round_up(cells, LANES)
        first = offset_of(level)
        shift = first % LANES
        noise = jnp.concatenate(
            [unshifted(first - shift + t * LANES, shift) for t in range(padded // LANES)], axis=1
        )
        noise = jnp.where(owned(level), noise, 0.0)
        if cells < padded:
            noise = jnp.where(iota((rows, padded), 1) < cells, noise, 0.0)
        if parent is None:
            up = jnp.zeros((rows, padded), F32)
        else:
            q = parent.shape[1]
            half = nx // 2

            def source_of(shape):
                cell = iota(shape, 1)
                x = cell & (nx - 1)
                y = (cell >> log2(nx)) & (side - 1)
                z = cell >> log2(nx * side)
                return x, y, z

            x, y, z = source_of((q, padded))
            source = ((z >> 1) * (side // 2) + (y >> 1)) * half + (x >> 1)
            pick = jnp.where(iota((q, padded), 0) == source, 1.0, 0.0).astype(BF16)
            up = picked(parent, pick)
        cell = iota((rows, padded), 1)
        octant = (
            4 * ((cell >> log2(nx * side)) & 1) + 2 * ((cell >> log2(nx)) & 1) + (cell & 1)
        )
        stack = jnp.concatenate(spread(up, octant, range(8)) + [noise], axis=0)
        parent = dot(w_all, stacked(stack))[:rows]

    r = Region(last, n_slab, n_pencil)
    half = r.nx // 2
    plane = (r.side // 2) * half
    cell = iota((plane, r.part), 1)
    y = (cell >> log2(r.nx)) + pencil * r.ny
    source = (y >> 1) * half + ((cell & (r.nx - 1)) >> 1)
    pick = jnp.where(iota((plane, r.part), 0) == source, 1.0, 0.0).astype(BF16)
    pieces = [split3(parent[:, z * plane : (z + 1) * plane]) for z in range(r.side // 2)]
    ups = dot(jnp.concatenate(pieces, axis=0), pick)
    cell = iota((rows, r.part), 1)
    octant = 2 * ((cell >> log2(r.nx)) & 1) + (cell & 1)
    first = offset_of(last)
    shift = first % LANES
    for octz in range(2):
        w = jnp.concatenate([blocks[octz], inner[:, :rows]], axis=1)
        high, low = split2(w)
        chain_w[octz] = jnp.concatenate([high, high, low], axis=1)
    for z in range(r.side):
        at = (z // 2) * 3 * rows
        up = ups[at : at + rows] + ups[at + rows : at + 2 * rows] + ups[at + 2 * rows : at + 3 * rows]
        start = first - shift + z * r.plane
        noise = jnp.concatenate(
            [
                unshifted(pl.multiple_of(start + pencil * r.part + t * LANES, LANES), shift)
                for t in range(r.part // LANES)
            ],
            axis=1,
        )
        noise = jnp.where(owned(last), noise, 0.0)
        stack = jnp.concatenate(spread(up, octant, range(4)) + [noise], axis=0)
        partial[z] = dot(chain_w[z % 2], stacked(stack))[:rows]

    for octz in range(2):
        fine_w[octz] = weave(fine_rows, fine_mask, fine_place, table[...], inner[...], maps, octz)
        mid_w[octz] = weave(mid_rows, mid_mask, mid_place, None, inner[...], maps, octz)


def routes(owner, n_slab):
    inner = 4
    others = [d for d in range(n_slab) if d != owner]
    if n_slab != inner * inner:
        return {d: None for d in others}
    own_z, own_p = divmod(owner, inner)

    def link(dest):
        z, p = divmod(dest, inner)
        if z != own_z:
            return "up" if z > own_z else "down"
        return "x" if (p ^ own_p) & 1 else "y"

    def options(dest):
        p = dest % inner
        found = [(None, link(dest))]
        for bit, name in ((1, "x"), (2, "y")):
            relay = own_z * inner + (own_p ^ bit)
            if relay != dest and (p ^ own_p) & bit:
                found.append((relay, name))
        return found

    load, via = {}, {}
    for d in others:
        load[link(d)] = load.get(link(d), 0) + 0.13
    for d in sorted(others, key=lambda d: (len(options(d)), d)):
        relay, name = min(
            options(d), key=lambda t: load.get(t[1], 0) + (0 if t[0] is None else 0.01)
        )
        load[name] = load.get(name, 0) + 1
        via[d] = relay
    return via


def share_kernel(owner, n_slab, n_pencil, bank, tail, partial, fresh, gathered, relay,
                 send, recv, own, to_relay, onward, give, take, keep):
    r = Region(LAST, n_slab, n_pencil)
    r4 = Region(LAST - 1, n_slab, n_pencil)
    me, pencil = lax.axis_index("slab"), lax.axis_index("pencil")
    base = offset_of(LAST) // LANES * LANES
    via = routes(owner, n_slab)
    relayed = [d for d in via if via[d] is not None]
    direct = [d for d in via if via[d] is None]
    slots = {}
    for d in relayed:
        slots[d] = sum(1 for e in slots if via[e] == via[d])

    def at(d):
        return {"slab": d}

    barrier = pltpu.get_barrier_semaphore()

    def greet(i, _):
        pl.semaphore_signal(
            barrier, inc=1, device_id=at(lax.rem(me + i, n_slab)), device_id_type=MESH
        )
        return 0

    lax.fori_loop(1, n_slab, greet, 0)
    pl.semaphore_wait(barrier, n_slab - 1)

    def source(d, z):
        start = base + (r.first_plane(d) + z) * r.plane + pencil * r.part
        return bank.at[:, :, pl.ds(pl.multiple_of(start, LANES), r.part)]

    def beyond(d, z, act):
        plane = r.first_plane(d) + z
        start = base + plane * r.plane + (pencil + 1) * r.part
        inside = bank.at[:, :, pl.ds(pl.multiple_of(start, LANES), LANES)]
        if isinstance(d, int) and plane < r.side - 1:
            act(inside)
            return
        ends = jnp.logical_and(plane == r.side - 1, pencil == n_pencil - 1)
        pl.when(ends)(lambda: act(tail))
        pl.when(jnp.logical_not(ends))(lambda: act(inside))

    def body(ref):
        return ref.at[:, :, pl.ds(0, r.part)]

    def rest(ref):
        return ref.at[:, :, pl.ds(r.part, LANES)]

    def remote(src, dst, ssem, rsem, d):
        return pltpu.make_async_remote_copy(
            src, dst, ssem, rsem, device_id=at(d), device_id_type=MESH
        )

    def start_block(d, z):
        if isinstance(d, int) and via[d] is not None:
            dst, rsem, to = relay.at[slots[d], z], to_relay.at[slots[d], z], via[d]
        else:
            dst, rsem, to = fresh.at[z], recv.at[z], d
        remote(source(d, z), body(dst), send.at[d, z, 0], rsem.at[0], to).start()
        beyond(d, z, lambda src: remote(src, rest(dst), send.at[d, z, 1], rsem.at[1], to).start())

    def drain_block(d, z):
        remote(source(d, z), body(fresh.at[z]), send.at[d, z, 0], recv.at[z, 0], d).wait_send()
        remote(tail, rest(fresh.at[z]), send.at[d, z, 1], recv.at[z, 1], d).wait_send()

    def landed(dst, rsem, d):
        remote(source(0, 0), body(dst), send.at[0, 0, 0], rsem.at[0], d).wait_recv()
        remote(tail, rest(dst), send.at[0, 0, 1], rsem.at[1], d).wait_recv()

    def forward(d, z):
        return remote(relay.at[slots[d], z], fresh.at[z], onward.at[slots[d], z], recv.at[z, 2], d)

    @pl.when(me == owner)
    def _():
        if relayed:
            for d in relayed + direct:
                for z in range(r.nz):
                    start_block(d, z)
        else:

            def step(i, _):
                for z in range(r.nz):
                    start_block(lax.rem(owner + i, n_slab), z)
                return 0

            lax.fori_loop(1, n_slab, step, 0)
        for z in range(r.nz):
            pltpu.make_async_copy(source(owner, z), body(fresh.at[z]), own.at[z, 0]).start()
            beyond(
                owner,
                z,
                lambda src: pltpu.make_async_copy(src, rest(fresh.at[z]), own.at[z, 1]).start(),
            )

    def piece(d):
        return partial.at[r4.first_plane(d)]

    def give_one(i, _):
        d = lax.rem(me + i, n_slab)
        remote(piece(d), gathered.at[me], give.at[d], take.at[me], d).start()
        return 0

    lax.fori_loop(1, n_slab, give_one, 0)
    mine = pltpu.make_async_copy(piece(me), gathered.at[me], keep)
    mine.start()

    for hub in sorted({via[d] for d in relayed}):

        @pl.when(me == hub)
        def _():
            group = [d for d in relayed if via[d] == hub]
            for d in group:
                for z in range(r.nz):
                    landed(relay.at[slots[d], z], to_relay.at[slots[d], z], owner)
                    forward(d, z).start()
            for d in group:
                for z in range(r.nz):
                    forward(d, z).wait_send()

    through = functools.reduce(jnp.logical_or, [me == d for d in relayed], False)

    @pl.when(jnp.logical_and(me != owner, jnp.logical_not(through)))
    def _():
        for z in range(r.nz):
            landed(fresh.at[z], recv.at[z], owner)

    if relayed:

        @pl.when(through)
        def _():
            for z in range(r.nz):
                remote(relay.at[0, z], fresh.at[z], onward.at[0, z], recv.at[z, 2], owner).wait_recv()

    @pl.when(me == owner)
    def _():
        if relayed:
            for d in relayed + direct:
                for z in range(r.nz):
                    drain_block(d, z)
        else:

            def step(i, _):
                for z in range(r.nz):
                    drain_block(lax.rem(owner + i, n_slab), z)
                return 0

            lax.fori_loop(1, n_slab, step, 0)
        for z in range(r.nz):
            pltpu.make_async_copy(source(owner, z), body(fresh.at[z]), own.at[z, 0]).wait()
            pltpu.make_async_copy(tail, rest(fresh.at[z]), own.at[z, 1]).wait()

    def take_one(i, _):
        d = lax.rem(me + i, n_slab)
        remote(piece(d), gathered.at[d], give.at[d], take.at[d], d).wait()
        return 0

    lax.fori_loop(1, n_slab, take_one, 0)
    mine.wait()


def share(owner, n_slab, n_pencil, count, bank, tail, partial):
    r = Region(LAST, n_slab, n_pencil)
    block = (r.nz, count, 1, r.part + LANES)
    via = routes(owner, n_slab)
    hubs = [v for v in via.values() if v is not None]
    slots = max([hubs.count(h) for h in hubs], default=1)
    dma = pltpu.SemaphoreType.DMA
    anywhere = pl.BlockSpec(memory_space=pl.ANY)
    return pl.pallas_call(
        functools.partial(share_kernel, owner, n_slab, n_pencil),
        in_specs=[anywhere] * 3,
        out_specs=[anywhere] * 2,
        out_shape=[
            jax.ShapeDtypeStruct(block, F32),
            jax.ShapeDtypeStruct((n_slab, *partial.shape[1:]), F32),
        ],
        scratch_shapes=[
            pltpu.VMEM((slots, *block), F32),
            dma((n_slab, r.nz, 2)),
            dma((r.nz, 3)),
            dma((r.nz, 2)),
            dma((slots, r.nz, 2)),
            dma((slots, r.nz)),
            dma((n_slab,)),
            dma((n_slab,)),
            dma,
        ],
        compiler_params=pltpu.CompilerParams(collective_id=owner, has_side_effects=True),
        name="share",
    )(bank, tail, partial)


def middle_kernel(n_slab, n_pencil, per, info, gathered, fresh, noise, chain_w, weights,
                  fine_plane, fine_row, fine_w, out, lower, south, last_coarse):
    r = Region(LAST, n_slab, n_pencil)
    q = Region(LAST - 1, n_slab, n_pencil)
    rows = gathered.shape[1]
    count = noise.shape[0]
    step = pl.program_id(0)
    pencil = info[0]

    @pl.when(step == 0)
    def _():
        parent = gathered[0]
        for d in range(1, gathered.shape[0]):
            parent = parent + gathered[d]
        cell = iota((q.part, r.part), 1)
        source = (cell >> (log2(r.nx) + 1)) * q.nx + ((cell & (r.nx - 1)) >> 1)
        pick = jnp.where(iota((q.part, r.part), 0) == source, 1.0, 0.0).astype(BF16)
        up = picked(parent, pick)
        cell = iota((rows, r.part), 1)
        octant = 2 * ((cell >> log2(r.nx)) & 1) + (cell & 1)
        spreads = spread(up, octant, range(4))
        shift = offset_of(LAST) % LANES
        lane = iota((count, LANES), 1)
        for z in range(r.nz):
            raw = fresh[z, :, 0, :]
            rolled = [
                pltpu.roll(raw[:, t * LANES : (t + 1) * LANES], LANES - shift, 1)
                for t in range(r.part // LANES + 1)
            ]
            block = jnp.concatenate(
                [
                    jnp.where(lane < LANES - shift, rolled[t], rolled[t + 1])
                    for t in range(r.part // LANES)
                ],
                axis=1,
            )
            last_coarse[z] = jnp.zeros_like(last_coarse[z])
            last_coarse[z, :count, :] = block
            stack = jnp.concatenate(spreads + [last_coarse[z]], axis=0)
            octz = (info[1] + z) & 1
            last_coarse[z] = dot(chain_w[octz], stacked(stack))[:rows]

    octz = lax.rem(step, per) if per == 2 else info[2]
    at = step // per
    wide = noise.shape[3]
    lane = iota((rows, LANES), 1)
    even = (lane & 1) == 0
    half = TILE // 2
    across = LANES // r.nx

    def parents(t):
        pieces = []
        for yy in range(half):
            y = t * half + yy
            cells = last_coarse[at, :, (y // across) * LANES : (y // across + 1) * LANES]
            index = (y % across) * r.nx + (lane >> 1)
            pieces.append(jnp.take_along_axis(cells, index, axis=1))
        return [jnp.where(even, p, 0.0) for p in pieces] + [jnp.where(even, 0.0, p) for p in pieces]

    group = 2
    for j in range(noise.shape[2] // (TILE * group)):
        columns = []
        for g in range(group):
            t = j * group + g
            fresh_part = noise[:, 0, t * TILE : (t + 1) * TILE, :].reshape(count * TILE, wide)
            columns.append(jnp.concatenate([fresh_part] + parents(t), axis=0))
        result = dot(weights[octz], stacked(jnp.concatenate(columns, axis=1)))
        size = count * half
        for g in range(group):
            for h in range(2):
                out[0, (j * group + g) * 2 + h] = result[
                    h * size : (h + 1) * size, g * wide : (g + 1) * wide
                ]

    cols = fine_row.shape[3]
    edges = 2 * TILE
    ends = fine_w.shape[1]
    doubled = doubled_columns(out[0, 0], cols)
    for octz in range(2):
        fresh_part = fine_row[:, octz].reshape(count * TILE, cols)
        south[octz] = dot(fine_w[octz, ends - edges :], joined(fresh_part, doubled))

    @pl.when(step == 0)
    def _():
        for t in range(out.shape[1]):
            fresh_part = fine_plane[:, 0, t * TILE : (t + 1) * TILE, :].reshape(count * TILE, cols)
            lower[t] = dot(
                fine_w[0, BOTTOM * TILE : (BOTTOM + 4) * TILE],
                joined(fresh_part, doubled_columns(out[0, t], cols)),
            )


def interleave(even, odd):
    rows, cols = even.shape
    lane = iota((rows, LANES), 1)
    half = LANES // 2
    first = lane < half
    index = (lane >> 1) + (lane & 1) * half
    parts = []
    for j in range(cols // LANES):
        a = even[:, j * LANES : (j + 1) * LANES]
        b = odd[:, j * LANES : (j + 1) * LANES]
        left = jnp.where(first, a, pltpu.roll(b, half, 1))
        right = jnp.where(first, pltpu.roll(a, half, 1), b)
        parts.append(jnp.take_along_axis(left, index, axis=1))
        parts.append(jnp.take_along_axis(right, index, axis=1))
    return jnp.concatenate(parts, axis=1)


def doubled_columns(parent, cols):
    rows = parent.shape[0]
    lane = iota((rows, LANES), 1)
    even = (lane & 1) == 0
    parts = []
    for c in range(cols // LANES):
        index = (c % 2) * (LANES // 2) + (lane >> 1)
        from_lanes = parent[:, (c // 2) * LANES : (c // 2 + 1) * LANES]
        parts.append(jnp.take_along_axis(from_lanes, index, axis=1))
    evens = jnp.concatenate([jnp.where(even, p, 0.0) for p in parts], axis=1)
    odds = jnp.concatenate([jnp.where(even, 0.0, p) for p in parts], axis=1)
    return split2(jnp.concatenate([evens, odds], axis=0))


def joined(fresh, doubled):
    high, low = split2(fresh)
    up_high, up_low = doubled
    return jnp.concatenate([high, up_high, low, up_low, high, up_high], axis=0)


def fine_kernel(middle, noise, weights, field, zface, yface, carry_z, carry_y):
    count = noise.shape[0]
    cols = noise.shape[3]
    tiles = noise.shape[2] // TILE
    depth_step, row_step = pl.program_id(0), pl.program_id(1)

    @pl.when(depth_step == 0)
    def _():
        carry_z[row_step] = jnp.zeros(carry_z.shape[1:], F32)

    @pl.when(row_step == 0)
    def _():
        carry_y[...] = jnp.zeros_like(carry_y)

    end_row = iota((TILE, cols), 0) == TILE - 1
    edges = [carry_y[0], carry_y[1]]
    for j in reversed(range(tiles)):
        doubled = doubled_columns(middle[0, j], cols)
        above = carry_z[row_step, j]
        for octz in (1, 0):
            fresh = noise[:, octz, j * TILE : (j + 1) * TILE, :].reshape(count * TILE, cols)
            result = dot(weights[octz], joined(fresh, doubled))
            at = 0

            def take(size):
                nonlocal at
                at += size
                return result[at - size : at]

            rows = slice(2 * TILE * j, 2 * TILE * (j + 1))
            for half in range(2):
                field[2 * octz + half, rows] = interleave(take(2 * TILE), take(2 * TILE))
            top = take(4 * TILE) + above
            zface[octz, rows] = interleave(top[: 2 * TILE], top[2 * TILE :])
            above = take(4 * TILE)
            for half in range(2):
                pair = []
                for side in range(2):
                    k = TILE * side + half
                    edge = edges[octz][k : k + 1, :]
                    pair.append(take(TILE) + jnp.where(end_row, edge, 0.0))
                yface[2 * octz + half, TILE * j : TILE * (j + 1)] = interleave(*pair)
            edges[octz] = take(2 * TILE)
        carry_z[row_step, j] = above
    for octz in range(2):
        carry_y[octz] = edges[octz]


def seam_kernel(lower, south, zface, yface, z_out, y_out):
    rows = zface.shape[1] // lower.shape[0]
    for t in range(lower.shape[0]):
        block = lower[t]
        at = slice(t * rows, (t + 1) * rows)
        z_out[0, at] = zface[0, at] + interleave(block[:rows], block[rows:])
    last = yface.shape[1] - 1
    end_row = iota(yface.shape[1:], 0) == last
    for plane in range(south.shape[0]):
        edge = interleave(south[plane, :TILE], south[plane, TILE:])
        for half in range(2):
            y_out[2 * plane + half] = yface[2 * plane + half] + jnp.where(
                end_row, edge[half : half + 1], 0.0
            )


def fine_rows():
    table, index = [], {}

    def entry(point, scale):
        key = (point, scale)
        if key not in index:
            index[key] = len(table)
            table.append(scale * basis_row(point))
        return index[key]

    halves = [-0.5, 0.5]
    rows = []
    for pz in halves:
        for px in halves:
            for y in range(TILE):
                for py in halves:
                    rows.append([(entry((pz, py, px), 1.0), y)])
    for w in (1.0, -1.0):
        for px in halves:
            for y in range(TILE):
                for py in halves:
                    rows.append([(entry((w, py, px), 0.5), y)])
    for pz in halves:
        for px in halves:
            for y in range(TILE):
                terms = [(entry((pz, 1.0, px), 0.5), y)]
                if y + 1 < TILE:
                    terms.append((entry((pz, -1.0, px), 0.5), y + 1))
                rows.append(terms)
    for px in halves:
        for pz in halves:
            rows.append([(entry((pz, -1.0, px), 0.5), 0)])
        rows.extend([[]] * (TILE - 2))
    return np.array(table), rows


def layout_of(rows, count, parent_columns):
    columns = count * TILE + 2 * len(parent_columns)
    place = np.zeros((3, LANES, columns), np.float32)
    at_y = np.zeros((columns,), np.int64)
    for k in range(count):
        for y in range(TILE):
            place[0, k, k * TILE + y] = 1
            at_y[k * TILE + y] = y
    for block in (1, 2):
        for i, (k, y) in enumerate(parent_columns):
            c = count * TILE + (block - 1) * len(parent_columns) + i
            at_y[c] = y
            if k < count:
                place[block, k, c] = 1
    noise = np.arange(columns) < count * TILE
    terms = max(len(r) for r in rows)
    pick = np.zeros((terms, len(rows), LANES), np.float32)
    mask = np.zeros((terms, len(rows), columns), np.float32)
    for term in range(terms):
        for i, row in enumerate(rows):
            if term < len(row):
                q, y = row[term]
                pick[term, i, (y % 2) * (LANES // 2) + q] = 1
                mask[term, i] = np.where(noise, at_y == y, at_y == y // 2)
    return tuple(jnp.asarray(a, BF16) for a in (pick, mask, place.reshape(3 * LANES, columns)))


def shards(n_slab, n_pencil, owner_map, window_start, child_maps, innovation, bank,
           noise_middle, noise_finest):
    slab = lax.axis_index("slab").astype(jnp.int32)
    pencil = lax.axis_index("pencil").astype(jnp.int32)
    count = innovation.shape[0]
    padded = round_up(count, 8)
    total = bank.shape[2]
    owner = owner_map[window_start[0] + LAST]
    smem = pl.BlockSpec(memory_space=pltpu.SMEM)
    vmem = pl.BlockSpec(memory_space=pltpu.VMEM)
    top = Region(LAST, n_slab, n_pencil)
    under = Region(LAST - 1, n_slab, n_pencil)

    rows3 = bank.reshape(count, 1, total)
    head_width = offset_of(LAST) // LANES * LANES + LANES
    head = jnp.pad(bank[0, :, :head_width], ((0, padded - count), (0, 0)))
    table, row_list = fine_rows()
    half = TILE // 2
    fine_columns = [(k, y) for k in range(count) for y in range(half)]
    fine_parts = layout_of(row_list, count, fine_columns)
    mid_columns = [(k, y) for y in range(half) for k in range(padded)]
    mid_list = [[(k, h * half + y)] for h in range(2) for k in range(count) for y in range(half)]
    mid_parts = layout_of(mid_list, count, mid_columns)
    fine_k, mid_k = fine_parts[1].shape[2], mid_parts[1].shape[2]

    partial, tail, fine_weights, mid_weights, chain_weights = pl.pallas_call(
        functools.partial(head_kernel, n_slab, n_pencil),
        grid=(1,),
        in_specs=[
            smem,
            smem,
            vmem,
            pl.BlockSpec((count, 1, LANES), lambda i: (0, 0, total // LANES)),
        ]
        + [vmem] * 9,
        out_specs=[vmem] * 5,
        out_shape=[
            jax.ShapeDtypeStruct((under.side, padded, under.part), F32),
            jax.ShapeDtypeStruct((count, 1, LANES), F32),
            jax.ShapeDtypeStruct((2, len(row_list), 3 * fine_k), BF16),
            jax.ShapeDtypeStruct((2, len(mid_list), 3 * mid_k), BF16),
            jax.ShapeDtypeStruct((2, padded, 15 * padded), BF16),
        ],
        scratch_shapes=[pltpu.VMEM((8, padded, LANES), F32), pltpu.VMEM((padded, LANES), F32)],
        name="head",
    )(owner_map, window_start, head, rows3, child_maps, innovation,
      jnp.asarray(np.pad(table, ((0, 0), (0, LANES - count))), F32), *fine_parts, *mid_parts)

    fresh, gathered = lax.switch(
        owner,
        [functools.partial(share, o, n_slab, n_pencil, count) for o in range(n_slab)],
        rows3, tail, partial,
    )

    _, planes, rows, cols = noise_middle.shape
    per = planes // top.nz
    tiles = 2 * rows // TILE
    _, fine_planes, fine_y, fine_x = noise_finest.shape
    out_x = 2 * fine_x
    place = jnp.stack([pencil, top.first_plane(slab), (slab * planes) % 2])
    middle, lower, south = pl.pallas_call(
        functools.partial(middle_kernel, n_slab, n_pencil, per),
        grid=(planes,),
        in_specs=[
            smem,
            pl.BlockSpec(gathered.shape, lambda z: (0, 0, 0)),
            pl.BlockSpec(fresh.shape, lambda z: (0, 0, 0, 0)),
            pl.BlockSpec((count, 1, rows, cols), lambda z: (0, z, 0, 0)),
            vmem,
            vmem,
            pl.BlockSpec((count, 1, fine_y, fine_x), lambda z: (0, 0, 0, 0)),
            pl.BlockSpec((count, 2, TILE, fine_x), lambda z: (0, z, 0, 0)),
            vmem,
        ],
        out_specs=[
            pl.BlockSpec((1, tiles, count * half, cols), lambda z: (z, 0, 0, 0)),
            pl.BlockSpec((tiles, 4 * TILE, fine_x), lambda z: (0, 0, 0)),
            pl.BlockSpec((2, 2 * TILE, fine_x), lambda z: (z, 0, 0)),
        ],
        out_shape=[
            jax.ShapeDtypeStruct((planes, tiles, count * half, cols), F32),
            jax.ShapeDtypeStruct((tiles, 4 * TILE, fine_x), F32),
            jax.ShapeDtypeStruct((fine_planes, 2 * TILE, fine_x), F32),
        ],
        scratch_shapes=[pltpu.VMEM((top.nz, padded, top.part), F32)],
        name="middle",
    )(place, gathered, fresh, noise_middle, chain_weights, mid_weights, noise_finest, noise_finest,
      fine_weights)
    above = shifted(lower, "slab", -1)
    beside = shifted(south, "pencil", -1)

    deep = 32
    nz, ny = planes, fine_y // deep
    each = deep // TILE

    def block(*where):
        def index(z, y):
            at = {"z": nz - 1 - z, "y": ny - 1 - y}
            return tuple(at.get(w, 0) for w in where)

        return index

    field, zface, yface = pl.pallas_call(
        fine_kernel,
        grid=(nz, ny),
        in_specs=[
            pl.BlockSpec((1, each, count * half, cols), block("z", "y", 0, 0)),
            pl.BlockSpec((count, 2, deep, fine_x), block(0, "z", "y", 0)),
            vmem,
        ],
        out_specs=[
            pl.BlockSpec((4, 2 * deep, out_x), block("z", "y", 0)),
            pl.BlockSpec((2, 2 * deep, out_x), block("z", "y", 0)),
            pl.BlockSpec((4, deep, out_x), block("z", "y", 0)),
        ],
        out_shape=[
            jax.ShapeDtypeStruct((2 * fine_planes, 2 * fine_y, out_x), F32),
            jax.ShapeDtypeStruct((fine_planes, 2 * fine_y, out_x), F32),
            jax.ShapeDtypeStruct((2 * fine_planes, fine_y, out_x), F32),
        ],
        scratch_shapes=[
            pltpu.VMEM((ny, each, 4 * TILE, fine_x), F32),
            pltpu.VMEM((2, 2 * TILE, fine_x), F32),
        ],
        cost_estimate=pl.CostEstimate(
            flops=2 * nz * (fine_y // TILE) * fine_weights.size * fine_x,
            bytes_accessed=4 * (noise_finest.size + 16 * fine_planes * fine_y * fine_x),
            transcendentals=0,
        ),
        name="fine",
    )(middle, noise_finest, fine_weights)
    z_spec = pl.BlockSpec((1, 2 * fine_y, out_x), lambda i: (fine_planes - 1, 0, 0))
    y_spec = pl.BlockSpec((2 * fine_planes, TILE, out_x), lambda i: (0, fine_y // TILE - 1, 0))
    zface, yface = pl.pallas_call(
        seam_kernel,
        grid=(1,),
        in_specs=[
            pl.BlockSpec(above.shape, lambda i: (0, 0, 0)),
            pl.BlockSpec(beside.shape, lambda i: (0, 0, 0)),
            z_spec,
            y_spec,
        ],
        out_specs=[z_spec, y_spec],
        out_shape=[
            jax.ShapeDtypeStruct(zface.shape, F32),
            jax.ShapeDtypeStruct(yface.shape, F32),
        ],
        input_output_aliases={2: 0, 3: 1},
        name="seam",
    )(above, beside, zface, yface)
    return field, zface, yface


def solution(mesh):
    placed = (
        P(),
        P(),
        P(),
        P(),
        P("slab", None, None),
        P(None, "slab", "pencil", None),
        P(None, "slab", "pencil", None),
    )
    return jax.shard_map(
        functools.partial(shards, mesh.shape["slab"], mesh.shape["pencil"]),
        mesh=mesh,
        in_specs=placed,
        out_specs=(P("slab", "pencil", None), P("slab", "pencil", None), P("slab", "pencil", None)),
        check_vma=False,
    )
```

```python
import functools
import math

import jax
import jax.numpy as jnp
import numpy as np
from jax import lax
from jax.experimental import pallas as pl
from jax.experimental.pallas import tpu as pltpu
from jax.sharding import PartitionSpec as P

LEVELS = 8
ROOTS = 2
BANKS = LEVELS - 2
LAST = BANKS - 1
LANES = 128
TILE = 8
BOTTOM = 12
MIB = 1 << 20
F32 = jnp.float32
BF16 = jnp.bfloat16
MESH = pl.DeviceIdType.MESH


def legendre(order, point):
    values = [1.0, point, 1.5 * point * point - 0.5, 2.5 * point * point * point - 1.5 * point]
    return values[order]


def basis_row(point):
    w_coord, v_coord, u_coord = point
    entry = []
    for deg_x in range(4):
        for deg_y in range(4):
            for deg_z in range(4):
                if deg_x + deg_y + deg_z <= 3:
                    factor = math.sqrt((2 * deg_x + 1) * (2 * deg_y + 1) * (2 * deg_z + 1))
                    entry.append(
                        factor
                        * legendre(deg_x, u_coord)
                        * legendre(deg_y, v_coord)
                        * legendre(deg_z, w_coord)
                    )
    return np.array(entry)


def shifted(block, axis, distance):
    devices = range(lax.axis_size(axis))
    route = [((i - distance) % len(devices), i) for i in devices]
    return lax.ppermute(block, axis, route)


def offset_of(level):
    return ROOTS * (8**level - 1) // 7


def round_up(size, unit):
    return -(-size // unit) * unit


def log2(n):
    return n.bit_length() - 1


class Region:
    def __init__(self, level, n_slab, n_pencil):
        side = 2**level
        self.level = level
        self.side = side
        self.nx = ROOTS * side
        self.ny = side // n_pencil
        self.nz = max(1, side // n_slab)
        self.plane = side * self.nx
        self.part = self.ny * self.nx
        self.n_slab = n_slab

    def first_plane(self, slab):
        return (slab * self.side) // self.n_slab


def split2(value):
    high = value.astype(BF16)
    low = (value - high.astype(F32)).astype(BF16)
    return high, low


def split3(value):
    high, low = split2(value)
    rest = value - high.astype(F32) - low.astype(F32)
    return jnp.concatenate([high.astype(F32), low.astype(F32), rest], axis=0).astype(BF16)


def dot(left, right):
    return jnp.dot(left, right, preferred_element_type=F32)


def exact(left, right):
    left_high, left_low = split2(left)
    right_high, right_low = split2(right)
    return dot(left_high, right_high) + (dot(left_low, right_high) + dot(left_high, right_low))


def chosen(pick, value):
    high, low = split2(value)
    return dot(pick, high) + dot(pick, low)


def placed_at(value, place):
    high, low = split2(value)
    return dot(high, place) + dot(low, place)


def stacked(value):
    high, low = split2(value)
    return jnp.concatenate([high, low, high], axis=0)


def picked(parent, pick):
    rows = parent.shape[0]
    up = dot(split3(parent), pick)
    return up[:rows] + up[rows : 2 * rows] + up[2 * rows :]


def spread(up, octant, names):
    return [jnp.where(octant == o, up, 0.0) for o in names]


def iota(shape, dim):
    return lax.broadcasted_iota(jnp.int32, shape, dim)


def deepened(value, rows):
    return jnp.concatenate(
        [value, jnp.zeros((rows - value.shape[0], value.shape[1]), F32)], axis=0
    )


def weave(table_terms, mask, place, table, innovation, maps, octz):
    both = []
    for octy in range(2):
        o = 4 * octz + 2 * octy
        wide = placed_at(jnp.concatenate([innovation, maps[o], maps[o + 1]], axis=1), place[...])
        if table is not None:
            wide = exact(table, deepened(wide, LANES))
        both.append(deepened(wide, LANES // 2))
    both = jnp.concatenate(both, axis=0)
    total = 0.0
    for term in range(table_terms.shape[0]):
        total = total + chosen(table_terms[term], both) * mask[term].astype(F32)
    high, low = split2(total)
    return jnp.concatenate([high, high, low], axis=1)


def head_kernel(n_slab, n_pencil, owner_map, window_start, bank, end, child_maps, innovation,
                table, fine_rows, fine_mask, fine_place, mid_rows, mid_mask, mid_place,
                partial, tail, fine_w, mid_w, chain_w, maps, inner, head):
    rows = head.shape[0]
    count = innovation.shape[0]
    head[count // 8 * 8 :, :] = jnp.zeros((rows - count // 8 * 8, head.shape[1]), F32)
    head[:count, :] = bank[...]
    slab, pencil = lax.axis_index("slab"), lax.axis_index("pencil")

    def owned(level):
        return owner_map[window_start[0] + level] == slab

    tail[...] = end[...]
    maps[...] = jnp.zeros_like(maps)
    inner[...] = jnp.zeros_like(inner)
    for o in range(8):
        maps[o, :count, :count] = child_maps[:, o, :]
    inner[:count, :count] = innovation[...]
    quad = 4 * rows
    blocks = []
    for octz in range(2):
        block = 0.0
        for o in range(4):
            block = block + pltpu.roll(maps[4 * octz + o], o * rows, 1)
        blocks.append(block[:, :quad])
    flat = jnp.concatenate(blocks + [inner[:, :rows]], axis=1)
    w_high, w_low = split2(flat)
    w_all = jnp.concatenate([w_high, w_high, w_low], axis=1)
    lane = iota((rows, LANES), 1)
    last = LAST - 1

    def unshifted(at, shift):
        if shift == 0:
            return head[:, pl.ds(at, LANES)]
        left = pltpu.roll(head[:, pl.ds(at, LANES)], LANES - shift, 1)
        right = pltpu.roll(head[:, pl.ds(at + LANES, LANES)], LANES - shift, 1)
        return jnp.where(lane < LANES - shift, left, right)

    parent = None
    for level in range(last):
        side, nx = 2**level, ROOTS * 2**level
        cells = side * side * nx
        padded = round_up(cells, LANES)
        first = offset_of(level)
        shift = first % LANES
        noise = jnp.concatenate(
            [unshifted(first - shift + t * LANES, shift) for t in range(padded // LANES)], axis=1
        )
        noise = jnp.where(owned(level), noise, 0.0)
        if cells < padded:
            noise = jnp.where(iota((rows, padded), 1) < cells, noise, 0.0)
        if parent is None:
            up = jnp.zeros((rows, padded), F32)
        else:
            q = parent.shape[1]
            half = nx // 2

            def source_of(shape):
                cell = iota(shape, 1)
                x = cell & (nx - 1)
                y = (cell >> log2(nx)) & (side - 1)
                z = cell >> log2(nx * side)
                return x, y, z

            x, y, z = source_of((q, padded))
            source = ((z >> 1) * (side // 2) + (y >> 1)) * half + (x >> 1)
            pick = jnp.where(iota((q, padded), 0) == source, 1.0, 0.0).astype(BF16)
            up = picked(parent, pick)
        cell = iota((rows, padded), 1)
        octant = (
            4 * ((cell >> log2(nx * side)) & 1) + 2 * ((cell >> log2(nx)) & 1) + (cell & 1)
        )
        stack = jnp.concatenate(spread(up, octant, range(8)) + [noise], axis=0)
        parent = dot(w_all, stacked(stack))[:rows]

    r = Region(last, n_slab, n_pencil)
    half = r.nx // 2
    plane = (r.side // 2) * half
    cell = iota((plane, r.part), 1)
    y = (cell >> log2(r.nx)) + pencil * r.ny
    source = (y >> 1) * half + ((cell & (r.nx - 1)) >> 1)
    pick = jnp.where(iota((plane, r.part), 0) == source, 1.0, 0.0).astype(BF16)
    pieces = [split3(parent[:, z * plane : (z + 1) * plane]) for z in range(r.side // 2)]
    ups = dot(jnp.concatenate(pieces, axis=0), pick)
    cell = iota((rows, r.part), 1)
    octant = 2 * ((cell >> log2(r.nx)) & 1) + (cell & 1)
    first = offset_of(last)
    shift = first % LANES
    for octz in range(2):
        w = jnp.concatenate([blocks[octz], inner[:, :rows]], axis=1)
        high, low = split2(w)
        chain_w[octz] = jnp.concatenate([high, high, low], axis=1)
    for z in range(r.side):
        at = (z // 2) * 3 * rows
        up = ups[at : at + rows] + ups[at + rows : at + 2 * rows] + ups[at + 2 * rows : at + 3 * rows]
        start = first - shift + z * r.plane
        noise = jnp.concatenate(
            [
                unshifted(pl.multiple_of(start + pencil * r.part + t * LANES, LANES), shift)
                for t in range(r.part // LANES)
            ],
            axis=1,
        )
        noise = jnp.where(owned(last), noise, 0.0)
        stack = jnp.concatenate(spread(up, octant, range(4)) + [noise], axis=0)
        partial[z] = dot(chain_w[z % 2], stacked(stack))[:rows]

    for octz in range(2):
        fine_w[octz] = weave(fine_rows, fine_mask, fine_place, table[...], inner[...], maps, octz)
        mid_w[octz] = weave(mid_rows, mid_mask, mid_place, None, inner[...], maps, octz)


def routes(owner, n_slab):
    inner = 4
    others = [d for d in range(n_slab) if d != owner]
    if n_slab != inner * inner:
        return {d: None for d in others}
    own_z, own_p = divmod(owner, inner)

    def link(dest):
        z, p = divmod(dest, inner)
        if z != own_z:
            return "up" if z > own_z else "down"
        return "x" if (p ^ own_p) & 1 else "y"

    def options(dest):
        p = dest % inner
        found = [(None, link(dest))]
        for bit, name in ((1, "x"), (2, "y")):
            relay = own_z * inner + (own_p ^ bit)
            if relay != dest and (p ^ own_p) & bit:
                found.append((relay, name))
        return found

    load, via = {}, {}
    for d in others:
        load[link(d)] = load.get(link(d), 0) + 0.13
    for d in sorted(others, key=lambda d: (len(options(d)), d)):
        relay, name = min(
            options(d), key=lambda t: load.get(t[1], 0) + (0 if t[0] is None else 0.01)
        )
        load[name] = load.get(name, 0) + 1
        via[d] = relay
    return via


def share_kernel(owner, n_slab, n_pencil, bank, tail, partial, fresh, gathered, relay,
                 send, recv, own, to_relay, onward, give, take, keep):
    r = Region(LAST, n_slab, n_pencil)
    r4 = Region(LAST - 1, n_slab, n_pencil)
    me, pencil = lax.axis_index("slab"), lax.axis_index("pencil")
    base = offset_of(LAST) // LANES * LANES
    via = routes(owner, n_slab)
    relayed = [d for d in via if via[d] is not None]
    direct = [d for d in via if via[d] is None]
    slots = {}
    for d in relayed:
        slots[d] = sum(1 for e in slots if via[e] == via[d])

    def at(d):
        return {"slab": d}

    barrier = pltpu.get_barrier_semaphore()

    def greet(i, _):
        pl.semaphore_signal(
            barrier, inc=1, device_id=at(lax.rem(me + i, n_slab)), device_id_type=MESH
        )
        return 0

    lax.fori_loop(1, n_slab, greet, 0)
    pl.semaphore_wait(barrier, n_slab - 1)

    def source(d, z):
        start = base + (r.first_plane(d) + z) * r.plane + pencil * r.part
        return bank.at[:, :, pl.ds(pl.multiple_of(start, LANES), r.part)]

    def beyond(d, z, act):
        plane = r.first_plane(d) + z
        start = base + plane * r.plane + (pencil + 1) * r.part
        inside = bank.at[:, :, pl.ds(pl.multiple_of(start, LANES), LANES)]
        if isinstance(d, int) and plane < r.side - 1:
            act(inside)
            return
        ends = jnp.logical_and(plane == r.side - 1, pencil == n_pencil - 1)
        pl.when(ends)(lambda: act(tail))
        pl.when(jnp.logical_not(ends))(lambda: act(inside))

    def body(ref):
        return ref.at[:, :, pl.ds(0, r.part)]

    def rest(ref):
        return ref.at[:, :, pl.ds(r.part, LANES)]

    def remote(src, dst, ssem, rsem, d):
        return pltpu.make_async_remote_copy(
            src, dst, ssem, rsem, device_id=at(d), device_id_type=MESH
        )

    def start_block(d, z):
        if isinstance(d, int) and via[d] is not None:
            dst, rsem, to = relay.at[slots[d], z], to_relay.at[slots[d], z], via[d]
        else:
            dst, rsem, to = fresh.at[z], recv.at[z], d
        remote(source(d, z), body(dst), send.at[d, z, 0], rsem.at[0], to).start()
        beyond(d, z, lambda src: remote(src, rest(dst), send.at[d, z, 1], rsem.at[1], to).start())

    def drain_block(d, z):
        remote(source(d, z), body(fresh.at[z]), send.at[d, z, 0], recv.at[z, 0], d).wait_send()
        remote(tail, rest(fresh.at[z]), send.at[d, z, 1], recv.at[z, 1], d).wait_send()

    def landed(dst, rsem, d):
        remote(source(0, 0), body(dst), send.at[0, 0, 0], rsem.at[0], d).wait_recv()
        remote(tail, rest(dst), send.at[0, 0, 1], rsem.at[1], d).wait_recv()

    def forward(d, z):
        return remote(relay.at[slots[d], z], fresh.at[z], onward.at[slots[d], z], recv.at[z, 2], d)

    @pl.when(me == owner)
    def _():
        if relayed:
            for d in relayed + direct:
                for z in range(r.nz):
                    start_block(d, z)
        else:

            def step(i, _):
                for z in range(r.nz):
                    start_block(lax.rem(owner + i, n_slab), z)
                return 0

            lax.fori_loop(1, n_slab, step, 0)
        for z in range(r.nz):
            pltpu.make_async_copy(source(owner, z), body(fresh.at[z]), own.at[z, 0]).start()
            beyond(
                owner,
                z,
                lambda src: pltpu.make_async_copy(src, rest(fresh.at[z]), own.at[z, 1]).start(),
            )

    def piece(d):
        return partial.at[r4.first_plane(d)]

    def give_one(i, _):
        d = lax.rem(me + i, n_slab)
        remote(piece(d), gathered.at[me], give.at[d], take.at[me], d).start()
        return 0

    lax.fori_loop(1, n_slab, give_one, 0)
    mine = pltpu.make_async_copy(piece(me), gathered.at[me], keep)
    mine.start()

    for hub in sorted({via[d] for d in relayed}):

        @pl.when(me == hub)
        def _():
            group = [d for d in relayed if via[d] == hub]
            for d in group:
                for z in range(r.nz):
                    landed(relay.at[slots[d], z], to_relay.at[slots[d], z], owner)
                    forward(d, z).start()
            for d in group:
                for z in range(r.nz):
                    forward(d, z).wait_send()

    through = functools.reduce(jnp.logical_or, [me == d for d in relayed], False)

    @pl.when(jnp.logical_and(me != owner, jnp.logical_not(through)))
    def _():
        for z in range(r.nz):
            landed(fresh.at[z], recv.at[z], owner)

    if relayed:

        @pl.when(through)
        def _():
            for z in range(r.nz):
                remote(relay.at[0, z], fresh.at[z], onward.at[0, z], recv.at[z, 2], owner).wait_recv()

    @pl.when(me == owner)
    def _():
        if relayed:
            for d in relayed + direct:
                for z in range(r.nz):
                    drain_block(d, z)
        else:

            def step(i, _):
                for z in range(r.nz):
                    drain_block(lax.rem(owner + i, n_slab), z)
                return 0

            lax.fori_loop(1, n_slab, step, 0)
        for z in range(r.nz):
            pltpu.make_async_copy(source(owner, z), body(fresh.at[z]), own.at[z, 0]).wait()
            pltpu.make_async_copy(tail, rest(fresh.at[z]), own.at[z, 1]).wait()

    def take_one(i, _):
        d = lax.rem(me + i, n_slab)
        remote(piece(d), gathered.at[d], give.at[d], take.at[d], d).wait()
        return 0

    lax.fori_loop(1, n_slab, take_one, 0)
    mine.wait()


def share(owner, n_slab, n_pencil, count, bank, tail, partial):
    r = Region(LAST, n_slab, n_pencil)
    block = (r.nz, count, 1, r.part + LANES)
    via = routes(owner, n_slab)
    hubs = [v for v in via.values() if v is not None]
    slots = max([hubs.count(h) for h in hubs], default=1)
    dma = pltpu.SemaphoreType.DMA
    anywhere = pl.BlockSpec(memory_space=pl.ANY)
    return pl.pallas_call(
        functools.partial(share_kernel, owner, n_slab, n_pencil),
        in_specs=[anywhere] * 3,
        out_specs=[anywhere] * 2,
        out_shape=[
            jax.ShapeDtypeStruct(block, F32),
            jax.ShapeDtypeStruct((n_slab, *partial.shape[1:]), F32),
        ],
        scratch_shapes=[
            pltpu.VMEM((slots, *block), F32),
            dma((n_slab, r.nz, 2)),
            dma((r.nz, 3)),
            dma((r.nz, 2)),
            dma((slots, r.nz, 2)),
            dma((slots, r.nz)),
            dma((n_slab,)),
            dma((n_slab,)),
            dma,
        ],
        compiler_params=pltpu.CompilerParams(
            collective_id=owner, has_side_effects=True, vmem_limit_bytes=8 * MIB
        ),
        name="share",
    )(bank, tail, partial)


def middle_kernel(n_slab, n_pencil, per, gathered, fresh, noise, chain_w, weights,
                  fine_plane, fine_row, fine_w, out, lower, south, last_coarse):
    r = Region(LAST, n_slab, n_pencil)
    q = Region(LAST - 1, n_slab, n_pencil)
    rows = gathered.shape[1]
    count = noise.shape[0]
    step = pl.program_id(0)
    slab = lax.axis_index("slab")

    @pl.when(step == 0)
    def _():
        parent = gathered[0]
        for d in range(1, gathered.shape[0]):
            parent = parent + gathered[d]
        cell = iota((q.part, r.part), 1)
        source = (cell >> (log2(r.nx) + 1)) * q.nx + ((cell & (r.nx - 1)) >> 1)
        pick = jnp.where(iota((q.part, r.part), 0) == source, 1.0, 0.0).astype(BF16)
        up = picked(parent, pick)
        cell = iota((rows, r.part), 1)
        octant = 2 * ((cell >> log2(r.nx)) & 1) + (cell & 1)
        spreads = spread(up, octant, range(4))
        shift = offset_of(LAST) % LANES
        lane = iota((count, LANES), 1)
        for z in range(r.nz):
            raw = fresh[z, :, 0, :]
            rolled = [
                pltpu.roll(raw[:, t * LANES : (t + 1) * LANES], LANES - shift, 1)
                for t in range(r.part // LANES + 1)
            ]
            block = jnp.concatenate(
                [
                    jnp.where(lane < LANES - shift, rolled[t], rolled[t + 1])
                    for t in range(r.part // LANES)
                ],
                axis=1,
            )
            last_coarse[z] = jnp.zeros_like(last_coarse[z])
            last_coarse[z, :count, :] = block
            stack = jnp.concatenate(spreads + [last_coarse[z]], axis=0)
            octz = (r.first_plane(slab) + z) & 1
            last_coarse[z] = dot(chain_w[octz], stacked(stack))[:rows]

    octz = lax.rem(slab * per * r.nz + step, 2)
    at = step // per
    wide = noise.shape[3]
    lane = iota((rows, LANES), 1)
    even = (lane & 1) == 0
    half = TILE // 2
    across = LANES // r.nx

    def parents(t):
        pieces = []
        for yy in range(half):
            y = t * half + yy
            cells = last_coarse[at, :, (y // across) * LANES : (y // across + 1) * LANES]
            index = (y % across) * r.nx + (lane >> 1)
            pieces.append(jnp.take_along_axis(cells, index, axis=1))
        return [jnp.where(even, p, 0.0) for p in pieces] + [jnp.where(even, 0.0, p) for p in pieces]

    group = 2
    for j in range(noise.shape[2] // (TILE * group)):
        columns = []
        for g in range(group):
            t = j * group + g
            fresh_part = noise[:, 0, t * TILE : (t + 1) * TILE, :].reshape(count * TILE, wide)
            columns.append(jnp.concatenate([fresh_part] + parents(t), axis=0))
        result = dot(weights[octz], stacked(jnp.concatenate(columns, axis=1)))
        size = count * half
        for g in range(group):
            for h in range(2):
                out[0, (j * group + g) * 2 + h] = result[
                    h * size : (h + 1) * size, g * wide : (g + 1) * wide
                ]

    cols = fine_row.shape[3]
    edges = 2 * TILE
    ends = fine_w.shape[1]
    doubled = doubled_columns(out[0, 0], cols)
    for octz in range(2):
        fresh_part = fine_row[:, octz].reshape(count * TILE, cols)
        south[octz] = dot(fine_w[octz, ends - edges :], joined(fresh_part, doubled))

    @pl.when(step == 0)
    def _():
        for t in range(out.shape[1]):
            fresh_part = fine_plane[:, 0, t * TILE : (t + 1) * TILE, :].reshape(count * TILE, cols)
            lower[t] = dot(
                fine_w[0, BOTTOM * TILE : (BOTTOM + 4) * TILE],
                joined(fresh_part, doubled_columns(out[0, t], cols)),
            )


def interleave(even, odd):
    rows, cols = even.shape
    lane = iota((rows, LANES), 1)
    half = LANES // 2
    first = lane < half
    index = (lane >> 1) + (lane & 1) * half
    parts = []
    for j in range(cols // LANES):
        a = even[:, j * LANES : (j + 1) * LANES]
        b = odd[:, j * LANES : (j + 1) * LANES]
        left = jnp.where(first, a, pltpu.roll(b, half, 1))
        right = jnp.where(first, pltpu.roll(a, half, 1), b)
        parts.append(jnp.take_along_axis(left, index, axis=1))
        parts.append(jnp.take_along_axis(right, index, axis=1))
    return jnp.concatenate(parts, axis=1)


def doubled_columns(parent, cols):
    rows = parent.shape[0]
    lane = iota((rows, LANES), 1)
    even = (lane & 1) == 0
    parts = []
    for c in range(cols // LANES):
        index = (c % 2) * (LANES // 2) + (lane >> 1)
        from_lanes = parent[:, (c // 2) * LANES : (c // 2 + 1) * LANES]
        parts.append(jnp.take_along_axis(from_lanes, index, axis=1))
    evens = jnp.concatenate([jnp.where(even, p, 0.0) for p in parts], axis=1)
    odds = jnp.concatenate([jnp.where(even, 0.0, p) for p in parts], axis=1)
    return split2(jnp.concatenate([evens, odds], axis=0))


def joined(fresh, doubled):
    high, low = split2(fresh)
    up_high, up_low = doubled
    return jnp.concatenate([high, up_high, low, up_low, high, up_high], axis=0)


def fine_kernel(middle, noise, weights, field, zface, yface, carry_z, carry_y):
    count = noise.shape[0]
    cols = noise.shape[3]
    tiles = noise.shape[2] // TILE
    depth_step, row_step = pl.program_id(0), pl.program_id(1)

    @pl.when(depth_step == 0)
    def _():
        carry_z[row_step] = jnp.zeros(carry_z.shape[1:], F32)

    @pl.when(row_step == 0)
    def _():
        carry_y[...] = jnp.zeros_like(carry_y)

    end_row = iota((TILE, cols), 0) == TILE - 1
    edges = [carry_y[0], carry_y[1]]
    for j in reversed(range(tiles)):
        doubled = doubled_columns(middle[0, j], cols)
        above = carry_z[row_step, j]
        for octz in (1, 0):
            fresh = noise[:, octz, j * TILE : (j + 1) * TILE, :].reshape(count * TILE, cols)
            result = dot(weights[octz], joined(fresh, doubled))
            at = 0

            def take(size):
                nonlocal at
                at += size
                return result[at - size : at]

            rows = slice(2 * TILE * j, 2 * TILE * (j + 1))
            for half in range(2):
                field[2 * octz + half, rows] = interleave(take(2 * TILE), take(2 * TILE))
            top = take(4 * TILE) + above
            zface[octz, rows] = interleave(top[: 2 * TILE], top[2 * TILE :])
            above = take(4 * TILE)
            for half in range(2):
                pair = []
                for side in range(2):
                    k = TILE * side + half
                    edge = edges[octz][k : k + 1, :]
                    pair.append(take(TILE) + jnp.where(end_row, edge, 0.0))
                yface[2 * octz + half, TILE * j : TILE * (j + 1)] = interleave(*pair)
            edges[octz] = take(2 * TILE)
        carry_z[row_step, j] = above
    for octz in range(2):
        carry_y[octz] = edges[octz]


def seam_kernel(lower, south, zface, yface, z_out, y_out):
    rows = zface.shape[1] // lower.shape[0]
    for t in range(lower.shape[0]):
        block = lower[t]
        at = slice(t * rows, (t + 1) * rows)
        z_out[0, at] = zface[0, at] + interleave(block[:rows], block[rows:])
    last = yface.shape[1] - 1
    end_row = iota(yface.shape[1:], 0) == last
    for plane in range(south.shape[0]):
        edge = interleave(south[plane, :TILE], south[plane, TILE:])
        for half in range(2):
            y_out[2 * plane + half] = yface[2 * plane + half] + jnp.where(
                end_row, edge[half : half + 1], 0.0
            )


def fine_rows():
    table, index = [], {}

    def entry(point, scale):
        key = (point, scale)
        if key not in index:
            index[key] = len(table)
            table.append(scale * basis_row(point))
        return index[key]

    halves = [-0.5, 0.5]
    rows = []
    for pz in halves:
        for px in halves:
            for y in range(TILE):
                for py in halves:
                    rows.append([(entry((pz, py, px), 1.0), y)])
    for w in (1.0, -1.0):
        for px in halves:
            for y in range(TILE):
                for py in halves:
                    rows.append([(entry((w, py, px), 0.5), y)])
    for pz in halves:
        for px in halves:
            for y in range(TILE):
                terms = [(entry((pz, 1.0, px), 0.5), y)]
                if y + 1 < TILE:
                    terms.append((entry((pz, -1.0, px), 0.5), y + 1))
                rows.append(terms)
    for px in halves:
        for pz in halves:
            rows.append([(entry((pz, -1.0, px), 0.5), 0)])
        rows.extend([[]] * (TILE - 2))
    return np.array(table), rows


def layout_of(rows, count, parent_columns):
    columns = count * TILE + 2 * len(parent_columns)
    place = np.zeros((3, LANES, columns), np.float32)
    at_y = np.zeros((columns,), np.int64)
    for k in range(count):
        for y in range(TILE):
            place[0, k, k * TILE + y] = 1
            at_y[k * TILE + y] = y
    for block in (1, 2):
        for i, (k, y) in enumerate(parent_columns):
            c = count * TILE + (block - 1) * len(parent_columns) + i
            at_y[c] = y
            if k < count:
                place[block, k, c] = 1
    noise = np.arange(columns) < count * TILE
    terms = max(len(r) for r in rows)
    pick = np.zeros((terms, len(rows), LANES), np.float32)
    mask = np.zeros((terms, len(rows), columns), np.float32)
    for term in range(terms):
        for i, row in enumerate(rows):
            if term < len(row):
                q, y = row[term]
                pick[term, i, (y % 2) * (LANES // 2) + q] = 1
                mask[term, i] = np.where(noise, at_y == y, at_y == y // 2)
    return tuple(jnp.asarray(a, BF16) for a in (pick, mask, place.reshape(3 * LANES, columns)))


def shards(n_slab, n_pencil, owner_map, window_start, child_maps, innovation, bank,
           noise_middle, noise_finest):
    count = innovation.shape[0]
    padded = round_up(count, 8)
    total = bank.shape[2]
    owner = owner_map[window_start[0] + LAST]
    smem = pl.BlockSpec(memory_space=pltpu.SMEM)
    vmem = pl.BlockSpec(memory_space=pltpu.VMEM)
    top = Region(LAST, n_slab, n_pencil)
    under = Region(LAST - 1, n_slab, n_pencil)

    rows3 = bank.reshape(count, 1, total)
    head_width = offset_of(LAST) // LANES * LANES + LANES
    head = bank[0, :, :head_width]
    table, row_list = fine_rows()
    half = TILE // 2
    fine_columns = [(k, y) for k in range(count) for y in range(half)]
    fine_parts = layout_of(row_list, count, fine_columns)
    mid_columns = [(k, y) for y in range(half) for k in range(padded)]
    mid_list = [[(k, h * half + y)] for h in range(2) for k in range(count) for y in range(half)]
    mid_parts = layout_of(mid_list, count, mid_columns)
    fine_k, mid_k = fine_parts[1].shape[2], mid_parts[1].shape[2]

    partial, tail, fine_weights, mid_weights, chain_weights = pl.pallas_call(
        functools.partial(head_kernel, n_slab, n_pencil),
        grid=(1,),
        in_specs=[
            smem,
            smem,
            vmem,
            pl.BlockSpec((count, 1, LANES), lambda i: (0, 0, total // LANES)),
        ]
        + [vmem] * 9,
        out_specs=[vmem] * 5,
        out_shape=[
            jax.ShapeDtypeStruct((under.side, padded, under.part), F32),
            jax.ShapeDtypeStruct((count, 1, LANES), F32),
            jax.ShapeDtypeStruct((2, len(row_list), 3 * fine_k), BF16),
            jax.ShapeDtypeStruct((2, len(mid_list), 3 * mid_k), BF16),
            jax.ShapeDtypeStruct((2, padded, 15 * padded), BF16),
        ],
        scratch_shapes=[
            pltpu.VMEM((8, padded, LANES), F32),
            pltpu.VMEM((padded, LANES), F32),
            pltpu.VMEM((padded, head_width), F32),
        ],
        compiler_params=pltpu.CompilerParams(vmem_limit_bytes=20 * MIB),
        name="head",
    )(owner_map, window_start, head, rows3, child_maps.transpose(1, 0, 2), innovation,
      jnp.asarray(np.pad(table, ((0, 0), (0, LANES - count))), F32), *fine_parts, *mid_parts)

    fresh, gathered = lax.switch(
        owner,
        [functools.partial(share, o, n_slab, n_pencil, count) for o in range(n_slab)],
        rows3, tail, partial,
    )

    _, planes, rows, cols = noise_middle.shape
    per = planes // top.nz
    tiles = 2 * rows // TILE
    _, fine_planes, fine_y, fine_x = noise_finest.shape
    out_x = 2 * fine_x
    middle, lower, south = pl.pallas_call(
        functools.partial(middle_kernel, n_slab, n_pencil, per),
        grid=(planes,),
        in_specs=[
            pl.BlockSpec(gathered.shape, lambda z: (0, 0, 0)),
            pl.BlockSpec(fresh.shape, lambda z: (0, 0, 0, 0)),
            pl.BlockSpec((count, 1, rows, cols), lambda z: (0, z, 0, 0)),
            vmem,
            vmem,
            pl.BlockSpec((count, 1, fine_y, fine_x), lambda z: (0, 0, 0, 0)),
            pl.BlockSpec((count, 2, TILE, fine_x), lambda z: (0, z, 0, 0)),
            vmem,
        ],
        out_specs=[
            pl.BlockSpec((1, tiles, count * half, cols), lambda z: (z, 0, 0, 0)),
            pl.BlockSpec((tiles, 4 * TILE, fine_x), lambda z: (0, 0, 0)),
            pl.BlockSpec((2, 2 * TILE, fine_x), lambda z: (z, 0, 0)),
        ],
        out_shape=[
            jax.ShapeDtypeStruct((planes, tiles, count * half, cols), F32),
            jax.ShapeDtypeStruct((tiles, 4 * TILE, fine_x), F32),
            jax.ShapeDtypeStruct((fine_planes, 2 * TILE, fine_x), F32),
        ],
        scratch_shapes=[pltpu.VMEM((top.nz, padded, top.part), F32)],
        compiler_params=pltpu.CompilerParams(vmem_limit_bytes=48 * MIB),
        name="middle",
    )(gathered, fresh, noise_middle, chain_weights, mid_weights, noise_finest, noise_finest,
      fine_weights)
    above = shifted(lower, "slab", -1)
    beside = shifted(south, "pencil", -1)

    deep = 32
    nz, ny = planes, fine_y // deep
    each = deep // TILE

    def block(*where):
        def index(z, y):
            at = {"z": nz - 1 - z, "y": ny - 1 - y}
            return tuple(at.get(w, 0) for w in where)

        return index

    field, zface, yface = pl.pallas_call(
        fine_kernel,
        grid=(nz, ny),
        in_specs=[
            pl.BlockSpec((1, each, count * half, cols), block("z", "y", 0, 0)),
            pl.BlockSpec((count, 2, deep, fine_x), block(0, "z", "y", 0)),
            vmem,
        ],
        out_specs=[
            pl.BlockSpec((4, 2 * deep, out_x), block("z", "y", 0)),
            pl.BlockSpec((2, 2 * deep, out_x), block("z", "y", 0)),
            pl.BlockSpec((4, deep, out_x), block("z", "y", 0)),
        ],
        out_shape=[
            jax.ShapeDtypeStruct((2 * fine_planes, 2 * fine_y, out_x), F32),
            jax.ShapeDtypeStruct((fine_planes, 2 * fine_y, out_x), F32),
            jax.ShapeDtypeStruct((2 * fine_planes, fine_y, out_x), F32),
        ],
        scratch_shapes=[
            pltpu.VMEM((ny, each, 4 * TILE, fine_x), F32),
            pltpu.VMEM((2, 2 * TILE, fine_x), F32),
        ],
        cost_estimate=pl.CostEstimate(
            flops=2 * nz * (fine_y // TILE) * fine_weights.size * fine_x,
            bytes_accessed=4 * (noise_finest.size + 16 * fine_planes * fine_y * fine_x),
            transcendentals=0,
        ),
        compiler_params=pltpu.CompilerParams(vmem_limit_bytes=48 * MIB),
        name="fine",
    )(middle, noise_finest, fine_weights)
    z_spec = pl.BlockSpec((1, 2 * fine_y, out_x), lambda i: (fine_planes - 1, 0, 0))
    y_spec = pl.BlockSpec((2 * fine_planes, TILE, out_x), lambda i: (0, fine_y // TILE - 1, 0))
    zface, yface = pl.pallas_call(
        seam_kernel,
        grid=(1,),
        in_specs=[
            pl.BlockSpec(above.shape, lambda i: (0, 0, 0)),
            pl.BlockSpec(beside.shape, lambda i: (0, 0, 0)),
            z_spec,
            y_spec,
        ],
        out_specs=[z_spec, y_spec],
        out_shape=[
            jax.ShapeDtypeStruct(zface.shape, F32),
            jax.ShapeDtypeStruct(yface.shape, F32),
        ],
        input_output_aliases={2: 0, 3: 1},
        compiler_params=pltpu.CompilerParams(vmem_limit_bytes=8 * MIB),
        name="seam",
    )(above, beside, zface, yface)
    return field, zface, yface


def solution(mesh):
    placed = (
        P(),
        P(),
        P(),
        P(),
        P("slab", None, None),
        P(None, "slab", "pencil", None),
        P(None, "slab", "pencil", None),
    )
    return jax.shard_map(
        functools.partial(shards, mesh.shape["slab"], mesh.shape["pencil"]),
        mesh=mesh,
        in_specs=placed,
        out_specs=(P("slab", "pencil", None), P("slab", "pencil", None), P("slab", "pencil", None)),
        check_vma=False,
    )
```

```python
import functools
import math

import jax
import jax.numpy as jnp
import numpy as np
from jax import lax
from jax.experimental import pallas as pl
from jax.experimental.pallas import tpu as pltpu
from jax.sharding import PartitionSpec as P

LEVELS = 8
ROOTS = 2
BANKS = LEVELS - 2
LAST = BANKS - 1
LANES = 128
TILE = 8
BOTTOM = 12
MIB = 1 << 20
SHARE_FLOPS = 20 * 10**9
SHARE_BYTES = 80 * 10**6
MID_FLOPS = 6 * 10**9
F32 = jnp.float32
BF16 = jnp.bfloat16
MESH = pl.DeviceIdType.MESH


def legendre(order, point):
    values = [1.0, point, 1.5 * point * point - 0.5, 2.5 * point * point * point - 1.5 * point]
    return values[order]


def basis_row(point):
    w_coord, v_coord, u_coord = point
    entry = []
    for deg_x in range(4):
        for deg_y in range(4):
            for deg_z in range(4):
                if deg_x + deg_y + deg_z <= 3:
                    factor = math.sqrt((2 * deg_x + 1) * (2 * deg_y + 1) * (2 * deg_z + 1))
                    entry.append(
                        factor
                        * legendre(deg_x, u_coord)
                        * legendre(deg_y, v_coord)
                        * legendre(deg_z, w_coord)
                    )
    return np.array(entry)


def shifted(block, axis, distance):
    devices = range(lax.axis_size(axis))
    route = [((i - distance) % len(devices), i) for i in devices]
    return lax.ppermute(block, axis, route)


def offset_of(level):
    return ROOTS * (8**level - 1) // 7


def round_up(size, unit):
    return -(-size // unit) * unit


def log2(n):
    return n.bit_length() - 1


class Region:
    def __init__(self, level, n_slab, n_pencil):
        side = 2**level
        self.level = level
        self.side = side
        self.nx = ROOTS * side
        self.ny = side // n_pencil
        self.nz = max(1, side // n_slab)
        self.plane = side * self.nx
        self.part = self.ny * self.nx
        self.n_slab = n_slab

    def first_plane(self, slab):
        return (slab * self.side) // self.n_slab


def split2(value):
    high = value.astype(BF16)
    low = (value - high.astype(F32)).astype(BF16)
    return high, low


def split3(value):
    high, low = split2(value)
    rest = value - high.astype(F32) - low.astype(F32)
    return jnp.concatenate([high.astype(F32), low.astype(F32), rest], axis=0).astype(BF16)


def dot(left, right):
    return jnp.dot(left, right, preferred_element_type=F32)


def exact(left, right):
    left_high, left_low = split2(left)
    right_high, right_low = split2(right)
    return dot(left_high, right_high) + (dot(left_low, right_high) + dot(left_high, right_low))


def chosen(pick, value):
    high, low = split2(value)
    return dot(pick, high) + dot(pick, low)


def placed_at(value, place):
    high, low = split2(value)
    return dot(high, place) + dot(low, place)


def stacked(value):
    high, low = split2(value)
    return jnp.concatenate([high, low, high], axis=0)


def picked(parent, pick):
    rows = parent.shape[0]
    up = dot(split3(parent), pick)
    return up[:rows] + up[rows : 2 * rows] + up[2 * rows :]


def spread(up, octant, names):
    return [jnp.where(octant == o, up, 0.0) for o in names]


def iota(shape, dim):
    return lax.broadcasted_iota(jnp.int32, shape, dim)


def deepened(value, rows):
    return jnp.concatenate(
        [value, jnp.zeros((rows - value.shape[0], value.shape[1]), F32)], axis=0
    )


def weave(table_terms, mask, place, table, innovation, maps, octz):
    both = []
    for octy in range(2):
        o = 4 * octz + 2 * octy
        wide = placed_at(jnp.concatenate([innovation, maps[o], maps[o + 1]], axis=1), place[...])
        if table is not None:
            wide = exact(table, deepened(wide, LANES))
        both.append(deepened(wide, LANES // 2))
    both = jnp.concatenate(both, axis=0)
    total = 0.0
    for term in range(table_terms.shape[0]):
        total = total + chosen(table_terms[term], both) * mask[term].astype(F32)
    high, low = split2(total)
    return jnp.concatenate([high, high, low], axis=1)


def head_kernel(n_slab, n_pencil, owner_map, window_start, bank, end, child_maps, innovation,
                table, fine_rows, fine_mask, fine_place, mid_rows, mid_mask, mid_place,
                partial, tail, fine_w, mid_w, chain_w, maps, inner, head):
    rows = head.shape[0]
    count = innovation.shape[0]
    head[count // 8 * 8 :, :] = jnp.zeros((rows - count // 8 * 8, head.shape[1]), F32)
    head[:count, :] = bank[...]
    slab, pencil = lax.axis_index("slab"), lax.axis_index("pencil")

    def owned(level):
        return owner_map[window_start[0] + level] == slab

    tail[...] = end[...]
    maps[...] = jnp.zeros_like(maps)
    inner[...] = jnp.zeros_like(inner)
    for o in range(8):
        maps[o, :count, :count] = child_maps[:, o, :]
    inner[:count, :count] = innovation[...]
    quad = 4 * rows
    blocks = []
    for octz in range(2):
        block = 0.0
        for o in range(4):
            block = block + pltpu.roll(maps[4 * octz + o], o * rows, 1)
        blocks.append(block[:, :quad])
    flat = jnp.concatenate(blocks + [inner[:, :rows]], axis=1)
    w_high, w_low = split2(flat)
    w_all = jnp.concatenate([w_high, w_high, w_low], axis=1)
    lane = iota((rows, LANES), 1)
    last = LAST - 1

    def unshifted(at, shift):
        if shift == 0:
            return head[:, pl.ds(at, LANES)]
        left = pltpu.roll(head[:, pl.ds(at, LANES)], LANES - shift, 1)
        right = pltpu.roll(head[:, pl.ds(at + LANES, LANES)], LANES - shift, 1)
        return jnp.where(lane < LANES - shift, left, right)

    parent = None
    for level in range(last):
        side, nx = 2**level, ROOTS * 2**level
        cells = side * side * nx
        padded = round_up(cells, LANES)
        first = offset_of(level)
        shift = first % LANES
        noise = jnp.concatenate(
            [unshifted(first - shift + t * LANES, shift) for t in range(padded // LANES)], axis=1
        )
        noise = jnp.where(owned(level), noise, 0.0)
        if cells < padded:
            noise = jnp.where(iota((rows, padded), 1) < cells, noise, 0.0)
        if parent is None:
            up = jnp.zeros((rows, padded), F32)
        else:
            q = parent.shape[1]
            half = nx // 2

            def source_of(shape):
                cell = iota(shape, 1)
                x = cell & (nx - 1)
                y = (cell >> log2(nx)) & (side - 1)
                z = cell >> log2(nx * side)
                return x, y, z

            x, y, z = source_of((q, padded))
            source = ((z >> 1) * (side // 2) + (y >> 1)) * half + (x >> 1)
            pick = jnp.where(iota((q, padded), 0) == source, 1.0, 0.0).astype(BF16)
            up = picked(parent, pick)
        cell = iota((rows, padded), 1)
        octant = (
            4 * ((cell >> log2(nx * side)) & 1) + 2 * ((cell >> log2(nx)) & 1) + (cell & 1)
        )
        stack = jnp.concatenate(spread(up, octant, range(8)) + [noise], axis=0)
        parent = dot(w_all, stacked(stack))[:rows]

    r = Region(last, n_slab, n_pencil)
    half = r.nx // 2
    plane = (r.side // 2) * half
    cell = iota((plane, r.part), 1)
    y = (cell >> log2(r.nx)) + pencil * r.ny
    source = (y >> 1) * half + ((cell & (r.nx - 1)) >> 1)
    pick = jnp.where(iota((plane, r.part), 0) == source, 1.0, 0.0).astype(BF16)
    pieces = [split3(parent[:, z * plane : (z + 1) * plane]) for z in range(r.side // 2)]
    ups = dot(jnp.concatenate(pieces, axis=0), pick)
    cell = iota((rows, r.part), 1)
    octant = 2 * ((cell >> log2(r.nx)) & 1) + (cell & 1)
    first = offset_of(last)
    shift = first % LANES
    for octz in range(2):
        w = jnp.concatenate([blocks[octz], inner[:, :rows]], axis=1)
        high, low = split2(w)
        chain_w[octz] = jnp.concatenate([high, high, low], axis=1)
    for z in range(r.side):
        at = (z // 2) * 3 * rows
        up = ups[at : at + rows] + ups[at + rows : at + 2 * rows] + ups[at + 2 * rows : at + 3 * rows]
        start = first - shift + z * r.plane
        noise = jnp.concatenate(
            [
                unshifted(pl.multiple_of(start + pencil * r.part + t * LANES, LANES), shift)
                for t in range(r.part // LANES)
            ],
            axis=1,
        )
        noise = jnp.where(owned(last), noise, 0.0)
        stack = jnp.concatenate(spread(up, octant, range(4)) + [noise], axis=0)
        partial[z] = dot(chain_w[z % 2], stacked(stack))[:rows]

    for octz in range(2):
        fine_w[octz] = weave(fine_rows, fine_mask, fine_place, table[...], inner[...], maps, octz)
        mid_w[octz] = weave(mid_rows, mid_mask, mid_place, None, inner[...], maps, octz)


def routes(owner, n_slab):
    inner = 4
    others = [d for d in range(n_slab) if d != owner]
    if n_slab != inner * inner:
        return {d: None for d in others}
    own_z, own_p = divmod(owner, inner)

    def link(dest):
        z, p = divmod(dest, inner)
        if z != own_z:
            return "up" if z > own_z else "down"
        return "x" if (p ^ own_p) & 1 else "y"

    def options(dest):
        p = dest % inner
        found = [(None, link(dest))]
        for bit, name in ((1, "x"), (2, "y")):
            relay = own_z * inner + (own_p ^ bit)
            if relay != dest and (p ^ own_p) & bit:
                found.append((relay, name))
        return found

    load, via = {}, {}
    for d in others:
        load[link(d)] = load.get(link(d), 0) + 0.13
    for d in sorted(others, key=lambda d: (len(options(d)), d)):
        relay, name = min(
            options(d), key=lambda t: load.get(t[1], 0) + (0 if t[0] is None else 0.01)
        )
        load[name] = load.get(name, 0) + 1
        via[d] = relay
    return via


def share_kernel(owner, n_slab, n_pencil, bank, tail, partial, fresh, gathered, relay,
                 send, recv, own, to_relay, onward, give, take, keep):
    r = Region(LAST, n_slab, n_pencil)
    r4 = Region(LAST - 1, n_slab, n_pencil)
    me, pencil = lax.axis_index("slab"), lax.axis_index("pencil")
    base = offset_of(LAST) // LANES * LANES
    via = routes(owner, n_slab)
    relayed = [d for d in via if via[d] is not None]
    direct = [d for d in via if via[d] is None]
    slots = {}
    for d in relayed:
        slots[d] = sum(1 for e in slots if via[e] == via[d])

    def at(d):
        return {"slab": d}

    barrier = pltpu.get_barrier_semaphore()

    def greet(i, _):
        pl.semaphore_signal(
            barrier, inc=1, device_id=at(lax.rem(me + i, n_slab)), device_id_type=MESH
        )
        return 0

    lax.fori_loop(1, n_slab, greet, 0)
    pl.semaphore_wait(barrier, n_slab - 1)

    def source(d, z):
        start = base + (r.first_plane(d) + z) * r.plane + pencil * r.part
        return bank.at[:, :, pl.ds(pl.multiple_of(start, LANES), r.part)]

    def beyond(d, z, act):
        plane = r.first_plane(d) + z
        start = base + plane * r.plane + (pencil + 1) * r.part
        inside = bank.at[:, :, pl.ds(pl.multiple_of(start, LANES), LANES)]
        if isinstance(d, int) and plane < r.side - 1:
            act(inside)
            return
        ends = jnp.logical_and(plane == r.side - 1, pencil == n_pencil - 1)
        pl.when(ends)(lambda: act(tail))
        pl.when(jnp.logical_not(ends))(lambda: act(inside))

    def body(ref):
        return ref.at[:, :, pl.ds(0, r.part)]

    def rest(ref):
        return ref.at[:, :, pl.ds(r.part, LANES)]

    def remote(src, dst, ssem, rsem, d):
        return pltpu.make_async_remote_copy(
            src, dst, ssem, rsem, device_id=at(d), device_id_type=MESH
        )

    def start_block(d, z):
        if isinstance(d, int) and via[d] is not None:
            dst, rsem, to = relay.at[slots[d], z], to_relay.at[slots[d], z], via[d]
        else:
            dst, rsem, to = fresh.at[z], recv.at[z], d
        remote(source(d, z), body(dst), send.at[d, z, 0], rsem.at[0], to).start()
        beyond(d, z, lambda src: remote(src, rest(dst), send.at[d, z, 1], rsem.at[1], to).start())

    def drain_block(d, z):
        remote(source(d, z), body(fresh.at[z]), send.at[d, z, 0], recv.at[z, 0], d).wait_send()
        remote(tail, rest(fresh.at[z]), send.at[d, z, 1], recv.at[z, 1], d).wait_send()

    def landed(dst, rsem, d):
        remote(source(0, 0), body(dst), send.at[0, 0, 0], rsem.at[0], d).wait_recv()
        remote(tail, rest(dst), send.at[0, 0, 1], rsem.at[1], d).wait_recv()

    def forward(d, z):
        return remote(relay.at[slots[d], z], fresh.at[z], onward.at[slots[d], z], recv.at[z, 2], d)

    @pl.when(me == owner)
    def _():
        if relayed:
            for d in relayed + direct:
                for z in range(r.nz):
                    start_block(d, z)
        else:

            def step(i, _):
                for z in range(r.nz):
                    start_block(lax.rem(owner + i, n_slab), z)
                return 0

            lax.fori_loop(1, n_slab, step, 0)
        for z in range(r.nz):
            pltpu.make_async_copy(source(owner, z), body(fresh.at[z]), own.at[z, 0]).start()
            beyond(
                owner,
                z,
                lambda src: pltpu.make_async_copy(src, rest(fresh.at[z]), own.at[z, 1]).start(),
            )

    def piece(d):
        return partial.at[r4.first_plane(d)]

    def give_one(i, _):
        d = lax.rem(me + i, n_slab)
        remote(piece(d), gathered.at[me], give.at[d], take.at[me], d).start()
        return 0

    lax.fori_loop(1, n_slab, give_one, 0)
    mine = pltpu.make_async_copy(piece(me), gathered.at[me], keep)
    mine.start()

    for hub in sorted({via[d] for d in relayed}):

        @pl.when(me == hub)
        def _():
            group = [d for d in relayed if via[d] == hub]
            for d in group:
                for z in range(r.nz):
                    landed(relay.at[slots[d], z], to_relay.at[slots[d], z], owner)
                    forward(d, z).start()
            for d in group:
                for z in range(r.nz):
                    forward(d, z).wait_send()

    through = functools.reduce(jnp.logical_or, [me == d for d in relayed], False)

    @pl.when(jnp.logical_and(me != owner, jnp.logical_not(through)))
    def _():
        for z in range(r.nz):
            landed(fresh.at[z], recv.at[z], owner)

    if relayed:

        @pl.when(through)
        def _():
            for z in range(r.nz):
                remote(relay.at[0, z], fresh.at[z], onward.at[0, z], recv.at[z, 2], owner).wait_recv()

    @pl.when(me == owner)
    def _():
        if relayed:
            for d in relayed + direct:
                for z in range(r.nz):
                    drain_block(d, z)
        else:

            def step(i, _):
                for z in range(r.nz):
                    drain_block(lax.rem(owner + i, n_slab), z)
                return 0

            lax.fori_loop(1, n_slab, step, 0)
        for z in range(r.nz):
            pltpu.make_async_copy(source(owner, z), body(fresh.at[z]), own.at[z, 0]).wait()
            pltpu.make_async_copy(tail, rest(fresh.at[z]), own.at[z, 1]).wait()

    def take_one(i, _):
        d = lax.rem(me + i, n_slab)
        remote(piece(d), gathered.at[d], give.at[d], take.at[d], d).wait()
        return 0

    lax.fori_loop(1, n_slab, take_one, 0)
    mine.wait()


def share(owner, n_slab, n_pencil, count, bank, tail, partial):
    r = Region(LAST, n_slab, n_pencil)
    block = (r.nz, count, 1, r.part + LANES)
    via = routes(owner, n_slab)
    hubs = [v for v in via.values() if v is not None]
    slots = max([hubs.count(h) for h in hubs], default=1)
    dma = pltpu.SemaphoreType.DMA
    anywhere = pl.BlockSpec(memory_space=pl.ANY)
    return pl.pallas_call(
        functools.partial(share_kernel, owner, n_slab, n_pencil),
        in_specs=[anywhere] * 3,
        out_specs=[anywhere] * 2,
        out_shape=[
            jax.ShapeDtypeStruct(block, F32),
            jax.ShapeDtypeStruct((n_slab, *partial.shape[1:]), F32),
        ],
        scratch_shapes=[
            pltpu.VMEM((slots, *block), F32),
            dma((n_slab, r.nz, 2)),
            dma((r.nz, 3)),
            dma((r.nz, 2)),
            dma((slots, r.nz, 2)),
            dma((slots, r.nz)),
            dma((n_slab,)),
            dma((n_slab,)),
            dma,
        ],
        cost_estimate=pl.CostEstimate(
            flops=SHARE_FLOPS, bytes_accessed=SHARE_BYTES, transcendentals=0
        ),
        compiler_params=pltpu.CompilerParams(
            collective_id=owner, has_side_effects=True, vmem_limit_bytes=8 * MIB
        ),
        name="share",
    )(bank, tail, partial)


def middle_kernel(n_slab, n_pencil, per, gathered, fresh, noise, chain_w, weights,
                  fine_plane, fine_row, fine_w, out, lower, south, last_coarse):
    r = Region(LAST, n_slab, n_pencil)
    q = Region(LAST - 1, n_slab, n_pencil)
    rows = gathered.shape[1]
    count = noise.shape[0]
    step = pl.program_id(0)
    slab = lax.axis_index("slab")

    @pl.when(step == 0)
    def _():
        parent = gathered[0]
        for d in range(1, gathered.shape[0]):
            parent = parent + gathered[d]
        cell = iota((q.part, r.part), 1)
        source = (cell >> (log2(r.nx) + 1)) * q.nx + ((cell & (r.nx - 1)) >> 1)
        pick = jnp.where(iota((q.part, r.part), 0) == source, 1.0, 0.0).astype(BF16)
        up = picked(parent, pick)
        cell = iota((rows, r.part), 1)
        octant = 2 * ((cell >> log2(r.nx)) & 1) + (cell & 1)
        spreads = spread(up, octant, range(4))
        shift = offset_of(LAST) % LANES
        lane = iota((count, LANES), 1)
        for z in range(r.nz):
            raw = fresh[z, :, 0, :]
            rolled = [
                pltpu.roll(raw[:, t * LANES : (t + 1) * LANES], LANES - shift, 1)
                for t in range(r.part // LANES + 1)
            ]
            block = jnp.concatenate(
                [
                    jnp.where(lane < LANES - shift, rolled[t], rolled[t + 1])
                    for t in range(r.part // LANES)
                ],
                axis=1,
            )
            last_coarse[z] = jnp.zeros_like(last_coarse[z])
            last_coarse[z, :count, :] = block
            stack = jnp.concatenate(spreads + [last_coarse[z]], axis=0)
            octz = (r.first_plane(slab) + z) & 1
            last_coarse[z] = dot(chain_w[octz], stacked(stack))[:rows]

    octz = lax.rem(slab * per * r.nz + step, 2)
    at = step // per
    wide = noise.shape[3]
    lane = iota((rows, LANES), 1)
    even = (lane & 1) == 0
    half = TILE // 2
    across = LANES // r.nx

    def parents(t):
        pieces = []
        for yy in range(half):
            y = t * half + yy
            cells = last_coarse[at, :, (y // across) * LANES : (y // across + 1) * LANES]
            index = (y % across) * r.nx + (lane >> 1)
            pieces.append(jnp.take_along_axis(cells, index, axis=1))
        return [jnp.where(even, p, 0.0) for p in pieces] + [jnp.where(even, 0.0, p) for p in pieces]

    group = 2
    for j in range(noise.shape[2] // (TILE * group)):
        columns = []
        for g in range(group):
            t = j * group + g
            fresh_part = noise[:, 0, t * TILE : (t + 1) * TILE, :].reshape(count * TILE, wide)
            columns.append(jnp.concatenate([fresh_part] + parents(t), axis=0))
        result = dot(weights[octz], stacked(jnp.concatenate(columns, axis=1)))
        size = count * half
        for g in range(group):
            for h in range(2):
                out[0, (j * group + g) * 2 + h] = result[
                    h * size : (h + 1) * size, g * wide : (g + 1) * wide
                ]

    cols = fine_row.shape[3]
    edges = 2 * TILE
    ends = fine_w.shape[1]
    doubled = doubled_columns(out[0, 0], cols)
    for octz in range(2):
        fresh_part = fine_row[:, octz].reshape(count * TILE, cols)
        south[octz] = dot(fine_w[octz, ends - edges :], joined(fresh_part, doubled))

    @pl.when(step == 0)
    def _():
        for t in range(out.shape[1]):
            fresh_part = fine_plane[:, 0, t * TILE : (t + 1) * TILE, :].reshape(count * TILE, cols)
            lower[t] = dot(
                fine_w[0, BOTTOM * TILE : (BOTTOM + 4) * TILE],
                joined(fresh_part, doubled_columns(out[0, t], cols)),
            )


def interleave(even, odd):
    rows, cols = even.shape
    lane = iota((rows, LANES), 1)
    half = LANES // 2
    first = lane < half
    index = (lane >> 1) + (lane & 1) * half
    parts = []
    for j in range(cols // LANES):
        a = even[:, j * LANES : (j + 1) * LANES]
        b = odd[:, j * LANES : (j + 1) * LANES]
        left = jnp.where(first, a, pltpu.roll(b, half, 1))
        right = jnp.where(first, pltpu.roll(a, half, 1), b)
        parts.append(jnp.take_along_axis(left, index, axis=1))
        parts.append(jnp.take_along_axis(right, index, axis=1))
    return jnp.concatenate(parts, axis=1)


def doubled_columns(parent, cols):
    rows = parent.shape[0]
    lane = iota((rows, LANES), 1)
    even = (lane & 1) == 0
    parts = []
    for c in range(cols // LANES):
        index = (c % 2) * (LANES // 2) + (lane >> 1)
        from_lanes = parent[:, (c // 2) * LANES : (c // 2 + 1) * LANES]
        parts.append(jnp.take_along_axis(from_lanes, index, axis=1))
    evens = jnp.concatenate([jnp.where(even, p, 0.0) for p in parts], axis=1)
    odds = jnp.concatenate([jnp.where(even, 0.0, p) for p in parts], axis=1)
    return split2(jnp.concatenate([evens, odds], axis=0))


def joined(fresh, doubled):
    high, low = split2(fresh)
    up_high, up_low = doubled
    return jnp.concatenate([high, up_high, low, up_low, high, up_high], axis=0)


def fine_kernel(middle, noise, weights, field, zface, yface, carry_z, carry_y):
    count = noise.shape[0]
    cols = noise.shape[3]
    tiles = noise.shape[2] // TILE
    depth_step, row_step = pl.program_id(0), pl.program_id(1)

    @pl.when(depth_step == 0)
    def _():
        carry_z[row_step] = jnp.zeros(carry_z.shape[1:], F32)

    @pl.when(row_step == 0)
    def _():
        carry_y[...] = jnp.zeros_like(carry_y)

    end_row = iota((TILE, cols), 0) == TILE - 1
    edges = [carry_y[0], carry_y[1]]
    for j in reversed(range(tiles)):
        doubled = doubled_columns(middle[0, j], cols)
        above = carry_z[row_step, j]
        for octz in (1, 0):
            fresh = noise[:, octz, j * TILE : (j + 1) * TILE, :].reshape(count * TILE, cols)
            result = dot(weights[octz], joined(fresh, doubled))
            at = 0

            def take(size):
                nonlocal at
                at += size
                return result[at - size : at]

            rows = slice(2 * TILE * j, 2 * TILE * (j + 1))
            for half in range(2):
                field[2 * octz + half, rows] = interleave(take(2 * TILE), take(2 * TILE))
            top = take(4 * TILE) + above
            zface[octz, rows] = interleave(top[: 2 * TILE], top[2 * TILE :])
            above = take(4 * TILE)
            for half in range(2):
                pair = []
                for side in range(2):
                    k = TILE * side + half
                    edge = edges[octz][k : k + 1, :]
                    pair.append(take(TILE) + jnp.where(end_row, edge, 0.0))
                yface[2 * octz + half, TILE * j : TILE * (j + 1)] = interleave(*pair)
            edges[octz] = take(2 * TILE)
        carry_z[row_step, j] = above
    for octz in range(2):
        carry_y[octz] = edges[octz]


def seam_kernel(lower, south, zface, yface, z_out, y_out):
    rows = zface.shape[1] // lower.shape[0]
    for t in range(lower.shape[0]):
        block = lower[t]
        at = slice(t * rows, (t + 1) * rows)
        z_out[0, at] = zface[0, at] + interleave(block[:rows], block[rows:])
    last = yface.shape[1] - 1
    end_row = iota(yface.shape[1:], 0) == last
    for plane in range(south.shape[0]):
        edge = interleave(south[plane, :TILE], south[plane, TILE:])
        for half in range(2):
            y_out[2 * plane + half] = yface[2 * plane + half] + jnp.where(
                end_row, edge[half : half + 1], 0.0
            )


def fine_rows():
    table, index = [], {}

    def entry(point, scale):
        key = (point, scale)
        if key not in index:
            index[key] = len(table)
            table.append(scale * basis_row(point))
        return index[key]

    halves = [-0.5, 0.5]
    rows = []
    for pz in halves:
        for px in halves:
            for y in range(TILE):
                for py in halves:
                    rows.append([(entry((pz, py, px), 1.0), y)])
    for w in (1.0, -1.0):
        for px in halves:
            for y in range(TILE):
                for py in halves:
                    rows.append([(entry((w, py, px), 0.5), y)])
    for pz in halves:
        for px in halves:
            for y in range(TILE):
                terms = [(entry((pz, 1.0, px), 0.5), y)]
                if y + 1 < TILE:
                    terms.append((entry((pz, -1.0, px), 0.5), y + 1))
                rows.append(terms)
    for px in halves:
        for pz in halves:
            rows.append([(entry((pz, -1.0, px), 0.5), 0)])
        rows.extend([[]] * (TILE - 2))
    return np.array(table), rows


def layout_of(rows, count, parent_columns):
    columns = count * TILE + 2 * len(parent_columns)
    place = np.zeros((3, LANES, columns), np.float32)
    at_y = np.zeros((columns,), np.int64)
    for k in range(count):
        for y in range(TILE):
            place[0, k, k * TILE + y] = 1
            at_y[k * TILE + y] = y
    for block in (1, 2):
        for i, (k, y) in enumerate(parent_columns):
            c = count * TILE + (block - 1) * len(parent_columns) + i
            at_y[c] = y
            if k < count:
                place[block, k, c] = 1
    noise = np.arange(columns) < count * TILE
    terms = max(len(r) for r in rows)
    pick = np.zeros((terms, len(rows), LANES), np.float32)
    mask = np.zeros((terms, len(rows), columns), np.float32)
    for term in range(terms):
        for i, row in enumerate(rows):
            if term < len(row):
                q, y = row[term]
                pick[term, i, (y % 2) * (LANES // 2) + q] = 1
                mask[term, i] = np.where(noise, at_y == y, at_y == y // 2)
    return tuple(jnp.asarray(a, BF16) for a in (pick, mask, place.reshape(3 * LANES, columns)))


def shards(n_slab, n_pencil, owner_map, window_start, child_maps, innovation, bank,
           noise_middle, noise_finest):
    count = innovation.shape[0]
    padded = round_up(count, 8)
    total = bank.shape[2]
    owner = owner_map[window_start[0] + LAST]
    smem = pl.BlockSpec(memory_space=pltpu.SMEM)
    vmem = pl.BlockSpec(memory_space=pltpu.VMEM)
    top = Region(LAST, n_slab, n_pencil)
    under = Region(LAST - 1, n_slab, n_pencil)

    rows3 = bank.reshape(count, 1, total)
    head_width = offset_of(LAST) // LANES * LANES + LANES
    head = bank[0, :, :head_width]
    table, row_list = fine_rows()
    half = TILE // 2
    fine_columns = [(k, y) for k in range(count) for y in range(half)]
    fine_parts = layout_of(row_list, count, fine_columns)
    mid_columns = [(k, y) for y in range(half) for k in range(padded)]
    mid_list = [[(k, h * half + y)] for h in range(2) for k in range(count) for y in range(half)]
    mid_parts = layout_of(mid_list, count, mid_columns)
    fine_k, mid_k = fine_parts[1].shape[2], mid_parts[1].shape[2]

    partial, tail, fine_weights, mid_weights, chain_weights = pl.pallas_call(
        functools.partial(head_kernel, n_slab, n_pencil),
        grid=(1,),
        in_specs=[
            smem,
            smem,
            vmem,
            pl.BlockSpec((count, 1, LANES), lambda i: (0, 0, total // LANES)),
        ]
        + [vmem] * 9,
        out_specs=[vmem] * 5,
        out_shape=[
            jax.ShapeDtypeStruct((under.side, padded, under.part), F32),
            jax.ShapeDtypeStruct((count, 1, LANES), F32),
            jax.ShapeDtypeStruct((2, len(row_list), 3 * fine_k), BF16),
            jax.ShapeDtypeStruct((2, len(mid_list), 3 * mid_k), BF16),
            jax.ShapeDtypeStruct((2, padded, 15 * padded), BF16),
        ],
        scratch_shapes=[
            pltpu.VMEM((8, padded, LANES), F32),
            pltpu.VMEM((padded, LANES), F32),
            pltpu.VMEM((padded, head_width), F32),
        ],
        compiler_params=pltpu.CompilerParams(vmem_limit_bytes=20 * MIB),
        name="head",
    )(owner_map, window_start, head, rows3, child_maps.transpose(1, 0, 2), innovation,
      jnp.asarray(np.pad(table, ((0, 0), (0, LANES - count))), F32), *fine_parts, *mid_parts)

    fresh, gathered = lax.switch(
        owner,
        [functools.partial(share, o, n_slab, n_pencil, count) for o in range(n_slab)],
        rows3, tail, partial,
    )

    _, planes, rows, cols = noise_middle.shape
    per = planes // top.nz
    tiles = 2 * rows // TILE
    _, fine_planes, fine_y, fine_x = noise_finest.shape
    out_x = 2 * fine_x
    in_hbm = pltpu.with_memory_space_constraint(noise_finest, pltpu.HBM)
    middle, lower, south = pl.pallas_call(
        functools.partial(middle_kernel, n_slab, n_pencil, per),
        grid=(planes,),
        in_specs=[
            pl.BlockSpec(gathered.shape, lambda z: (0, 0, 0)),
            pl.BlockSpec(fresh.shape, lambda z: (0, 0, 0, 0)),
            pl.BlockSpec((count, 1, rows, cols), lambda z: (0, z, 0, 0)),
            vmem,
            vmem,
            pl.BlockSpec((count, 1, fine_y, fine_x), lambda z: (0, 0, 0, 0)),
            pl.BlockSpec((count, 2, TILE, fine_x), lambda z: (0, z, 0, 0)),
            vmem,
        ],
        out_specs=[
            pl.BlockSpec((1, tiles, count * half, cols), lambda z: (z, 0, 0, 0)),
            pl.BlockSpec((tiles, 4 * TILE, fine_x), lambda z: (0, 0, 0)),
            pl.BlockSpec((2, 2 * TILE, fine_x), lambda z: (z, 0, 0)),
        ],
        out_shape=[
            jax.ShapeDtypeStruct((planes, tiles, count * half, cols), F32),
            jax.ShapeDtypeStruct((tiles, 4 * TILE, fine_x), F32),
            jax.ShapeDtypeStruct((fine_planes, 2 * TILE, fine_x), F32),
        ],
        scratch_shapes=[pltpu.VMEM((top.nz, padded, top.part), F32)],
        cost_estimate=pl.CostEstimate(
            flops=MID_FLOPS, bytes_accessed=4 * noise_middle.size, transcendentals=0
        ),
        compiler_params=pltpu.CompilerParams(vmem_limit_bytes=24 * MIB),
        name="middle",
    )(gathered, fresh, noise_middle, chain_weights, mid_weights, in_hbm, in_hbm,
      fine_weights)
    above = shifted(lower, "slab", -1)
    beside = shifted(south, "pencil", -1)

    deep = 64
    nz, ny = planes, fine_y // deep
    each = deep // TILE

    def block(*where):
        def index(z, y):
            at = {"z": nz - 1 - z, "y": ny - 1 - y}
            return tuple(at.get(w, 0) for w in where)

        return index

    field, zface, yface = pl.pallas_call(
        fine_kernel,
        grid=(nz, ny),
        in_specs=[
            pl.BlockSpec((1, each, count * half, cols), block("z", "y", 0, 0)),
            pl.BlockSpec((count, 2, deep, fine_x), block(0, "z", "y", 0)),
            vmem,
        ],
        out_specs=[
            pl.BlockSpec((4, 2 * deep, out_x), block("z", "y", 0)),
            pl.BlockSpec((2, 2 * deep, out_x), block("z", "y", 0)),
            pl.BlockSpec((4, deep, out_x), block("z", "y", 0)),
        ],
        out_shape=[
            jax.ShapeDtypeStruct((2 * fine_planes, 2 * fine_y, out_x), F32),
            jax.ShapeDtypeStruct((fine_planes, 2 * fine_y, out_x), F32),
            jax.ShapeDtypeStruct((2 * fine_planes, fine_y, out_x), F32),
        ],
        scratch_shapes=[
            pltpu.VMEM((ny, each, 4 * TILE, fine_x), F32),
            pltpu.VMEM((2, 2 * TILE, fine_x), F32),
        ],
        cost_estimate=pl.CostEstimate(
            flops=2 * nz * (fine_y // TILE) * fine_weights.size * fine_x,
            bytes_accessed=4 * (noise_finest.size + 16 * fine_planes * fine_y * fine_x),
            transcendentals=0,
        ),
        compiler_params=pltpu.CompilerParams(vmem_limit_bytes=24 * MIB),
        name="fine",
    )(middle, noise_finest, fine_weights)
    z_spec = pl.BlockSpec((1, 2 * fine_y, out_x), lambda i: (fine_planes - 1, 0, 0))
    y_spec = pl.BlockSpec((2 * fine_planes, TILE, out_x), lambda i: (0, fine_y // TILE - 1, 0))
    zface, yface = pl.pallas_call(
        seam_kernel,
        grid=(1,),
        in_specs=[
            pl.BlockSpec(above.shape, lambda i: (0, 0, 0)),
            pl.BlockSpec(beside.shape, lambda i: (0, 0, 0)),
            z_spec,
            y_spec,
        ],
        out_specs=[z_spec, y_spec],
        out_shape=[
            jax.ShapeDtypeStruct(zface.shape, F32),
            jax.ShapeDtypeStruct(yface.shape, F32),
        ],
        input_output_aliases={2: 0, 3: 1},
        compiler_params=pltpu.CompilerParams(vmem_limit_bytes=8 * MIB),
        name="seam",
    )(above, beside, zface, yface)
    return field, zface, yface


def solution(mesh):
    placed = (
        P(),
        P(),
        P(),
        P(),
        P("slab", None, None),
        P(None, "slab", "pencil", None),
        P(None, "slab", "pencil", None),
    )
    return jax.shard_map(
        functools.partial(shards, mesh.shape["slab"], mesh.shape["pencil"]),
        mesh=mesh,
        in_specs=placed,
        out_specs=(P("slab", "pencil", None), P("slab", "pencil", None), P("slab", "pencil", None)),
        check_vma=False,
    )
```

```python
import functools
import math

import jax
import jax.numpy as jnp
import numpy as np
from jax import lax
from jax.experimental import pallas as pl
from jax.experimental.pallas import tpu as pltpu
from jax.sharding import PartitionSpec as P

LEVELS = 8
ROOTS = 2
BANKS = LEVELS - 2
LAST = BANKS - 1
LANES = 128
TILE = 8
BOTTOM = 12
MIB = 1 << 20
SHARE_FLOPS = 20 * 10**9
SHARE_BYTES = 80 * 10**6
MID_FLOPS = 6 * 10**9
F32 = jnp.float32
BF16 = jnp.bfloat16
MESH = pl.DeviceIdType.MESH


def legendre(order, point):
    values = [1.0, point, 1.5 * point * point - 0.5, 2.5 * point * point * point - 1.5 * point]
    return values[order]


def basis_row(point):
    w_coord, v_coord, u_coord = point
    entry = []
    for deg_x in range(4):
        for deg_y in range(4):
            for deg_z in range(4):
                if deg_x + deg_y + deg_z <= 3:
                    factor = math.sqrt((2 * deg_x + 1) * (2 * deg_y + 1) * (2 * deg_z + 1))
                    entry.append(
                        factor
                        * legendre(deg_x, u_coord)
                        * legendre(deg_y, v_coord)
                        * legendre(deg_z, w_coord)
                    )
    return np.array(entry)


def shifted(block, axis, distance):
    devices = range(lax.axis_size(axis))
    route = [((i - distance) % len(devices), i) for i in devices]
    return lax.ppermute(block, axis, route)


def offset_of(level):
    return ROOTS * (8**level - 1) // 7


def round_up(size, unit):
    return -(-size // unit) * unit


def log2(n):
    return n.bit_length() - 1


class Region:
    def __init__(self, level, n_slab, n_pencil):
        side = 2**level
        self.level = level
        self.side = side
        self.nx = ROOTS * side
        self.ny = side // n_pencil
        self.nz = max(1, side // n_slab)
        self.plane = side * self.nx
        self.part = self.ny * self.nx
        self.n_slab = n_slab

    def first_plane(self, slab):
        return (slab * self.side) // self.n_slab


def split2(value):
    high = value.astype(BF16)
    low = (value - high.astype(F32)).astype(BF16)
    return high, low


def split3(value):
    high, low = split2(value)
    rest = value - high.astype(F32) - low.astype(F32)
    return jnp.concatenate([high.astype(F32), low.astype(F32), rest], axis=0).astype(BF16)


def dot(left, right):
    return jnp.dot(left, right, preferred_element_type=F32)


def exact(left, right):
    left_high, left_low = split2(left)
    right_high, right_low = split2(right)
    return dot(left_high, right_high) + (dot(left_low, right_high) + dot(left_high, right_low))


def chosen(pick, value):
    high, low = split2(value)
    return dot(pick, high) + dot(pick, low)


def placed_at(value, place):
    high, low = split2(value)
    return dot(high, place) + dot(low, place)


def stacked(value):
    high, low = split2(value)
    return jnp.concatenate([high, low, high], axis=0)


def picked(parent, pick):
    rows = parent.shape[0]
    up = dot(split3(parent), pick)
    return up[:rows] + up[rows : 2 * rows] + up[2 * rows :]


def spread(up, octant, names):
    return [jnp.where(octant == o, up, 0.0) for o in names]


def iota(shape, dim):
    return lax.broadcasted_iota(jnp.int32, shape, dim)


def packed(value, count):
    full, short = count // 8 * 8, count % 8
    tiles = [value[:, t * LANES : (t + 1) * LANES] for t in range(value.shape[1] // LANES)]
    if not 0 < short <= 4:
        return jnp.concatenate(tiles, axis=0)
    row = iota((8, LANES), 0)
    ends = [
        jnp.where(row < 4, a[full:], pltpu.roll(b[full:], 4, 0))
        for a, b in zip(tiles[::2], tiles[1::2])
    ]
    return jnp.concatenate([t[:full] for t in tiles] + ends, axis=0)


def unpacked(value, count, tiles):
    full, short = count // 8 * 8, count % 8
    rows = round_up(count, 8)
    if not 0 < short <= 4:
        return jnp.concatenate([value[t * rows : (t + 1) * rows] for t in range(tiles)], axis=1)
    row = iota((8, LANES), 0)
    parts = []
    for t in range(tiles):
        at = full * tiles + 8 * (t // 2)
        end = value[at : at + 8]
        if t % 2:
            end = pltpu.roll(end, 4, 0)
        end = jnp.where(row < 4, end, 0.0)
        parts.append(jnp.concatenate([value[t * full : (t + 1) * full], end], axis=0))
    return jnp.concatenate(parts, axis=1)


def packed_rows(count, width):
    tiles = width // LANES
    if not 0 < count % 8 <= 4:
        return tiles * round_up(count, 8)
    return tiles * (count // 8 * 8) + 8 * (tiles // 2)


def deepened(value, rows):
    return jnp.concatenate(
        [value, jnp.zeros((rows - value.shape[0], value.shape[1]), F32)], axis=0
    )


def weave(table_terms, mask, place, table, innovation, maps, octz):
    both = []
    for octy in range(2):
        o = 4 * octz + 2 * octy
        wide = placed_at(jnp.concatenate([innovation, maps[o], maps[o + 1]], axis=1), place[...])
        if table is not None:
            wide = exact(table, deepened(wide, LANES))
        both.append(deepened(wide, LANES // 2))
    both = jnp.concatenate(both, axis=0)
    total = 0.0
    for term in range(table_terms.shape[0]):
        total = total + chosen(table_terms[term], both) * mask[term].astype(F32)
    high, low = split2(total)
    return jnp.concatenate([high, high, low], axis=1)


def head_kernel(n_slab, n_pencil, owner_map, window_start, bank, end, child_maps, innovation,
                table, fine_rows, fine_mask, fine_place, mid_rows, mid_mask, mid_place,
                partial, tail, fine_w, mid_w, maps, inner, head):
    rows = head.shape[0]
    count = innovation.shape[0]
    head[count // 8 * 8 :, :] = jnp.zeros((rows - count // 8 * 8, head.shape[1]), F32)
    head[:count, :] = bank[...]
    slab, pencil = lax.axis_index("slab"), lax.axis_index("pencil")

    def owned(level):
        return owner_map[window_start[0] + level] == slab

    tail[...] = end[...]
    maps[...] = jnp.zeros_like(maps)
    inner[...] = jnp.zeros_like(inner)
    for o in range(8):
        maps[o, :count, :count] = child_maps[:, o, :]
    inner[:count, :count] = innovation[...]
    quad = 4 * rows
    blocks = []
    for octz in range(2):
        block = 0.0
        for o in range(4):
            block = block + pltpu.roll(maps[4 * octz + o], o * rows, 1)
        blocks.append(block[:, :quad])
    flat = jnp.concatenate(blocks + [inner[:, :rows]], axis=1)
    w_high, w_low = split2(flat)
    w_all = jnp.concatenate([w_high, w_high, w_low], axis=1)
    lane = iota((rows, LANES), 1)
    last = LAST - 1

    def unshifted(at, shift):
        if shift == 0:
            return head[:, pl.ds(at, LANES)]
        left = pltpu.roll(head[:, pl.ds(at, LANES)], LANES - shift, 1)
        right = pltpu.roll(head[:, pl.ds(at + LANES, LANES)], LANES - shift, 1)
        return jnp.where(lane < LANES - shift, left, right)

    parent = None
    for level in range(last):
        side, nx = 2**level, ROOTS * 2**level
        cells = side * side * nx
        padded = round_up(cells, LANES)
        first = offset_of(level)
        shift = first % LANES
        noise = jnp.concatenate(
            [unshifted(first - shift + t * LANES, shift) for t in range(padded // LANES)], axis=1
        )
        noise = jnp.where(owned(level), noise, 0.0)
        if cells < padded:
            noise = jnp.where(iota((rows, padded), 1) < cells, noise, 0.0)
        if parent is None:
            up = jnp.zeros((rows, padded), F32)
        else:
            q = parent.shape[1]
            half = nx // 2

            def source_of(shape):
                cell = iota(shape, 1)
                x = cell & (nx - 1)
                y = (cell >> log2(nx)) & (side - 1)
                z = cell >> log2(nx * side)
                return x, y, z

            x, y, z = source_of((q, padded))
            source = ((z >> 1) * (side // 2) + (y >> 1)) * half + (x >> 1)
            pick = jnp.where(iota((q, padded), 0) == source, 1.0, 0.0).astype(BF16)
            up = picked(parent, pick)
        cell = iota((rows, padded), 1)
        octant = (
            4 * ((cell >> log2(nx * side)) & 1) + 2 * ((cell >> log2(nx)) & 1) + (cell & 1)
        )
        stack = jnp.concatenate(spread(up, octant, range(8)) + [noise], axis=0)
        parent = dot(w_all, stacked(stack))[:rows]

    r = Region(last, n_slab, n_pencil)
    half = r.nx // 2
    plane = (r.side // 2) * half
    cell = iota((plane, r.part), 1)
    y = (cell >> log2(r.nx)) + pencil * r.ny
    source = (y >> 1) * half + ((cell & (r.nx - 1)) >> 1)
    pick = jnp.where(iota((plane, r.part), 0) == source, 1.0, 0.0).astype(BF16)
    pieces = [split3(parent[:, z * plane : (z + 1) * plane]) for z in range(r.side // 2)]
    ups = dot(jnp.concatenate(pieces, axis=0), pick)
    cell = iota((rows, r.part), 1)
    octant = 2 * ((cell >> log2(r.nx)) & 1) + (cell & 1)
    first = offset_of(last)
    shift = first % LANES
    chain_w = []
    for octz in range(2):
        w = jnp.concatenate([blocks[octz], inner[:, :rows]], axis=1)
        high, low = split2(w)
        chain_w.append(jnp.concatenate([high, high, low], axis=1))
    for z in range(r.side):
        at = (z // 2) * 3 * rows
        up = ups[at : at + rows] + ups[at + rows : at + 2 * rows] + ups[at + 2 * rows : at + 3 * rows]
        start = first - shift + z * r.plane
        noise = jnp.concatenate(
            [
                unshifted(pl.multiple_of(start + pencil * r.part + t * LANES, LANES), shift)
                for t in range(r.part // LANES)
            ],
            axis=1,
        )
        noise = jnp.where(owned(last), noise, 0.0)
        stack = jnp.concatenate(spread(up, octant, range(4)) + [noise], axis=0)
        partial[z] = packed(dot(chain_w[z % 2], stacked(stack))[:rows], count)

    for octz in range(2):
        fine_w[octz] = weave(fine_rows, fine_mask, fine_place, table[...], inner[...], maps, octz)
        deep = chain_w[octz].shape[1]
        mid_w[octz, : mid_rows.shape[1]] = weave(mid_rows, mid_mask, mid_place, None, inner[...], maps, octz)
        mid_w[octz, mid_rows.shape[1] : mid_rows.shape[1] + rows, :deep] = chain_w[octz]


def routes(owner, n_slab):
    inner = 4
    others = [d for d in range(n_slab) if d != owner]
    if n_slab != inner * inner:
        return {d: None for d in others}
    own_z, own_p = divmod(owner, inner)

    def link(dest):
        z, p = divmod(dest, inner)
        if z != own_z:
            return "up" if z > own_z else "down"
        return "x" if (p ^ own_p) & 1 else "y"

    def options(dest):
        p = dest % inner
        found = [(None, link(dest))]
        for bit, name in ((1, "x"), (2, "y")):
            relay = own_z * inner + (own_p ^ bit)
            if relay != dest and (p ^ own_p) & bit:
                found.append((relay, name))
        return found

    load, via = {}, {}
    for d in others:
        load[link(d)] = load.get(link(d), 0) + 0.11
    for d in sorted(others, key=lambda d: (len(options(d)), d)):
        relay, name = min(
            options(d), key=lambda t: load.get(t[1], 0) + (0 if t[0] is None else 0.01)
        )
        load[name] = load.get(name, 0) + 1
        via[d] = relay
    return via


def share_kernel(owner, n_slab, n_pencil, bank, tail, partial, fresh, gathered, relay,
                 send, recv, own, to_relay, onward, give, take, keep):
    r = Region(LAST, n_slab, n_pencil)
    r4 = Region(LAST - 1, n_slab, n_pencil)
    me, pencil = lax.axis_index("slab"), lax.axis_index("pencil")
    base = offset_of(LAST) // LANES * LANES
    via = routes(owner, n_slab)
    relayed = [d for d in via if via[d] is not None]
    direct = [d for d in via if via[d] is None]
    slots = {}
    for d in relayed:
        slots[d] = sum(1 for e in slots if via[e] == via[d])

    def at(d):
        return {"slab": d}

    barrier = pltpu.get_barrier_semaphore()

    def greet(i, _):
        pl.semaphore_signal(
            barrier, inc=1, device_id=at(lax.rem(me + i, n_slab)), device_id_type=MESH
        )
        return 0

    lax.fori_loop(1, n_slab, greet, 0)
    pl.semaphore_wait(barrier, n_slab - 1)

    def source(d, z, size):
        start = base + (r.first_plane(d) + z) * r.plane + pencil * r.part
        return bank.at[:, :, pl.ds(pl.multiple_of(start, LANES), size)]

    def body(ref):
        return ref.at[:, :, pl.ds(0, r.part)]

    def rest(ref):
        return ref.at[:, :, pl.ds(r.part, LANES)]

    def remote(src, dst, ssem, rsem, d):
        return pltpu.make_async_remote_copy(
            src, dst, ssem, rsem, device_id=at(d), device_id_type=MESH
        )

    def start_pieces(d, z, dst, begin):
        plane = r.first_plane(d) + z
        whole = lambda: begin(source(d, z, r.part + LANES), dst)
        if isinstance(d, int) and plane < r.side - 1:
            whole()
            return
        ends = jnp.logical_and(plane == r.side - 1, pencil == n_pencil - 1)

        @pl.when(ends)
        def _():
            begin(source(d, z, r.part), body(dst))
            begin(tail, rest(dst))

        pl.when(jnp.logical_not(ends))(whole)

    def start_block(d, z):
        if isinstance(d, int) and via[d] is not None:
            dst, rsem, to = relay.at[slots[d], z], to_relay.at[slots[d], z], via[d]
        else:
            dst, rsem, to = fresh.at[z], recv.at[z], d
        start_pieces(d, z, dst, lambda src, ref: remote(src, ref, send.at[d, z], rsem, to).start())

    def drain_block(d, z):
        remote(fresh.at[z], fresh.at[z], send.at[d, z], recv.at[z], d).wait_send()

    def landed(dst, rsem, d):
        remote(dst, dst, send.at[0, 0], rsem, d).wait_recv()

    def forward(d, z):
        return remote(relay.at[slots[d], z], fresh.at[z], onward.at[slots[d], z], recv.at[z], d)

    @pl.when(me == owner)
    def _():
        if relayed:
            for d in relayed + direct:
                for z in range(r.nz):
                    start_block(d, z)
        else:

            def step(i, _):
                for z in range(r.nz):
                    start_block(lax.rem(owner + i, n_slab), z)
                return 0

            lax.fori_loop(1, n_slab, step, 0)
        for z in range(r.nz):
            start_pieces(
                owner,
                z,
                fresh.at[z],
                lambda src, ref: pltpu.make_async_copy(src, ref, own.at[z]).start(),
            )

    def piece(d):
        return partial.at[r4.first_plane(d)]

    def give_one(i, _):
        d = lax.rem(me + i, n_slab)
        remote(piece(d), gathered.at[me], give.at[d], take.at[me], d).start()
        return 0

    lax.fori_loop(1, n_slab, give_one, 0)
    mine = pltpu.make_async_copy(piece(me), gathered.at[me], keep)
    mine.start()

    for hub in sorted({via[d] for d in relayed}):

        @pl.when(me == hub)
        def _():
            group = [d for d in relayed if via[d] == hub]
            for d in group:
                for z in range(r.nz):
                    landed(relay.at[slots[d], z], to_relay.at[slots[d], z], owner)
                    forward(d, z).start()
            for d in group:
                for z in range(r.nz):
                    forward(d, z).wait_send()

    @pl.when(me != owner)
    def _():
        for z in range(r.nz):
            landed(fresh.at[z], recv.at[z], owner)

    @pl.when(me == owner)
    def _():
        if relayed:
            for d in relayed + direct:
                for z in range(r.nz):
                    drain_block(d, z)
        else:

            def step(i, _):
                for z in range(r.nz):
                    drain_block(lax.rem(owner + i, n_slab), z)
                return 0

            lax.fori_loop(1, n_slab, step, 0)
        for z in range(r.nz):
            pltpu.make_async_copy(relay.at[0, z], fresh.at[z], own.at[z]).wait()

    def take_one(i, _):
        d = lax.rem(me + i, n_slab)
        remote(piece(d), gathered.at[d], give.at[d], take.at[d], d).wait()
        return 0

    lax.fori_loop(1, n_slab, take_one, 0)
    mine.wait()


def share(owner, n_slab, n_pencil, count, bank, tail, partial):
    r = Region(LAST, n_slab, n_pencil)
    block = (r.nz, count, 1, r.part + LANES)
    via = routes(owner, n_slab)
    hubs = [v for v in via.values() if v is not None]
    slots = max([hubs.count(h) for h in hubs], default=1)
    dma = pltpu.SemaphoreType.DMA
    anywhere = pl.BlockSpec(memory_space=pl.ANY)
    return pl.pallas_call(
        functools.partial(share_kernel, owner, n_slab, n_pencil),
        in_specs=[anywhere] * 3,
        out_specs=[anywhere] * 2,
        out_shape=[
            jax.ShapeDtypeStruct(block, F32),
            jax.ShapeDtypeStruct((n_slab, *partial.shape[1:]), F32),
        ],
        scratch_shapes=[
            pltpu.VMEM((slots, *block), F32),
            dma((n_slab, r.nz)),
            dma((r.nz,)),
            dma((r.nz,)),
            dma((slots, r.nz)),
            dma((slots, r.nz)),
            dma((n_slab,)),
            dma((n_slab,)),
            dma,
        ],
        cost_estimate=pl.CostEstimate(
            flops=SHARE_FLOPS, bytes_accessed=SHARE_BYTES, transcendentals=0
        ),
        compiler_params=pltpu.CompilerParams(
            collective_id=owner, has_side_effects=True, vmem_limit_bytes=8 * MIB
        ),
        name="share",
    )(bank, tail, partial)


def middle_kernel(n_slab, n_pencil, per, gathered, fresh, noise, weights,
                  fine_plane, fine_row, fine_w, out, lower, south, last_coarse):
    r = Region(LAST, n_slab, n_pencil)
    q = Region(LAST - 1, n_slab, n_pencil)
    count = noise.shape[0]
    rows = round_up(count, 8)
    step = pl.program_id(0)
    slab = lax.axis_index("slab")

    @pl.when(step == 0)
    def _():
        parent = gathered[0]
        for d in range(1, gathered.shape[0]):
            parent = parent + gathered[d]
        parent = unpacked(parent, count, q.part // LANES)
        cell = iota((q.part, r.part), 1)
        source = (cell >> (log2(r.nx) + 1)) * q.nx + ((cell & (r.nx - 1)) >> 1)
        pick = jnp.where(iota((q.part, r.part), 0) == source, 1.0, 0.0).astype(BF16)
        up = picked(parent, pick)
        cell = iota((rows, r.part), 1)
        octant = 2 * ((cell >> log2(r.nx)) & 1) + (cell & 1)
        spreads = spread(up, octant, range(4))
        shift = offset_of(LAST) % LANES
        lane = iota((count, LANES), 1)
        for z in range(r.nz):
            raw = fresh[z, :, 0, :]
            rolled = [
                pltpu.roll(raw[:, t * LANES : (t + 1) * LANES], LANES - shift, 1)
                for t in range(r.part // LANES + 1)
            ]
            block = jnp.concatenate(
                [
                    jnp.where(lane < LANES - shift, rolled[t], rolled[t + 1])
                    for t in range(r.part // LANES)
                ],
                axis=1,
            )
            last_coarse[z] = jnp.zeros_like(last_coarse[z])
            last_coarse[z, :count, :] = block
            stack = jnp.concatenate(spreads + [last_coarse[z]], axis=0)
            octz = (r.first_plane(slab) + z) & 1
            chain_w = weights[octz, TILE * count : TILE * count + rows, : 15 * rows]
            last_coarse[z] = dot(chain_w, stacked(stack))[:rows]

    octz = lax.rem(slab * per * r.nz + step, 2)
    at = step // per
    wide = noise.shape[3]
    lane = iota((rows, LANES), 1)
    even = (lane & 1) == 0
    half = TILE // 2
    across = LANES // r.nx

    def parents(t):
        pieces = []
        for yy in range(half):
            y = t * half + yy
            cells = last_coarse[at, :, (y // across) * LANES : (y // across + 1) * LANES]
            index = (y % across) * r.nx + (lane >> 1)
            pieces.append(jnp.take_along_axis(cells, index, axis=1))
        return [jnp.where(even, p, 0.0) for p in pieces] + [jnp.where(even, 0.0, p) for p in pieces]

    group = 2
    for j in range(noise.shape[2] // (TILE * group)):
        columns = []
        for g in range(group):
            t = j * group + g
            fresh_part = noise[:, 0, t * TILE : (t + 1) * TILE, :].reshape(count * TILE, wide)
            columns.append(jnp.concatenate([fresh_part] + parents(t), axis=0))
        result = dot(weights[octz, : TILE * count], stacked(jnp.concatenate(columns, axis=1)))
        size = count * half
        for g in range(group):
            for h in range(2):
                out[0, (j * group + g) * 2 + h] = result[
                    h * size : (h + 1) * size, g * wide : (g + 1) * wide
                ]

    cols = fine_row.shape[3]
    edges = 2 * TILE
    ends = fine_w.shape[1]
    doubled = doubled_columns(out[0, 0], cols)
    for octz in range(2):
        fresh_part = fine_row[:, octz].reshape(count * TILE, cols)
        south[octz] = dot(fine_w[octz, ends - edges :], joined(fresh_part, doubled))

    @pl.when(step == 0)
    def _():
        for t in range(out.shape[1]):
            fresh_part = fine_plane[:, 0, t * TILE : (t + 1) * TILE, :].reshape(count * TILE, cols)
            lower[t] = dot(
                fine_w[0, BOTTOM * TILE : (BOTTOM + 4) * TILE],
                joined(fresh_part, doubled_columns(out[0, t], cols)),
            )


def interleave(even, odd):
    rows, cols = even.shape
    lane = iota((rows, LANES), 1)
    half = LANES // 2
    first = lane < half
    index = (lane >> 1) + (lane & 1) * half
    parts = []
    for j in range(cols // LANES):
        a = even[:, j * LANES : (j + 1) * LANES]
        b = odd[:, j * LANES : (j + 1) * LANES]
        left = jnp.where(first, a, pltpu.roll(b, half, 1))
        right = jnp.where(first, pltpu.roll(a, half, 1), b)
        parts.append(jnp.take_along_axis(left, index, axis=1))
        parts.append(jnp.take_along_axis(right, index, axis=1))
    return jnp.concatenate(parts, axis=1)


def doubled_columns(parent, cols):
    rows = parent.shape[0]
    lane = iota((rows, LANES), 1)
    even = (lane & 1) == 0
    parts = []
    for c in range(cols // LANES):
        index = (c % 2) * (LANES // 2) + (lane >> 1)
        from_lanes = parent[:, (c // 2) * LANES : (c // 2 + 1) * LANES]
        parts.append(jnp.take_along_axis(from_lanes, index, axis=1))
    evens = jnp.concatenate([jnp.where(even, p, 0.0) for p in parts], axis=1)
    odds = jnp.concatenate([jnp.where(even, 0.0, p) for p in parts], axis=1)
    return split2(jnp.concatenate([evens, odds], axis=0))


def joined(fresh, doubled):
    high, low = split2(fresh)
    up_high, up_low = doubled
    return jnp.concatenate([high, up_high, low, up_low, high, up_high], axis=0)


def fine_kernel(middle, noise, weights, field, zface, yface, carry_z, carry_y):
    count = noise.shape[0]
    cols = noise.shape[3]
    tiles = noise.shape[2] // TILE
    depth_step, row_step = pl.program_id(0), pl.program_id(1)

    @pl.when(depth_step == 0)
    def _():
        carry_z[row_step] = jnp.zeros(carry_z.shape[1:], F32)

    @pl.when(row_step == 0)
    def _():
        carry_y[...] = jnp.zeros_like(carry_y)

    end_row = iota((TILE, cols), 0) == TILE - 1
    edges = [carry_y[0], carry_y[1]]
    for j in reversed(range(tiles)):
        doubled = doubled_columns(middle[0, j], cols)
        above = carry_z[row_step, j]
        for octz in (1, 0):
            fresh = noise[:, octz, j * TILE : (j + 1) * TILE, :].reshape(count * TILE, cols)
            result = dot(weights[octz], joined(fresh, doubled))
            at = 0

            def take(size):
                nonlocal at
                at += size
                return result[at - size : at]

            rows = slice(2 * TILE * j, 2 * TILE * (j + 1))
            for half in range(2):
                field[2 * octz + half, rows] = interleave(take(2 * TILE), take(2 * TILE))
            top = take(4 * TILE) + above
            zface[octz, rows] = interleave(top[: 2 * TILE], top[2 * TILE :])
            above = take(4 * TILE)
            for half in range(2):
                pair = []
                for side in range(2):
                    k = TILE * side + half
                    edge = edges[octz][k : k + 1, :]
                    pair.append(take(TILE) + jnp.where(end_row, edge, 0.0))
                yface[2 * octz + half, TILE * j : TILE * (j + 1)] = interleave(*pair)
            edges[octz] = take(2 * TILE)
        carry_z[row_step, j] = above
    for octz in range(2):
        carry_y[octz] = edges[octz]


def seam_kernel(lower, south, zface, yface, z_out, y_out):
    rows = zface.shape[1] // lower.shape[0]
    for t in range(lower.shape[0]):
        block = lower[t]
        at = slice(t * rows, (t + 1) * rows)
        z_out[0, at] = zface[0, at] + interleave(block[:rows], block[rows:])
    last = yface.shape[1] - 1
    end_row = iota(yface.shape[1:], 0) == last
    for plane in range(south.shape[0]):
        edge = interleave(south[plane, :TILE], south[plane, TILE:])
        for half in range(2):
            y_out[2 * plane + half] = yface[2 * plane + half] + jnp.where(
                end_row, edge[half : half + 1], 0.0
            )


def fine_rows():
    table, index = [], {}

    def entry(point, scale):
        key = (point, scale)
        if key not in index:
            index[key] = len(table)
            table.append(scale * basis_row(point))
        return index[key]

    halves = [-0.5, 0.5]
    rows = []
    for pz in halves:
        for px in halves:
            for y in range(TILE):
                for py in halves:
                    rows.append([(entry((pz, py, px), 1.0), y)])
    for w in (1.0, -1.0):
        for px in halves:
            for y in range(TILE):
                for py in halves:
                    rows.append([(entry((w, py, px), 0.5), y)])
    for pz in halves:
        for px in halves:
            for y in range(TILE):
                terms = [(entry((pz, 1.0, px), 0.5), y)]
                if y + 1 < TILE:
                    terms.append((entry((pz, -1.0, px), 0.5), y + 1))
                rows.append(terms)
    for px in halves:
        for pz in halves:
            rows.append([(entry((pz, -1.0, px), 0.5), 0)])
        rows.extend([[]] * (TILE - 2))
    return np.array(table), rows


def layout_of(rows, count, parent_columns):
    columns = count * TILE + 2 * len(parent_columns)
    place = np.zeros((3, LANES, columns), np.float32)
    at_y = np.zeros((columns,), np.int64)
    for k in range(count):
        for y in range(TILE):
            place[0, k, k * TILE + y] = 1
            at_y[k * TILE + y] = y
    for block in (1, 2):
        for i, (k, y) in enumerate(parent_columns):
            c = count * TILE + (block - 1) * len(parent_columns) + i
            at_y[c] = y
            if k < count:
                place[block, k, c] = 1
    noise = np.arange(columns) < count * TILE
    terms = max(len(r) for r in rows)
    pick = np.zeros((terms, len(rows), LANES), np.float32)
    mask = np.zeros((terms, len(rows), columns), np.float32)
    for term in range(terms):
        for i, row in enumerate(rows):
            if term < len(row):
                q, y = row[term]
                pick[term, i, (y % 2) * (LANES // 2) + q] = 1
                mask[term, i] = np.where(noise, at_y == y, at_y == y // 2)
    return tuple(jnp.asarray(a, BF16) for a in (pick, mask, place.reshape(3 * LANES, columns)))


def shards(n_slab, n_pencil, owner_map, window_start, child_maps, innovation, bank,
           noise_middle, noise_finest):
    count = innovation.shape[0]
    padded = round_up(count, 8)
    total = bank.shape[2]
    owner = owner_map[window_start[0] + LAST]
    smem = pl.BlockSpec(memory_space=pltpu.SMEM)
    vmem = pl.BlockSpec(memory_space=pltpu.VMEM)
    top = Region(LAST, n_slab, n_pencil)
    under = Region(LAST - 1, n_slab, n_pencil)

    rows3 = bank.reshape(count, 1, total)
    head_width = offset_of(LAST) // LANES * LANES + LANES
    head = bank[0, :, :head_width]
    table, row_list = fine_rows()
    half = TILE // 2
    fine_columns = [(k, y) for k in range(count) for y in range(half)]
    fine_parts = layout_of(row_list, count, fine_columns)
    mid_columns = [(k, y) for y in range(half) for k in range(padded)]
    mid_list = [[(k, h * half + y)] for h in range(2) for k in range(count) for y in range(half)]
    mid_parts = layout_of(mid_list, count, mid_columns)
    fine_k, mid_k = fine_parts[1].shape[2], mid_parts[1].shape[2]

    partial, tail, fine_weights, mid_weights = pl.pallas_call(
        functools.partial(head_kernel, n_slab, n_pencil),
        grid=(1,),
        in_specs=[
            smem,
            smem,
            vmem,
            pl.BlockSpec((count, 1, LANES), lambda i: (0, 0, total // LANES)),
        ]
        + [vmem] * 9,
        out_specs=[vmem] * 4,
        out_shape=[
            jax.ShapeDtypeStruct((under.side, packed_rows(count, under.part), LANES), F32),
            jax.ShapeDtypeStruct((count, 1, LANES), F32),
            jax.ShapeDtypeStruct((2, len(row_list), 3 * fine_k), BF16),
            jax.ShapeDtypeStruct((2, len(mid_list) + round_up(padded, 16), 3 * mid_k), BF16),
        ],
        scratch_shapes=[
            pltpu.VMEM((8, padded, LANES), F32),
            pltpu.VMEM((padded, LANES), F32),
            pltpu.VMEM((padded, head_width), F32),
        ],
        compiler_params=pltpu.CompilerParams(vmem_limit_bytes=20 * MIB),
        name="head",
    )(owner_map, window_start, head, rows3, child_maps.transpose(1, 0, 2), innovation,
      jnp.asarray(np.pad(table, ((0, 0), (0, LANES - count))), F32), *fine_parts, *mid_parts)

    fresh, gathered = lax.switch(
        owner,
        [functools.partial(share, o, n_slab, n_pencil, count) for o in range(n_slab)],
        rows3, tail, partial,
    )

    _, planes, rows, cols = noise_middle.shape
    per = planes // top.nz
    tiles = 2 * rows // TILE
    _, fine_planes, fine_y, fine_x = noise_finest.shape
    out_x = 2 * fine_x
    in_hbm = pltpu.with_memory_space_constraint(noise_finest, pltpu.HBM)
    middle, lower, south = pl.pallas_call(
        functools.partial(middle_kernel, n_slab, n_pencil, per),
        grid=(planes,),
        in_specs=[
            pl.BlockSpec(gathered.shape, lambda z: (0, 0, 0)),
            pl.BlockSpec(fresh.shape, lambda z: (0, 0, 0, 0)),
            pl.BlockSpec((count, 1, rows, cols), lambda z: (0, z, 0, 0)),
            vmem,
            pl.BlockSpec((count, 1, fine_y, fine_x), lambda z: (0, 0, 0, 0)),
            pl.BlockSpec((count, 2, TILE, fine_x), lambda z: (0, z, 0, 0)),
            vmem,
        ],
        out_specs=[
            pl.BlockSpec((1, tiles, count * half, cols), lambda z: (z, 0, 0, 0)),
            pl.BlockSpec((tiles, 4 * TILE, fine_x), lambda z: (0, 0, 0)),
            pl.BlockSpec((2, 2 * TILE, fine_x), lambda z: (z, 0, 0)),
        ],
        out_shape=[
            jax.ShapeDtypeStruct((planes, tiles, count * half, cols), F32),
            jax.ShapeDtypeStruct((tiles, 4 * TILE, fine_x), F32),
            jax.ShapeDtypeStruct((fine_planes, 2 * TILE, fine_x), F32),
        ],
        scratch_shapes=[pltpu.VMEM((top.nz, padded, top.part), F32)],
        cost_estimate=pl.CostEstimate(
            flops=MID_FLOPS, bytes_accessed=4 * noise_middle.size, transcendentals=0
        ),
        compiler_params=pltpu.CompilerParams(vmem_limit_bytes=24 * MIB),
        name="middle",
    )(gathered, fresh, noise_middle, mid_weights, in_hbm, in_hbm,
      fine_weights)
    above = shifted(lower, "slab", -1)
    beside = shifted(south, "pencil", -1)

    deep = 64
    nz, ny = planes, fine_y // deep
    each = deep // TILE

    def block(*where):
        def index(z, y):
            at = {"z": nz - 1 - z, "y": ny - 1 - y}
            return tuple(at.get(w, 0) for w in where)

        return index

    field, zface, yface = pl.pallas_call(
        fine_kernel,
        grid=(nz, ny),
        in_specs=[
            pl.BlockSpec((1, each, count * half, cols), block("z", "y", 0, 0)),
            pl.BlockSpec((count, 2, deep, fine_x), block(0, "z", "y", 0)),
            vmem,
        ],
        out_specs=[
            pl.BlockSpec((4, 2 * deep, out_x), block("z", "y", 0)),
            pl.BlockSpec((2, 2 * deep, out_x), block("z", "y", 0)),
            pl.BlockSpec((4, deep, out_x), block("z", "y", 0)),
        ],
        out_shape=[
            jax.ShapeDtypeStruct((2 * fine_planes, 2 * fine_y, out_x), F32),
            jax.ShapeDtypeStruct((fine_planes, 2 * fine_y, out_x), F32),
            jax.ShapeDtypeStruct((2 * fine_planes, fine_y, out_x), F32),
        ],
        scratch_shapes=[
            pltpu.VMEM((ny, each, 4 * TILE, fine_x), F32),
            pltpu.VMEM((2, 2 * TILE, fine_x), F32),
        ],
        cost_estimate=pl.CostEstimate(
            flops=2 * nz * (fine_y // TILE) * fine_weights.size * fine_x,
            bytes_accessed=4 * (noise_finest.size + 16 * fine_planes * fine_y * fine_x),
            transcendentals=0,
        ),
        compiler_params=pltpu.CompilerParams(vmem_limit_bytes=24 * MIB),
        name="fine",
    )(middle, noise_finest, fine_weights)
    z_spec = pl.BlockSpec((1, 2 * fine_y, out_x), lambda i: (fine_planes - 1, 0, 0))
    y_spec = pl.BlockSpec((2 * fine_planes, TILE, out_x), lambda i: (0, fine_y // TILE - 1, 0))
    zface, yface = pl.pallas_call(
        seam_kernel,
        grid=(1,),
        in_specs=[
            pl.BlockSpec(above.shape, lambda i: (0, 0, 0)),
            pl.BlockSpec(beside.shape, lambda i: (0, 0, 0)),
            z_spec,
            y_spec,
        ],
        out_specs=[z_spec, y_spec],
        out_shape=[
            jax.ShapeDtypeStruct(zface.shape, F32),
            jax.ShapeDtypeStruct(yface.shape, F32),
        ],
        input_output_aliases={2: 0, 3: 1},
        compiler_params=pltpu.CompilerParams(vmem_limit_bytes=8 * MIB),
        name="seam",
    )(above, beside, zface, yface)
    return field, zface, yface


def solution(mesh):
    placed = (
        P(),
        P(),
        P(),
        P(),
        P("slab", None, None),
        P(None, "slab", "pencil", None),
        P(None, "slab", "pencil", None),
    )
    return jax.shard_map(
        functools.partial(shards, mesh.shape["slab"], mesh.shape["pencil"]),
        mesh=mesh,
        in_specs=placed,
        out_specs=(P("slab", "pencil", None), P("slab", "pencil", None), P("slab", "pencil", None)),
        check_vma=False,
    )
```

```python
import functools
import math

import jax
import jax.numpy as jnp
import numpy as np
from jax import lax
from jax.experimental import pallas as pl
from jax.experimental.pallas import tpu as pltpu
from jax.sharding import PartitionSpec as P

LEVELS = 8
ROOTS = 2
BANKS = LEVELS - 2
LAST = BANKS - 1
LANES = 128
TILE = 8
BOTTOM = 12
MIB = 1 << 20
SHARE_FLOPS = 20 * 10**9
SHARE_BYTES = 80 * 10**6
MID_FLOPS = 6 * 10**9
F32 = jnp.float32
BF16 = jnp.bfloat16
MESH = pl.DeviceIdType.MESH


def legendre(order, point):
    values = [1.0, point, 1.5 * point * point - 0.5, 2.5 * point * point * point - 1.5 * point]
    return values[order]


def basis_row(point):
    w_coord, v_coord, u_coord = point
    entry = []
    for deg_x in range(4):
        for deg_y in range(4):
            for deg_z in range(4):
                if deg_x + deg_y + deg_z <= 3:
                    factor = math.sqrt((2 * deg_x + 1) * (2 * deg_y + 1) * (2 * deg_z + 1))
                    entry.append(
                        factor
                        * legendre(deg_x, u_coord)
                        * legendre(deg_y, v_coord)
                        * legendre(deg_z, w_coord)
                    )
    return np.array(entry)


def shifted(block, axis, distance):
    devices = range(lax.axis_size(axis))
    route = [((i - distance) % len(devices), i) for i in devices]
    return lax.ppermute(block, axis, route)


def offset_of(level):
    return ROOTS * (8**level - 1) // 7


def round_up(size, unit):
    return -(-size // unit) * unit


def log2(n):
    return n.bit_length() - 1


class Region:
    def __init__(self, level, n_slab, n_pencil):
        side = 2**level
        self.level = level
        self.side = side
        self.nx = ROOTS * side
        self.ny = side // n_pencil
        self.nz = max(1, side // n_slab)
        self.plane = side * self.nx
        self.part = self.ny * self.nx
        self.n_slab = n_slab

    def first_plane(self, slab):
        return (slab * self.side) // self.n_slab


def split2(value):
    high = value.astype(BF16)
    low = (value - high.astype(F32)).astype(BF16)
    return high, low


def split3(value):
    high, low = split2(value)
    rest = value - high.astype(F32) - low.astype(F32)
    return jnp.concatenate([high.astype(F32), low.astype(F32), rest], axis=0).astype(BF16)


def dot(left, right):
    return jnp.dot(left, right, preferred_element_type=F32)


def exact(left, right):
    left_high, left_low = split2(left)
    right_high, right_low = split2(right)
    return dot(left_high, right_high) + (dot(left_low, right_high) + dot(left_high, right_low))


def chosen(pick, value):
    high, low = split2(value)
    return dot(pick, high) + dot(pick, low)


def placed_at(value, place):
    high, low = split2(value)
    return dot(high, place) + dot(low, place)


def stacked(value):
    high, low = split2(value)
    return jnp.concatenate([high, low, high], axis=0)


def picked(parent, pick):
    rows = parent.shape[0]
    up = dot(split3(parent), pick)
    return up[:rows] + up[rows : 2 * rows] + up[2 * rows :]


def spread(up, octant, names):
    return [jnp.where(octant == o, up, 0.0) for o in names]


def iota(shape, dim):
    return lax.broadcasted_iota(jnp.int32, shape, dim)


def packed(value, count):
    full, short = count // 8 * 8, count % 8
    tiles = [value[:, t * LANES : (t + 1) * LANES] for t in range(value.shape[1] // LANES)]
    if not 0 < short <= 4:
        return jnp.concatenate(tiles, axis=0)
    row = iota((8, LANES), 0)
    ends = [
        jnp.where(row < 4, a[full:], pltpu.roll(b[full:], 4, 0))
        for a, b in zip(tiles[::2], tiles[1::2])
    ]
    return jnp.concatenate([t[:full] for t in tiles] + ends, axis=0)


def unpacked(value, count, tiles):
    full, short = count // 8 * 8, count % 8
    rows = round_up(count, 8)
    if not 0 < short <= 4:
        return jnp.concatenate([value[t * rows : (t + 1) * rows] for t in range(tiles)], axis=1)
    row = iota((8, LANES), 0)
    parts = []
    for t in range(tiles):
        at = full * tiles + 8 * (t // 2)
        end = value[at : at + 8]
        if t % 2:
            end = pltpu.roll(end, 4, 0)
        end = jnp.where(row < 4, end, 0.0)
        parts.append(jnp.concatenate([value[t * full : (t + 1) * full], end], axis=0))
    return jnp.concatenate(parts, axis=1)


def packed_rows(count, width):
    tiles = width // LANES
    if not 0 < count % 8 <= 4:
        return tiles * round_up(count, 8)
    return tiles * (count // 8 * 8) + 8 * (tiles // 2)


def deepened(value, rows):
    return jnp.concatenate(
        [value, jnp.zeros((rows - value.shape[0], value.shape[1]), F32)], axis=0
    )


def weave(table_terms, mask, place, table, innovation, maps, octz):
    both = []
    for octy in range(2):
        o = 4 * octz + 2 * octy
        wide = placed_at(jnp.concatenate([innovation, maps[o], maps[o + 1]], axis=1), place[...])
        if table is not None:
            wide = exact(table, deepened(wide, LANES))
        both.append(deepened(wide, LANES // 2))
    both = jnp.concatenate(both, axis=0)
    total = 0.0
    for term in range(table_terms.shape[0]):
        total = total + chosen(table_terms[term], both) * mask[term].astype(F32)
    high, low = split2(total)
    return jnp.concatenate([high, high, low], axis=1)


def head_kernel(n_slab, n_pencil, owner_map, window_start, bank, end, child_maps, innovation,
                table, fine_rows, fine_mask, fine_place, mid_rows, mid_mask, mid_place,
                partial, tail, fine_w, mid_w, maps, inner, head):
    rows = head.shape[0]
    count = innovation.shape[0]
    head[count // 8 * 8 :, :] = jnp.zeros((rows - count // 8 * 8, head.shape[1]), F32)
    head[:count, :] = bank[...]
    slab, pencil = lax.axis_index("slab"), lax.axis_index("pencil")

    def owned(level):
        return owner_map[window_start[0] + level] == slab

    tail[...] = end[...]
    maps[...] = jnp.zeros_like(maps)
    inner[...] = jnp.zeros_like(inner)
    for o in range(8):
        maps[o, :count, :count] = child_maps[:, o, :]
    inner[:count, :count] = innovation[...]
    quad = 4 * rows
    blocks = []
    for octz in range(2):
        block = 0.0
        for o in range(4):
            block = block + pltpu.roll(maps[4 * octz + o], o * rows, 1)
        blocks.append(block[:, :quad])
    flat = jnp.concatenate(blocks + [inner[:, :rows]], axis=1)
    w_high, w_low = split2(flat)
    w_all = jnp.concatenate([w_high, w_high, w_low], axis=1)
    lane = iota((rows, LANES), 1)
    last = LAST - 1

    def unshifted(at, shift):
        if shift == 0:
            return head[:, pl.ds(at, LANES)]
        left = pltpu.roll(head[:, pl.ds(at, LANES)], LANES - shift, 1)
        right = pltpu.roll(head[:, pl.ds(at + LANES, LANES)], LANES - shift, 1)
        return jnp.where(lane < LANES - shift, left, right)

    parent = None
    for level in range(last):
        side, nx = 2**level, ROOTS * 2**level
        cells = side * side * nx
        padded = round_up(cells, LANES)
        first = offset_of(level)
        shift = first % LANES
        noise = jnp.concatenate(
            [unshifted(first - shift + t * LANES, shift) for t in range(padded // LANES)], axis=1
        )
        noise = jnp.where(owned(level), noise, 0.0)
        if cells < padded:
            noise = jnp.where(iota((rows, padded), 1) < cells, noise, 0.0)
        if parent is None:
            up = jnp.zeros((rows, padded), F32)
        else:
            q = parent.shape[1]
            half = nx // 2

            def source_of(shape):
                cell = iota(shape, 1)
                x = cell & (nx - 1)
                y = (cell >> log2(nx)) & (side - 1)
                z = cell >> log2(nx * side)
                return x, y, z

            x, y, z = source_of((q, padded))
            source = ((z >> 1) * (side // 2) + (y >> 1)) * half + (x >> 1)
            pick = jnp.where(iota((q, padded), 0) == source, 1.0, 0.0).astype(BF16)
            up = picked(parent, pick)
        cell = iota((rows, padded), 1)
        octant = (
            4 * ((cell >> log2(nx * side)) & 1) + 2 * ((cell >> log2(nx)) & 1) + (cell & 1)
        )
        stack = jnp.concatenate(spread(up, octant, range(8)) + [noise], axis=0)
        parent = dot(w_all, stacked(stack))[:rows]

    r = Region(last, n_slab, n_pencil)
    half = r.nx // 2
    plane = (r.side // 2) * half
    cell = iota((plane, r.part), 1)
    y = (cell >> log2(r.nx)) + pencil * r.ny
    source = (y >> 1) * half + ((cell & (r.nx - 1)) >> 1)
    pick = jnp.where(iota((plane, r.part), 0) == source, 1.0, 0.0).astype(BF16)
    pieces = [split3(parent[:, z * plane : (z + 1) * plane]) for z in range(r.side // 2)]
    ups = dot(jnp.concatenate(pieces, axis=0), pick)
    cell = iota((rows, r.part), 1)
    octant = 2 * ((cell >> log2(r.nx)) & 1) + (cell & 1)
    first = offset_of(last)
    shift = first % LANES
    chain_w = []
    for octz in range(2):
        w = jnp.concatenate([blocks[octz], inner[:, :rows]], axis=1)
        high, low = split2(w)
        chain_w.append(jnp.concatenate([high, high, low], axis=1))
    for z in range(r.side):
        at = (z // 2) * 3 * rows
        up = ups[at : at + rows] + ups[at + rows : at + 2 * rows] + ups[at + 2 * rows : at + 3 * rows]
        start = first - shift + z * r.plane
        noise = jnp.concatenate(
            [
                unshifted(pl.multiple_of(start + pencil * r.part + t * LANES, LANES), shift)
                for t in range(r.part // LANES)
            ],
            axis=1,
        )
        noise = jnp.where(owned(last), noise, 0.0)
        stack = jnp.concatenate(spread(up, octant, range(4)) + [noise], axis=0)
        partial[z] = packed(dot(chain_w[z % 2], stacked(stack))[:rows], count)

    for octz in range(2):
        fine_w[octz] = weave(fine_rows, fine_mask, fine_place, table[...], inner[...], maps, octz)
        deep = chain_w[octz].shape[1]
        mid_w[octz, : mid_rows.shape[1]] = weave(mid_rows, mid_mask, mid_place, None, inner[...], maps, octz)
        mid_w[octz, mid_rows.shape[1] : mid_rows.shape[1] + rows, :deep] = chain_w[octz]


def routes(owner, n_slab, nz):
    inner = 4
    others = [d for d in range(n_slab) if d != owner]
    if n_slab != inner * inner:
        return {(d, z): None for d in others for z in range(nz)}
    own_z, own_p = divmod(owner, inner)

    def link(dest):
        z, p = divmod(dest, inner)
        if z != own_z:
            return "up" if z > own_z else "down"
        return "x" if (p ^ own_p) & 1 else "y"

    def options(dest):
        p = dest % inner
        found = [(None, link(dest))]
        for bit, name in ((1, "x"), (2, "y")):
            relay = own_z * inner + (own_p ^ bit)
            if relay != dest and (p ^ own_p) & bit:
                found.append((relay, name))
        return found

    load, via = {}, {}
    for d in others:
        load[link(d)] = load.get(link(d), 0) + 0.11 * nz
    for d in sorted(others, key=lambda d: (len(options(d)), d)):
        for z in range(nz):
            relay, name = min(
                options(d), key=lambda t: load.get(t[1], 0) + (0 if t[0] is None else 0.01)
            )
            load[name] = load.get(name, 0) + 1
            via[d, z] = relay
    return via


def share_kernel(owner, n_slab, n_pencil, bank, tail, partial, fresh, gathered, relay,
                 send, recv, own, to_relay, onward, give, take, keep):
    r = Region(LAST, n_slab, n_pencil)
    r4 = Region(LAST - 1, n_slab, n_pencil)
    me, pencil = lax.axis_index("slab"), lax.axis_index("pencil")
    base = offset_of(LAST) // LANES * LANES
    via = routes(owner, n_slab, r.nz)
    relayed = [k for k in via if via[k] is not None]
    direct = [k for k in via if via[k] is None]
    slots = {}
    for k in relayed:
        slots[k] = sum(1 for e in slots if via[e] == via[k])

    def at(d):
        return {"slab": d}

    barrier = pltpu.get_barrier_semaphore()

    def greet(i, _):
        pl.semaphore_signal(
            barrier, inc=1, device_id=at(lax.rem(me + i, n_slab)), device_id_type=MESH
        )
        return 0

    lax.fori_loop(1, n_slab, greet, 0)
    pl.semaphore_wait(barrier, n_slab - 1)

    def source(d, z, size):
        start = base + (r.first_plane(d) + z) * r.plane + pencil * r.part
        return bank.at[:, :, pl.ds(pl.multiple_of(start, LANES), size)]

    def body(ref):
        return ref.at[:, :, pl.ds(0, r.part)]

    def rest(ref):
        return ref.at[:, :, pl.ds(r.part, LANES)]

    def remote(src, dst, ssem, rsem, d):
        return pltpu.make_async_remote_copy(
            src, dst, ssem, rsem, device_id=at(d), device_id_type=MESH
        )

    def start_pieces(d, z, dst, begin):
        plane = r.first_plane(d) + z
        whole = lambda: begin(source(d, z, r.part + LANES), dst)
        if isinstance(d, int) and plane < r.side - 1:
            whole()
            return
        ends = jnp.logical_and(plane == r.side - 1, pencil == n_pencil - 1)

        @pl.when(ends)
        def _():
            begin(source(d, z, r.part), body(dst))
            begin(tail, rest(dst))

        pl.when(jnp.logical_not(ends))(whole)

    def start_block(d, z):
        if isinstance(d, int) and via[d, z] is not None:
            slot = slots[d, z]
            dst, rsem, to = relay.at[slot], to_relay.at[slot], via[d, z]
        else:
            dst, rsem, to = fresh.at[z], recv.at[z], d
        start_pieces(d, z, dst, lambda src, ref: remote(src, ref, send.at[d, z], rsem, to).start())

    def drain_block(d, z):
        remote(fresh.at[z], fresh.at[z], send.at[d, z], recv.at[z], d).wait_send()

    def landed(dst, rsem, d):
        remote(dst, dst, send.at[0, 0], rsem, d).wait_recv()

    def forward(d, z):
        slot = slots[d, z]
        return remote(relay.at[slot], fresh.at[z], onward.at[slot], recv.at[z], d)

    @pl.when(me == owner)
    def _():
        if relayed:
            for d, z in relayed + direct:
                start_block(d, z)
        else:

            def step(i, _):
                for z in range(r.nz):
                    start_block(lax.rem(owner + i, n_slab), z)
                return 0

            lax.fori_loop(1, n_slab, step, 0)
        for z in range(r.nz):
            start_pieces(
                owner,
                z,
                fresh.at[z],
                lambda src, ref: pltpu.make_async_copy(src, ref, own.at[z]).start(),
            )

    def piece(d):
        return partial.at[r4.first_plane(d)]

    def give_one(i, _):
        d = lax.rem(me + i, n_slab)
        remote(piece(d), gathered.at[me], give.at[d], take.at[me], d).start()
        return 0

    lax.fori_loop(1, n_slab, give_one, 0)
    mine = pltpu.make_async_copy(piece(me), gathered.at[me], keep)
    mine.start()

    for hub in sorted({via[k] for k in relayed}):

        @pl.when(me == hub)
        def _():
            group = [k for k in relayed if via[k] == hub]
            for d, z in group:
                landed(relay.at[slots[d, z]], to_relay.at[slots[d, z]], owner)
                forward(d, z).start()
            for d, z in group:
                forward(d, z).wait_send()

    @pl.when(me != owner)
    def _():
        for z in range(r.nz):
            landed(fresh.at[z], recv.at[z], owner)

    @pl.when(me == owner)
    def _():
        if relayed:
            for d, z in relayed + direct:
                drain_block(d, z)
        else:

            def step(i, _):
                for z in range(r.nz):
                    drain_block(lax.rem(owner + i, n_slab), z)
                return 0

            lax.fori_loop(1, n_slab, step, 0)
        for z in range(r.nz):
            pltpu.make_async_copy(relay.at[0], fresh.at[z], own.at[z]).wait()

    def take_one(i, _):
        d = lax.rem(me + i, n_slab)
        remote(piece(d), gathered.at[d], give.at[d], take.at[d], d).wait()
        return 0

    lax.fori_loop(1, n_slab, take_one, 0)
    mine.wait()


def share(owner, n_slab, n_pencil, count, bank, tail, partial):
    r = Region(LAST, n_slab, n_pencil)
    block = (r.nz, count, 1, r.part + LANES)
    via = routes(owner, n_slab, r.nz)
    hubs = [v for v in via.values() if v is not None]
    slots = max([hubs.count(h) for h in hubs], default=1)
    dma = pltpu.SemaphoreType.DMA
    anywhere = pl.BlockSpec(memory_space=pl.ANY)
    return pl.pallas_call(
        functools.partial(share_kernel, owner, n_slab, n_pencil),
        in_specs=[anywhere] * 3,
        out_specs=[anywhere] * 2,
        out_shape=[
            jax.ShapeDtypeStruct(block, F32),
            jax.ShapeDtypeStruct((n_slab, *partial.shape[1:]), F32),
        ],
        scratch_shapes=[
            pltpu.VMEM((slots, *block[1:]), F32),
            dma((n_slab, r.nz)),
            dma((r.nz,)),
            dma((r.nz,)),
            dma((slots,)),
            dma((slots,)),
            dma((n_slab,)),
            dma((n_slab,)),
            dma,
        ],
        cost_estimate=pl.CostEstimate(
            flops=SHARE_FLOPS, bytes_accessed=SHARE_BYTES, transcendentals=0
        ),
        compiler_params=pltpu.CompilerParams(
            collective_id=owner, has_side_effects=True, vmem_limit_bytes=8 * MIB
        ),
        name="share",
    )(bank, tail, partial)


def middle_kernel(n_slab, n_pencil, per, gathered, fresh, noise, weights,
                  fine_plane, fine_row, fine_w, out, lower, south, last_coarse):
    r = Region(LAST, n_slab, n_pencil)
    q = Region(LAST - 1, n_slab, n_pencil)
    count = noise.shape[0]
    rows = round_up(count, 8)
    step = pl.program_id(0)
    slab = lax.axis_index("slab")

    @pl.when(step == 0)
    def _():
        parent = gathered[0]
        for d in range(1, gathered.shape[0]):
            parent = parent + gathered[d]
        parent = unpacked(parent, count, q.part // LANES)
        cell = iota((q.part, r.part), 1)
        source = (cell >> (log2(r.nx) + 1)) * q.nx + ((cell & (r.nx - 1)) >> 1)
        pick = jnp.where(iota((q.part, r.part), 0) == source, 1.0, 0.0).astype(BF16)
        up = picked(parent, pick)
        cell = iota((rows, r.part), 1)
        octant = 2 * ((cell >> log2(r.nx)) & 1) + (cell & 1)
        spreads = spread(up, octant, range(4))
        shift = offset_of(LAST) % LANES
        lane = iota((count, LANES), 1)
        for z in range(r.nz):
            raw = fresh[z, :, 0, :]
            rolled = [
                pltpu.roll(raw[:, t * LANES : (t + 1) * LANES], LANES - shift, 1)
                for t in range(r.part // LANES + 1)
            ]
            block = jnp.concatenate(
                [
                    jnp.where(lane < LANES - shift, rolled[t], rolled[t + 1])
                    for t in range(r.part // LANES)
                ],
                axis=1,
            )
            last_coarse[z] = jnp.zeros_like(last_coarse[z])
            last_coarse[z, :count, :] = block
            stack = jnp.concatenate(spreads + [last_coarse[z]], axis=0)
            octz = (r.first_plane(slab) + z) & 1
            chain_w = weights[octz, TILE * count : TILE * count + rows, : 15 * rows]
            last_coarse[z] = dot(chain_w, stacked(stack))[:rows]

    octz = lax.rem(slab * per * r.nz + step, 2)
    at = step // per
    wide = noise.shape[3]
    lane = iota((rows, LANES), 1)
    even = (lane & 1) == 0
    half = TILE // 2
    across = LANES // r.nx

    def parents(t):
        pieces = []
        for yy in range(half):
            y = t * half + yy
            cells = last_coarse[at, :, (y // across) * LANES : (y // across + 1) * LANES]
            index = (y % across) * r.nx + (lane >> 1)
            pieces.append(jnp.take_along_axis(cells, index, axis=1))
        return [jnp.where(even, p, 0.0) for p in pieces] + [jnp.where(even, 0.0, p) for p in pieces]

    group = 2
    for j in range(noise.shape[2] // (TILE * group)):
        columns = []
        for g in range(group):
            t = j * group + g
            fresh_part = noise[:, 0, t * TILE : (t + 1) * TILE, :].reshape(count * TILE, wide)
            columns.append(jnp.concatenate([fresh_part] + parents(t), axis=0))
        result = dot(weights[octz, : TILE * count], stacked(jnp.concatenate(columns, axis=1)))
        size = count * half
        for g in range(group):
            for h in range(2):
                out[0, (j * group + g) * 2 + h] = result[
                    h * size : (h + 1) * size, g * wide : (g + 1) * wide
                ]

    cols = fine_row.shape[3]
    edges = 2 * TILE
    ends = fine_w.shape[1]
    doubled = doubled_columns(out[0, 0], cols)
    for octz in range(2):
        fresh_part = fine_row[:, octz].reshape(count * TILE, cols)
        south[octz] = dot(fine_w[octz, ends - edges :], joined(fresh_part, doubled))

    @pl.when(step == 0)
    def _():
        for t in range(out.shape[1]):
            fresh_part = fine_plane[:, 0, t * TILE : (t + 1) * TILE, :].reshape(count * TILE, cols)
            lower[t] = dot(
                fine_w[0, BOTTOM * TILE : (BOTTOM + 4) * TILE],
                joined(fresh_part, doubled_columns(out[0, t], cols)),
            )


def interleave(even, odd):
    rows, cols = even.shape
    lane = iota((rows, LANES), 1)
    half = LANES // 2
    first = lane < half
    index = (lane >> 1) + (lane & 1) * half
    parts = []
    for j in range(cols // LANES):
        a = even[:, j * LANES : (j + 1) * LANES]
        b = odd[:, j * LANES : (j + 1) * LANES]
        left = jnp.where(first, a, pltpu.roll(b, half, 1))
        right = jnp.where(first, pltpu.roll(a, half, 1), b)
        parts.append(jnp.take_along_axis(left, index, axis=1))
        parts.append(jnp.take_along_axis(right, index, axis=1))
    return jnp.concatenate(parts, axis=1)


def doubled_columns(parent, cols):
    rows = parent.shape[0]
    lane = iota((rows, LANES), 1)
    even = (lane & 1) == 0
    parts = []
    for c in range(cols // LANES):
        index = (c % 2) * (LANES // 2) + (lane >> 1)
        from_lanes = parent[:, (c // 2) * LANES : (c // 2 + 1) * LANES]
        parts.append(jnp.take_along_axis(from_lanes, index, axis=1))
    evens = jnp.concatenate([jnp.where(even, p, 0.0) for p in parts], axis=1)
    odds = jnp.concatenate([jnp.where(even, 0.0, p) for p in parts], axis=1)
    return split2(jnp.concatenate([evens, odds], axis=0))


def joined(fresh, doubled):
    high, low = split2(fresh)
    up_high, up_low = doubled
    return jnp.concatenate([high, up_high, low, up_low, high, up_high], axis=0)


def fine_kernel(middle, noise, weights, field, zface, yface, carry_z, carry_y):
    count = noise.shape[0]
    cols = noise.shape[3]
    tiles = noise.shape[2] // TILE
    depth_step, row_step = pl.program_id(0), pl.program_id(1)

    @pl.when(depth_step == 0)
    def _():
        carry_z[row_step] = jnp.zeros(carry_z.shape[1:], F32)

    @pl.when(row_step == 0)
    def _():
        carry_y[...] = jnp.zeros_like(carry_y)

    end_row = iota((TILE, cols), 0) == TILE - 1
    edges = [carry_y[0], carry_y[1]]
    for j in reversed(range(tiles)):
        doubled = doubled_columns(middle[0, j], cols)
        above = carry_z[row_step, j]
        for octz in (1, 0):
            fresh = noise[:, octz, j * TILE : (j + 1) * TILE, :].reshape(count * TILE, cols)
            result = dot(weights[octz], joined(fresh, doubled))
            at = 0

            def take(size):
                nonlocal at
                at += size
                return result[at - size : at]

            rows = slice(2 * TILE * j, 2 * TILE * (j + 1))
            for half in range(2):
                field[2 * octz + half, rows] = interleave(take(2 * TILE), take(2 * TILE))
            top = take(4 * TILE) + above
            zface[octz, rows] = interleave(top[: 2 * TILE], top[2 * TILE :])
            above = take(4 * TILE)
            for half in range(2):
                pair = []
                for side in range(2):
                    k = TILE * side + half
                    edge = edges[octz][k : k + 1, :]
                    pair.append(take(TILE) + jnp.where(end_row, edge, 0.0))
                yface[2 * octz + half, TILE * j : TILE * (j + 1)] = interleave(*pair)
            edges[octz] = take(2 * TILE)
        carry_z[row_step, j] = above
    for octz in range(2):
        carry_y[octz] = edges[octz]


def seam_kernel(lower, south, zface, yface, z_out, y_out):
    rows = zface.shape[1] // lower.shape[0]
    for t in range(lower.shape[0]):
        block = lower[t]
        at = slice(t * rows, (t + 1) * rows)
        z_out[0, at] = zface[0, at] + interleave(block[:rows], block[rows:])
    last = yface.shape[1] - 1
    end_row = iota(yface.shape[1:], 0) == last
    for plane in range(south.shape[0]):
        edge = interleave(south[plane, :TILE], south[plane, TILE:])
        for half in range(2):
            y_out[2 * plane + half] = yface[2 * plane + half] + jnp.where(
                end_row, edge[half : half + 1], 0.0
            )


def fine_rows():
    table, index = [], {}

    def entry(point, scale):
        key = (point, scale)
        if key not in index:
            index[key] = len(table)
            table.append(scale * basis_row(point))
        return index[key]

    halves = [-0.5, 0.5]
    rows = []
    for pz in halves:
        for px in halves:
            for y in range(TILE):
                for py in halves:
                    rows.append([(entry((pz, py, px), 1.0), y)])
    for w in (1.0, -1.0):
        for px in halves:
            for y in range(TILE):
                for py in halves:
                    rows.append([(entry((w, py, px), 0.5), y)])
    for pz in halves:
        for px in halves:
            for y in range(TILE):
                terms = [(entry((pz, 1.0, px), 0.5), y)]
                if y + 1 < TILE:
                    terms.append((entry((pz, -1.0, px), 0.5), y + 1))
                rows.append(terms)
    for px in halves:
        for pz in halves:
            rows.append([(entry((pz, -1.0, px), 0.5), 0)])
        rows.extend([[]] * (TILE - 2))
    return np.array(table), rows


def layout_of(rows, count, parent_columns):
    columns = count * TILE + 2 * len(parent_columns)
    place = np.zeros((3, LANES, columns), np.float32)
    at_y = np.zeros((columns,), np.int64)
    for k in range(count):
        for y in range(TILE):
            place[0, k, k * TILE + y] = 1
            at_y[k * TILE + y] = y
    for block in (1, 2):
        for i, (k, y) in enumerate(parent_columns):
            c = count * TILE + (block - 1) * len(parent_columns) + i
            at_y[c] = y
            if k < count:
                place[block, k, c] = 1
    noise = np.arange(columns) < count * TILE
    terms = max(len(r) for r in rows)
    pick = np.zeros((terms, len(rows), LANES), np.float32)
    mask = np.zeros((terms, len(rows), columns), np.float32)
    for term in range(terms):
        for i, row in enumerate(rows):
            if term < len(row):
                q, y = row[term]
                pick[term, i, (y % 2) * (LANES // 2) + q] = 1
                mask[term, i] = np.where(noise, at_y == y, at_y == y // 2)
    return tuple(jnp.asarray(a, BF16) for a in (pick, mask, place.reshape(3 * LANES, columns)))


def shards(n_slab, n_pencil, owner_map, window_start, child_maps, innovation, bank,
           noise_middle, noise_finest):
    count = innovation.shape[0]
    padded = round_up(count, 8)
    total = bank.shape[2]
    owner = owner_map[window_start[0] + LAST]
    smem = pl.BlockSpec(memory_space=pltpu.SMEM)
    vmem = pl.BlockSpec(memory_space=pltpu.VMEM)
    top = Region(LAST, n_slab, n_pencil)
    under = Region(LAST - 1, n_slab, n_pencil)

    rows3 = bank.reshape(count, 1, total)
    head_width = offset_of(LAST) // LANES * LANES + LANES
    head = bank[0, :, :head_width]
    table, row_list = fine_rows()
    half = TILE // 2
    fine_columns = [(k, y) for k in range(count) for y in range(half)]
    fine_parts = layout_of(row_list, count, fine_columns)
    mid_columns = [(k, y) for y in range(half) for k in range(padded)]
    mid_list = [[(k, h * half + y)] for h in range(2) for k in range(count) for y in range(half)]
    mid_parts = layout_of(mid_list, count, mid_columns)
    fine_k, mid_k = fine_parts[1].shape[2], mid_parts[1].shape[2]

    partial, tail, fine_weights, mid_weights = pl.pallas_call(
        functools.partial(head_kernel, n_slab, n_pencil),
        grid=(1,),
        in_specs=[
            smem,
            smem,
            vmem,
            pl.BlockSpec((count, 1, LANES), lambda i: (0, 0, total // LANES)),
        ]
        + [vmem] * 9,
        out_specs=[vmem] * 4,
        out_shape=[
            jax.ShapeDtypeStruct((under.side, packed_rows(count, under.part), LANES), F32),
            jax.ShapeDtypeStruct((count, 1, LANES), F32),
            jax.ShapeDtypeStruct((2, len(row_list), 3 * fine_k), BF16),
            jax.ShapeDtypeStruct((2, len(mid_list) + round_up(padded, 16), 3 * mid_k), BF16),
        ],
        scratch_shapes=[
            pltpu.VMEM((8, padded, LANES), F32),
            pltpu.VMEM((padded, LANES), F32),
            pltpu.VMEM((padded, head_width), F32),
        ],
        compiler_params=pltpu.CompilerParams(vmem_limit_bytes=20 * MIB),
        name="head",
    )(owner_map, window_start, head, rows3, child_maps.transpose(1, 0, 2), innovation,
      jnp.asarray(np.pad(table, ((0, 0), (0, LANES - count))), F32), *fine_parts, *mid_parts)

    fresh, gathered = lax.switch(
        owner,
        [functools.partial(share, o, n_slab, n_pencil, count) for o in range(n_slab)],
        rows3, tail, partial,
    )

    _, planes, rows, cols = noise_middle.shape
    per = planes // top.nz
    tiles = 2 * rows // TILE
    _, fine_planes, fine_y, fine_x = noise_finest.shape
    out_x = 2 * fine_x
    in_hbm = pltpu.with_memory_space_constraint(noise_finest, pltpu.HBM)
    middle, lower, south = pl.pallas_call(
        functools.partial(middle_kernel, n_slab, n_pencil, per),
        grid=(planes,),
        in_specs=[
            pl.BlockSpec(gathered.shape, lambda z: (0, 0, 0)),
            pl.BlockSpec(fresh.shape, lambda z: (0, 0, 0, 0)),
            pl.BlockSpec((count, 1, rows, cols), lambda z: (0, z, 0, 0)),
            vmem,
            pl.BlockSpec((count, 1, fine_y, fine_x), lambda z: (0, 0, 0, 0)),
            pl.BlockSpec((count, 2, TILE, fine_x), lambda z: (0, z, 0, 0)),
            vmem,
        ],
        out_specs=[
            pl.BlockSpec((1, tiles, count * half, cols), lambda z: (z, 0, 0, 0)),
            pl.BlockSpec((tiles, 4 * TILE, fine_x), lambda z: (0, 0, 0)),
            pl.BlockSpec((2, 2 * TILE, fine_x), lambda z: (z, 0, 0)),
        ],
        out_shape=[
            jax.ShapeDtypeStruct((planes, tiles, count * half, cols), F32),
            jax.ShapeDtypeStruct((tiles, 4 * TILE, fine_x), F32),
            jax.ShapeDtypeStruct((fine_planes, 2 * TILE, fine_x), F32),
        ],
        scratch_shapes=[pltpu.VMEM((top.nz, padded, top.part), F32)],
        cost_estimate=pl.CostEstimate(
            flops=MID_FLOPS, bytes_accessed=4 * noise_middle.size, transcendentals=0
        ),
        compiler_params=pltpu.CompilerParams(vmem_limit_bytes=24 * MIB),
        name="middle",
    )(gathered, fresh, noise_middle, mid_weights, in_hbm, in_hbm,
      fine_weights)
    above = shifted(lower, "slab", -1)
    beside = shifted(south, "pencil", -1)

    deep = 64
    nz, ny = planes, fine_y // deep
    each = deep // TILE

    def block(*where):
        def index(z, y):
            at = {"z": nz - 1 - z, "y": ny - 1 - y}
            return tuple(at.get(w, 0) for w in where)

        return index

    field, zface, yface = pl.pallas_call(
        fine_kernel,
        grid=(nz, ny),
        in_specs=[
            pl.BlockSpec((1, each, count * half, cols), block("z", "y", 0, 0)),
            pl.BlockSpec((count, 2, deep, fine_x), block(0, "z", "y", 0)),
            vmem,
        ],
        out_specs=[
            pl.BlockSpec((4, 2 * deep, out_x), block("z", "y", 0)),
            pl.BlockSpec((2, 2 * deep, out_x), block("z", "y", 0)),
            pl.BlockSpec((4, deep, out_x), block("z", "y", 0)),
        ],
        out_shape=[
            jax.ShapeDtypeStruct((2 * fine_planes, 2 * fine_y, out_x), F32),
            jax.ShapeDtypeStruct((fine_planes, 2 * fine_y, out_x), F32),
            jax.ShapeDtypeStruct((2 * fine_planes, fine_y, out_x), F32),
        ],
        scratch_shapes=[
            pltpu.VMEM((ny, each, 4 * TILE, fine_x), F32),
            pltpu.VMEM((2, 2 * TILE, fine_x), F32),
        ],
        cost_estimate=pl.CostEstimate(
            flops=2 * nz * (fine_y // TILE) * fine_weights.size * fine_x,
            bytes_accessed=4 * (noise_finest.size + 16 * fine_planes * fine_y * fine_x),
            transcendentals=0,
        ),
        compiler_params=pltpu.CompilerParams(vmem_limit_bytes=24 * MIB),
        name="fine",
    )(middle, noise_finest, fine_weights)
    z_spec = pl.BlockSpec((1, 2 * fine_y, out_x), lambda i: (fine_planes - 1, 0, 0))
    y_spec = pl.BlockSpec((2 * fine_planes, TILE, out_x), lambda i: (0, fine_y // TILE - 1, 0))
    zface, yface = pl.pallas_call(
        seam_kernel,
        grid=(1,),
        in_specs=[
            pl.BlockSpec(above.shape, lambda i: (0, 0, 0)),
            pl.BlockSpec(beside.shape, lambda i: (0, 0, 0)),
            z_spec,
            y_spec,
        ],
        out_specs=[z_spec, y_spec],
        out_shape=[
            jax.ShapeDtypeStruct(zface.shape, F32),
            jax.ShapeDtypeStruct(yface.shape, F32),
        ],
        input_output_aliases={2: 0, 3: 1},
        compiler_params=pltpu.CompilerParams(vmem_limit_bytes=8 * MIB),
        name="seam",
    )(above, beside, zface, yface)
    return field, zface, yface


def solution(mesh):
    placed = (
        P(),
        P(),
        P(),
        P(),
        P("slab", None, None),
        P(None, "slab", "pencil", None),
        P(None, "slab", "pencil", None),
    )
    return jax.shard_map(
        functools.partial(shards, mesh.shape["slab"], mesh.shape["pencil"]),
        mesh=mesh,
        in_specs=placed,
        out_specs=(P("slab", "pencil", None), P("slab", "pencil", None), P("slab", "pencil", None)),
        check_vma=False,
    )
```

```python
import functools
import math

import jax
import jax.numpy as jnp
import numpy as np
from jax import lax
from jax.experimental import pallas as pl
from jax.experimental.pallas import tpu as pltpu
from jax.sharding import PartitionSpec as P

LEVELS = 8
ROOTS = 2
BANKS = LEVELS - 2
LAST = BANKS - 1
LANES = 128
TILE = 8
BOTTOM = 12
MIB = 1 << 20
SHARE_FLOPS = 20 * 10**9
SHARE_BYTES = 80 * 10**6
MID_FLOPS = 6 * 10**9
F32 = jnp.float32
BF16 = jnp.bfloat16
MESH = pl.DeviceIdType.MESH


def legendre(order, point):
    values = [1.0, point, 1.5 * point * point - 0.5, 2.5 * point * point * point - 1.5 * point]
    return values[order]


def basis_row(point):
    w_coord, v_coord, u_coord = point
    entry = []
    for deg_x in range(4):
        for deg_y in range(4):
            for deg_z in range(4):
                if deg_x + deg_y + deg_z <= 3:
                    factor = math.sqrt((2 * deg_x + 1) * (2 * deg_y + 1) * (2 * deg_z + 1))
                    entry.append(
                        factor
                        * legendre(deg_x, u_coord)
                        * legendre(deg_y, v_coord)
                        * legendre(deg_z, w_coord)
                    )
    return np.array(entry)


def shifted(block, axis, distance):
    devices = range(lax.axis_size(axis))
    route = [((i - distance) % len(devices), i) for i in devices]
    return lax.ppermute(block, axis, route)


def offset_of(level):
    return ROOTS * (8**level - 1) // 7


def round_up(size, unit):
    return -(-size // unit) * unit


def log2(n):
    return n.bit_length() - 1


class Region:
    def __init__(self, level, n_slab, n_pencil):
        side = 2**level
        self.level = level
        self.side = side
        self.nx = ROOTS * side
        self.ny = side // n_pencil
        self.nz = max(1, side // n_slab)
        self.plane = side * self.nx
        self.part = self.ny * self.nx
        self.n_slab = n_slab

    def first_plane(self, slab):
        return (slab * self.side) // self.n_slab


def split2(value):
    high = value.astype(BF16)
    low = (value - high.astype(F32)).astype(BF16)
    return high, low


def split3(value):
    high, low = split2(value)
    rest = value - high.astype(F32) - low.astype(F32)
    return jnp.concatenate([high.astype(F32), low.astype(F32), rest], axis=0).astype(BF16)


def dot(left, right):
    return jnp.dot(left, right, preferred_element_type=F32)


def exact(left, right):
    left_high, left_low = split2(left)
    right_high, right_low = split2(right)
    return dot(left_high, right_high) + (dot(left_low, right_high) + dot(left_high, right_low))


def chosen(pick, value):
    high, low = split2(value)
    return dot(pick, high) + dot(pick, low)


def placed_at(value, place):
    high, low = split2(value)
    return dot(high, place) + dot(low, place)


def stacked(value):
    high, low = split2(value)
    return jnp.concatenate([high, low, high], axis=0)


def picked(parent, pick):
    rows = parent.shape[0]
    up = dot(split3(parent), pick)
    return up[:rows] + up[rows : 2 * rows] + up[2 * rows :]


def spread(up, octant, names):
    return [jnp.where(octant == o, up, 0.0) for o in names]


def iota(shape, dim):
    return lax.broadcasted_iota(jnp.int32, shape, dim)


def packed(value, count):
    full, short = count // 8 * 8, count % 8
    tiles = [value[:, t * LANES : (t + 1) * LANES] for t in range(value.shape[1] // LANES)]
    if not 0 < short <= 4:
        return jnp.concatenate(tiles, axis=0)
    row = iota((8, LANES), 0)
    ends = [
        jnp.where(row < 4, a[full:], pltpu.roll(b[full:], 4, 0))
        for a, b in zip(tiles[::2], tiles[1::2])
    ]
    return jnp.concatenate([t[:full] for t in tiles] + ends, axis=0)


def unpacked(value, count, tiles):
    full, short = count // 8 * 8, count % 8
    rows = round_up(count, 8)
    if not 0 < short <= 4:
        return jnp.concatenate([value[t * rows : (t + 1) * rows] for t in range(tiles)], axis=1)
    row = iota((8, LANES), 0)
    parts = []
    for t in range(tiles):
        at = full * tiles + 8 * (t // 2)
        end = value[at : at + 8]
        if t % 2:
            end = pltpu.roll(end, 4, 0)
        end = jnp.where(row < 4, end, 0.0)
        parts.append(jnp.concatenate([value[t * full : (t + 1) * full], end], axis=0))
    return jnp.concatenate(parts, axis=1)


def packed_rows(count, width):
    tiles = width // LANES
    if not 0 < count % 8 <= 4:
        return tiles * round_up(count, 8)
    return tiles * (count // 8 * 8) + 8 * (tiles // 2)


def deepened(value, rows):
    return jnp.concatenate(
        [value, jnp.zeros((rows - value.shape[0], value.shape[1]), F32)], axis=0
    )


def weave(table_terms, mask, place, table, innovation, maps, octz):
    both = []
    for octy in range(2):
        o = 4 * octz + 2 * octy
        wide = placed_at(jnp.concatenate([innovation, maps[o], maps[o + 1]], axis=1), place[...])
        if table is not None:
            wide = exact(table, deepened(wide, LANES))
        both.append(deepened(wide, LANES // 2))
    both = jnp.concatenate(both, axis=0)
    total = 0.0
    for term in range(table_terms.shape[0]):
        total = total + chosen(table_terms[term], both) * mask[term].astype(F32)
    high, low = split2(total)
    return jnp.concatenate([high, high, low], axis=1)


def head_kernel(n_slab, n_pencil, owner_map, window_start, bank, end, child_maps, innovation,
                table, fine_rows, fine_mask, fine_place, mid_rows, mid_mask, mid_place,
                partial, tail, fine_w, mid_w, maps, inner, head):
    rows = head.shape[0]
    count = innovation.shape[0]
    head[count // 8 * 8 :, :] = jnp.zeros((rows - count // 8 * 8, head.shape[1]), F32)
    head[:count, :] = bank[:, 0, :]
    slab, pencil = lax.axis_index("slab"), lax.axis_index("pencil")

    def owned(level):
        return owner_map[window_start[0] + level] == slab

    tail[...] = end[...]
    maps[...] = jnp.zeros_like(maps)
    inner[...] = jnp.zeros_like(inner)
    for o in range(8):
        maps[o, :count, :count] = child_maps[:, o, :]
    inner[:count, :count] = innovation[...]
    quad = 4 * rows
    blocks = []
    for octz in range(2):
        block = 0.0
        for o in range(4):
            block = block + pltpu.roll(maps[4 * octz + o], o * rows, 1)
        blocks.append(block[:, :quad])
    flat = jnp.concatenate(blocks + [inner[:, :rows]], axis=1)
    w_high, w_low = split2(flat)
    w_all = jnp.concatenate([w_high, w_high, w_low], axis=1)
    lane = iota((rows, LANES), 1)
    last = LAST - 1

    def unshifted(at, shift):
        if shift == 0:
            return head[:, pl.ds(at, LANES)]
        left = pltpu.roll(head[:, pl.ds(at, LANES)], LANES - shift, 1)
        right = pltpu.roll(head[:, pl.ds(at + LANES, LANES)], LANES - shift, 1)
        return jnp.where(lane < LANES - shift, left, right)

    parent = None
    for level in range(last):
        side, nx = 2**level, ROOTS * 2**level
        cells = side * side * nx
        padded = round_up(cells, LANES)
        first = offset_of(level)
        shift = first % LANES
        noise = jnp.concatenate(
            [unshifted(first - shift + t * LANES, shift) for t in range(padded // LANES)], axis=1
        )
        noise = jnp.where(owned(level), noise, 0.0)
        if cells < padded:
            noise = jnp.where(iota((rows, padded), 1) < cells, noise, 0.0)
        if parent is None:
            up = jnp.zeros((rows, padded), F32)
        else:
            q = parent.shape[1]
            half = nx // 2

            def source_of(shape):
                cell = iota(shape, 1)
                x = cell & (nx - 1)
                y = (cell >> log2(nx)) & (side - 1)
                z = cell >> log2(nx * side)
                return x, y, z

            x, y, z = source_of((q, padded))
            source = ((z >> 1) * (side // 2) + (y >> 1)) * half + (x >> 1)
            pick = jnp.where(iota((q, padded), 0) == source, 1.0, 0.0).astype(BF16)
            up = picked(parent, pick)
        cell = iota((rows, padded), 1)
        octant = (
            4 * ((cell >> log2(nx * side)) & 1) + 2 * ((cell >> log2(nx)) & 1) + (cell & 1)
        )
        stack = jnp.concatenate(spread(up, octant, range(8)) + [noise], axis=0)
        parent = dot(w_all, stacked(stack))[:rows]

    r = Region(last, n_slab, n_pencil)
    half = r.nx // 2
    plane = (r.side // 2) * half
    cell = iota((plane, r.part), 1)
    y = (cell >> log2(r.nx)) + pencil * r.ny
    source = (y >> 1) * half + ((cell & (r.nx - 1)) >> 1)
    pick = jnp.where(iota((plane, r.part), 0) == source, 1.0, 0.0).astype(BF16)
    pieces = [split3(parent[:, z * plane : (z + 1) * plane]) for z in range(r.side // 2)]
    ups = dot(jnp.concatenate(pieces, axis=0), pick)
    cell = iota((rows, r.part), 1)
    octant = 2 * ((cell >> log2(r.nx)) & 1) + (cell & 1)
    first = offset_of(last)
    shift = first % LANES
    chain_w = []
    for octz in range(2):
        w = jnp.concatenate([blocks[octz], inner[:, :rows]], axis=1)
        high, low = split2(w)
        chain_w.append(jnp.concatenate([high, high, low], axis=1))
    for z in range(r.side):
        at = (z // 2) * 3 * rows
        up = ups[at : at + rows] + ups[at + rows : at + 2 * rows] + ups[at + 2 * rows : at + 3 * rows]
        start = first - shift + z * r.plane
        noise = jnp.concatenate(
            [
                unshifted(pl.multiple_of(start + pencil * r.part + t * LANES, LANES), shift)
                for t in range(r.part // LANES)
            ],
            axis=1,
        )
        noise = jnp.where(owned(last), noise, 0.0)
        stack = jnp.concatenate(spread(up, octant, range(4)) + [noise], axis=0)
        partial[z] = packed(dot(chain_w[z % 2], stacked(stack))[:rows], count)

    for octz in range(2):
        fine_w[octz] = weave(fine_rows, fine_mask, fine_place, table[...], inner[...], maps, octz)
        deep = chain_w[octz].shape[1]
        mid_w[octz, : mid_rows.shape[1]] = weave(mid_rows, mid_mask, mid_place, None, inner[...], maps, octz)
        mid_w[octz, mid_rows.shape[1] : mid_rows.shape[1] + rows, :deep] = chain_w[octz]


def routes(owner, n_slab, nz):
    inner = 4
    others = [d for d in range(n_slab) if d != owner]
    if n_slab != inner * inner:
        return {(d, z): None for d in others for z in range(nz)}
    own_z, own_p = divmod(owner, inner)

    def link(dest):
        z, p = divmod(dest, inner)
        if z != own_z:
            return "up" if z > own_z else "down"
        return "x" if (p ^ own_p) & 1 else "y"

    def options(dest):
        p = dest % inner
        found = [(None, link(dest))]
        for bit, name in ((1, "x"), (2, "y")):
            relay = own_z * inner + (own_p ^ bit)
            if relay != dest and (p ^ own_p) & bit:
                found.append((relay, name))
        return found

    load, via = {}, {}
    for d in others:
        load[link(d)] = load.get(link(d), 0) + 0.11 * nz
    for d in sorted(others, key=lambda d: (len(options(d)), d)):
        for z in range(nz):
            relay, name = min(
                options(d), key=lambda t: load.get(t[1], 0) + (0 if t[0] is None else 0.01)
            )
            load[name] = load.get(name, 0) + 1
            via[d, z] = relay
    return via


def share_kernel(owner, n_slab, n_pencil, bank, tail, partial, fresh, gathered, relay,
                 send, recv, own, to_relay, onward, give, take, keep):
    r = Region(LAST, n_slab, n_pencil)
    r4 = Region(LAST - 1, n_slab, n_pencil)
    me, pencil = lax.axis_index("slab"), lax.axis_index("pencil")
    base = offset_of(LAST) // LANES * LANES
    via = routes(owner, n_slab, r.nz)
    relayed = [k for k in via if via[k] is not None]
    direct = [k for k in via if via[k] is None]
    slots = {}
    for k in relayed:
        slots[k] = sum(1 for e in slots if via[e] == via[k])

    def at(d):
        return {"slab": d}

    barrier = pltpu.get_barrier_semaphore()

    def greet(i, _):
        pl.semaphore_signal(
            barrier, inc=1, device_id=at(lax.rem(me + i, n_slab)), device_id_type=MESH
        )
        return 0

    lax.fori_loop(1, n_slab, greet, 0)
    pl.semaphore_wait(barrier, n_slab - 1)

    def source(d, z, size):
        start = base + (r.first_plane(d) + z) * r.plane + pencil * r.part
        return bank.at[:, :, pl.ds(pl.multiple_of(start, LANES), size)]

    def body(ref):
        return ref.at[:, :, pl.ds(0, r.part)]

    def rest(ref):
        return ref.at[:, :, pl.ds(r.part, LANES)]

    def remote(src, dst, ssem, rsem, d):
        return pltpu.make_async_remote_copy(
            src, dst, ssem, rsem, device_id=at(d), device_id_type=MESH
        )

    def start_pieces(d, z, dst, begin):
        plane = r.first_plane(d) + z
        whole = lambda: begin(source(d, z, r.part + LANES), dst)
        if isinstance(d, int) and plane < r.side - 1:
            whole()
            return
        ends = jnp.logical_and(plane == r.side - 1, pencil == n_pencil - 1)

        @pl.when(ends)
        def _():
            begin(source(d, z, r.part), body(dst))
            begin(tail, rest(dst))

        pl.when(jnp.logical_not(ends))(whole)

    def start_block(d, z):
        if isinstance(d, int) and via[d, z] is not None:
            slot = slots[d, z]
            dst, rsem, to = relay.at[slot], to_relay.at[slot], via[d, z]
        else:
            dst, rsem, to = fresh.at[z], recv.at[z], d
        start_pieces(d, z, dst, lambda src, ref: remote(src, ref, send.at[d, z], rsem, to).start())

    def drain_block(d, z):
        remote(fresh.at[z], fresh.at[z], send.at[d, z], recv.at[z], d).wait_send()

    def landed(dst, rsem, d):
        remote(dst, dst, send.at[0, 0], rsem, d).wait_recv()

    def forward(d, z):
        slot = slots[d, z]
        return remote(relay.at[slot], fresh.at[z], onward.at[slot], recv.at[z], d)

    @pl.when(me == owner)
    def _():
        if relayed:
            for d, z in relayed + direct:
                start_block(d, z)
        else:

            def step(i, _):
                for z in range(r.nz):
                    start_block(lax.rem(owner + i, n_slab), z)
                return 0

            lax.fori_loop(1, n_slab, step, 0)
        for z in range(r.nz):
            start_pieces(
                owner,
                z,
                fresh.at[z],
                lambda src, ref: pltpu.make_async_copy(src, ref, own.at[z]).start(),
            )

    def piece(d):
        return partial.at[r4.first_plane(d)]

    def give_one(i, _):
        d = lax.rem(me + i, n_slab)
        remote(piece(d), gathered.at[me], give.at[d], take.at[me], d).start()
        return 0

    lax.fori_loop(1, n_slab, give_one, 0)
    mine = pltpu.make_async_copy(piece(me), gathered.at[me], keep)
    mine.start()

    for hub in sorted({via[k] for k in relayed}):

        @pl.when(me == hub)
        def _():
            group = [k for k in relayed if via[k] == hub]
            for d, z in group:
                landed(relay.at[slots[d, z]], to_relay.at[slots[d, z]], owner)
                forward(d, z).start()
            for d, z in group:
                forward(d, z).wait_send()

    @pl.when(me != owner)
    def _():
        for z in range(r.nz):
            landed(fresh.at[z], recv.at[z], owner)

    @pl.when(me == owner)
    def _():
        if relayed:
            for d, z in relayed + direct:
                drain_block(d, z)
        else:

            def step(i, _):
                for z in range(r.nz):
                    drain_block(lax.rem(owner + i, n_slab), z)
                return 0

            lax.fori_loop(1, n_slab, step, 0)
        for z in range(r.nz):
            pltpu.make_async_copy(relay.at[0], fresh.at[z], own.at[z]).wait()

    def take_one(i, _):
        d = lax.rem(me + i, n_slab)
        remote(piece(d), gathered.at[d], give.at[d], take.at[d], d).wait()
        return 0

    lax.fori_loop(1, n_slab, take_one, 0)
    mine.wait()


def share(owner, n_slab, n_pencil, count, bank, tail, partial):
    r = Region(LAST, n_slab, n_pencil)
    block = (r.nz, count, 1, r.part + LANES)
    via = routes(owner, n_slab, r.nz)
    hubs = [v for v in via.values() if v is not None]
    slots = max([hubs.count(h) for h in hubs], default=1)
    dma = pltpu.SemaphoreType.DMA
    anywhere = pl.BlockSpec(memory_space=pl.ANY)
    return pl.pallas_call(
        functools.partial(share_kernel, owner, n_slab, n_pencil),
        in_specs=[anywhere] * 3,
        out_specs=[anywhere] * 2,
        out_shape=[
            jax.ShapeDtypeStruct(block, F32),
            jax.ShapeDtypeStruct((n_slab, *partial.shape[1:]), F32),
        ],
        scratch_shapes=[
            pltpu.VMEM((slots, *block[1:]), F32),
            dma((n_slab, r.nz)),
            dma((r.nz,)),
            dma((r.nz,)),
            dma((slots,)),
            dma((slots,)),
            dma((n_slab,)),
            dma((n_slab,)),
            dma,
        ],
        cost_estimate=pl.CostEstimate(
            flops=SHARE_FLOPS, bytes_accessed=SHARE_BYTES, transcendentals=0
        ),
        compiler_params=pltpu.CompilerParams(
            collective_id=owner, has_side_effects=True, vmem_limit_bytes=8 * MIB
        ),
        name="share",
    )(bank, tail, partial)


def middle_kernel(n_slab, n_pencil, per, gathered, fresh, noise, weights,
                  fine_plane, fine_row, fine_w, out, lower, south, last_coarse):
    r = Region(LAST, n_slab, n_pencil)
    q = Region(LAST - 1, n_slab, n_pencil)
    count = noise.shape[0]
    rows = round_up(count, 8)
    step = pl.program_id(0)
    slab = lax.axis_index("slab")

    @pl.when(step == 0)
    def _():
        parent = gathered[0]
        for d in range(1, gathered.shape[0]):
            parent = parent + gathered[d]
        parent = unpacked(parent, count, q.part // LANES)
        cell = iota((q.part, r.part), 1)
        source = (cell >> (log2(r.nx) + 1)) * q.nx + ((cell & (r.nx - 1)) >> 1)
        pick = jnp.where(iota((q.part, r.part), 0) == source, 1.0, 0.0).astype(BF16)
        up = picked(parent, pick)
        cell = iota((rows, r.part), 1)
        octant = 2 * ((cell >> log2(r.nx)) & 1) + (cell & 1)
        spreads = spread(up, octant, range(4))
        shift = offset_of(LAST) % LANES
        lane = iota((count, LANES), 1)
        for z in range(r.nz):
            raw = fresh[z, :, 0, :]
            rolled = [
                pltpu.roll(raw[:, t * LANES : (t + 1) * LANES], LANES - shift, 1)
                for t in range(r.part // LANES + 1)
            ]
            block = jnp.concatenate(
                [
                    jnp.where(lane < LANES - shift, rolled[t], rolled[t + 1])
                    for t in range(r.part // LANES)
                ],
                axis=1,
            )
            last_coarse[z] = jnp.zeros_like(last_coarse[z])
            last_coarse[z, :count, :] = block
            stack = jnp.concatenate(spreads + [last_coarse[z]], axis=0)
            octz = (r.first_plane(slab) + z) & 1
            chain_w = weights[octz, TILE * count : TILE * count + rows, : 15 * rows]
            last_coarse[z] = dot(chain_w, stacked(stack))[:rows]

    octz = lax.rem(slab * per * r.nz + step, 2)
    at = step // per
    wide = noise.shape[3]
    lane = iota((rows, LANES), 1)
    even = (lane & 1) == 0
    half = TILE // 2
    across = LANES // r.nx

    def parents(t):
        pieces = []
        for yy in range(half):
            y = t * half + yy
            cells = last_coarse[at, :, (y // across) * LANES : (y // across + 1) * LANES]
            index = (y % across) * r.nx + (lane >> 1)
            pieces.append(jnp.take_along_axis(cells, index, axis=1))
        return [jnp.where(even, p, 0.0) for p in pieces] + [jnp.where(even, 0.0, p) for p in pieces]

    group = 2
    for j in range(noise.shape[2] // (TILE * group)):
        columns = []
        for g in range(group):
            t = j * group + g
            fresh_part = noise[:, 0, t * TILE : (t + 1) * TILE, :].reshape(count * TILE, wide)
            columns.append(jnp.concatenate([fresh_part] + parents(t), axis=0))
        result = dot(weights[octz, : TILE * count], stacked(jnp.concatenate(columns, axis=1)))
        size = count * half
        for g in range(group):
            for h in range(2):
                out[0, (j * group + g) * 2 + h] = result[
                    h * size : (h + 1) * size, g * wide : (g + 1) * wide
                ]

    cols = fine_row.shape[3]
    edges = 2 * TILE
    ends = fine_w.shape[1]
    doubled = doubled_columns(out[0, 0], cols)
    for octz in range(2):
        fresh_part = fine_row[:, octz].reshape(count * TILE, cols)
        south[octz] = dot(fine_w[octz, ends - edges :], joined(fresh_part, doubled))

    @pl.when(step == 0)
    def _():
        for t in range(out.shape[1]):
            fresh_part = fine_plane[:, 0, t * TILE : (t + 1) * TILE, :].reshape(count * TILE, cols)
            lower[t] = dot(
                fine_w[0, BOTTOM * TILE : (BOTTOM + 4) * TILE],
                joined(fresh_part, doubled_columns(out[0, t], cols)),
            )


def interleave(even, odd):
    rows, cols = even.shape
    lane = iota((rows, LANES), 1)
    half = LANES // 2
    first = lane < half
    index = (lane >> 1) + (lane & 1) * half
    parts = []
    for j in range(cols // LANES):
        a = even[:, j * LANES : (j + 1) * LANES]
        b = odd[:, j * LANES : (j + 1) * LANES]
        left = jnp.where(first, a, pltpu.roll(b, half, 1))
        right = jnp.where(first, pltpu.roll(a, half, 1), b)
        parts.append(jnp.take_along_axis(left, index, axis=1))
        parts.append(jnp.take_along_axis(right, index, axis=1))
    return jnp.concatenate(parts, axis=1)


def doubled_columns(parent, cols):
    rows = parent.shape[0]
    lane = iota((rows, LANES), 1)
    even = (lane & 1) == 0
    parts = []
    for c in range(cols // LANES):
        index = (c % 2) * (LANES // 2) + (lane >> 1)
        from_lanes = parent[:, (c // 2) * LANES : (c // 2 + 1) * LANES]
        parts.append(jnp.take_along_axis(from_lanes, index, axis=1))
    evens = jnp.concatenate([jnp.where(even, p, 0.0) for p in parts], axis=1)
    odds = jnp.concatenate([jnp.where(even, 0.0, p) for p in parts], axis=1)
    return split2(jnp.concatenate([evens, odds], axis=0))


def joined(fresh, doubled):
    high, low = split2(fresh)
    up_high, up_low = doubled
    return jnp.concatenate([high, up_high, low, up_low, high, up_high], axis=0)


def fine_kernel(middle, noise, weights, field, zface, yface, carry_z, carry_y):
    count = noise.shape[0]
    cols = noise.shape[3]
    tiles = noise.shape[2] // TILE
    depth_step, row_step = pl.program_id(0), pl.program_id(1)

    @pl.when(depth_step == 0)
    def _():
        carry_z[row_step] = jnp.zeros(carry_z.shape[1:], F32)

    @pl.when(row_step == 0)
    def _():
        carry_y[...] = jnp.zeros_like(carry_y)

    end_row = iota((TILE, cols), 0) == TILE - 1
    edges = [carry_y[0], carry_y[1]]
    for j in reversed(range(tiles)):
        doubled = doubled_columns(middle[0, j], cols)
        above = carry_z[row_step, j]
        for octz in (1, 0):
            fresh = noise[:, octz, j * TILE : (j + 1) * TILE, :].reshape(count * TILE, cols)
            result = dot(weights[octz], joined(fresh, doubled))
            at = 0

            def take(size):
                nonlocal at
                at += size
                return result[at - size : at]

            rows = slice(2 * TILE * j, 2 * TILE * (j + 1))
            for half in range(2):
                field[2 * octz + half, rows] = interleave(take(2 * TILE), take(2 * TILE))
            top = take(4 * TILE) + above
            zface[octz, rows] = interleave(top[: 2 * TILE], top[2 * TILE :])
            above = take(4 * TILE)
            for half in range(2):
                pair = []
                for side in range(2):
                    k = TILE * side + half
                    edge = edges[octz][k : k + 1, :]
                    pair.append(take(TILE) + jnp.where(end_row, edge, 0.0))
                yface[2 * octz + half, TILE * j : TILE * (j + 1)] = interleave(*pair)
            edges[octz] = take(2 * TILE)
        carry_z[row_step, j] = above
    for octz in range(2):
        carry_y[octz] = edges[octz]


def seam_kernel(lower, south, zface, yface, z_out, y_out):
    rows = zface.shape[1] // lower.shape[0]
    for t in range(lower.shape[0]):
        block = lower[t]
        at = slice(t * rows, (t + 1) * rows)
        z_out[0, at] = zface[0, at] + interleave(block[:rows], block[rows:])
    last = yface.shape[1] - 1
    end_row = iota(yface.shape[1:], 0) == last
    for plane in range(south.shape[0]):
        edge = interleave(south[plane, :TILE], south[plane, TILE:])
        for half in range(2):
            y_out[2 * plane + half] = yface[2 * plane + half] + jnp.where(
                end_row, edge[half : half + 1], 0.0
            )


def fine_rows():
    table, index = [], {}

    def entry(point, scale):
        key = (point, scale)
        if key not in index:
            index[key] = len(table)
            table.append(scale * basis_row(point))
        return index[key]

    halves = [-0.5, 0.5]
    rows = []
    for pz in halves:
        for px in halves:
            for y in range(TILE):
                for py in halves:
                    rows.append([(entry((pz, py, px), 1.0), y)])
    for w in (1.0, -1.0):
        for px in halves:
            for y in range(TILE):
                for py in halves:
                    rows.append([(entry((w, py, px), 0.5), y)])
    for pz in halves:
        for px in halves:
            for y in range(TILE):
                terms = [(entry((pz, 1.0, px), 0.5), y)]
                if y + 1 < TILE:
                    terms.append((entry((pz, -1.0, px), 0.5), y + 1))
                rows.append(terms)
    for px in halves:
        for pz in halves:
            rows.append([(entry((pz, -1.0, px), 0.5), 0)])
        rows.extend([[]] * (TILE - 2))
    return np.array(table), rows


def layout_of(rows, count, parent_columns):
    columns = count * TILE + 2 * len(parent_columns)
    place = np.zeros((3, LANES, columns), np.float32)
    at_y = np.zeros((columns,), np.int64)
    for k in range(count):
        for y in range(TILE):
            place[0, k, k * TILE + y] = 1
            at_y[k * TILE + y] = y
    for block in (1, 2):
        for i, (k, y) in enumerate(parent_columns):
            c = count * TILE + (block - 1) * len(parent_columns) + i
            at_y[c] = y
            if k < count:
                place[block, k, c] = 1
    noise = np.arange(columns) < count * TILE
    terms = max(len(r) for r in rows)
    pick = np.zeros((terms, len(rows), LANES), np.float32)
    mask = np.zeros((terms, len(rows), columns), np.float32)
    for term in range(terms):
        for i, row in enumerate(rows):
            if term < len(row):
                q, y = row[term]
                pick[term, i, (y % 2) * (LANES // 2) + q] = 1
                mask[term, i] = np.where(noise, at_y == y, at_y == y // 2)
    return tuple(jnp.asarray(a, BF16) for a in (pick, mask, place.reshape(3 * LANES, columns)))


def shards(n_slab, n_pencil, owner_map, window_start, child_maps, innovation, bank,
           noise_middle, noise_finest):
    count = innovation.shape[0]
    padded = round_up(count, 8)
    total = bank.shape[2]
    owner = owner_map[window_start[0] + LAST]
    smem = pl.BlockSpec(memory_space=pltpu.SMEM)
    vmem = pl.BlockSpec(memory_space=pltpu.VMEM)
    top = Region(LAST, n_slab, n_pencil)
    under = Region(LAST - 1, n_slab, n_pencil)

    rows3 = bank.reshape(count, 1, total)
    head_width = offset_of(LAST) // LANES * LANES + LANES
    table, row_list = fine_rows()
    half = TILE // 2
    fine_columns = [(k, y) for k in range(count) for y in range(half)]
    fine_parts = layout_of(row_list, count, fine_columns)
    mid_columns = [(k, y) for y in range(half) for k in range(padded)]
    mid_list = [[(k, h * half + y)] for h in range(2) for k in range(count) for y in range(half)]
    mid_parts = layout_of(mid_list, count, mid_columns)
    fine_k, mid_k = fine_parts[1].shape[2], mid_parts[1].shape[2]

    partial, tail, fine_weights, mid_weights = pl.pallas_call(
        functools.partial(head_kernel, n_slab, n_pencil),
        grid=(1,),
        in_specs=[
            smem,
            smem,
            pl.BlockSpec((count, 1, head_width), lambda i: (0, 0, 0)),
            pl.BlockSpec((count, 1, LANES), lambda i: (0, 0, total // LANES)),
        ]
        + [vmem] * 9,
        out_specs=[vmem] * 4,
        out_shape=[
            jax.ShapeDtypeStruct((under.side, packed_rows(count, under.part), LANES), F32),
            jax.ShapeDtypeStruct((count, 1, LANES), F32),
            jax.ShapeDtypeStruct((2, len(row_list), 3 * fine_k), BF16),
            jax.ShapeDtypeStruct((2, len(mid_list) + round_up(padded, 16), 3 * mid_k), BF16),
        ],
        scratch_shapes=[
            pltpu.VMEM((8, padded, LANES), F32),
            pltpu.VMEM((padded, LANES), F32),
            pltpu.VMEM((padded, head_width), F32),
        ],
        compiler_params=pltpu.CompilerParams(vmem_limit_bytes=20 * MIB),
        name="head",
    )(owner_map, window_start, rows3, rows3, child_maps.transpose(1, 0, 2), innovation,
      jnp.asarray(np.pad(table, ((0, 0), (0, LANES - count))), F32), *fine_parts, *mid_parts)

    fresh, gathered = lax.switch(
        owner,
        [functools.partial(share, o, n_slab, n_pencil, count) for o in range(n_slab)],
        rows3, tail, partial,
    )

    _, planes, rows, cols = noise_middle.shape
    per = planes // top.nz
    tiles = 2 * rows // TILE
    _, fine_planes, fine_y, fine_x = noise_finest.shape
    out_x = 2 * fine_x
    in_hbm = pltpu.with_memory_space_constraint(noise_finest, pltpu.HBM)
    middle, lower, south = pl.pallas_call(
        functools.partial(middle_kernel, n_slab, n_pencil, per),
        grid=(planes,),
        in_specs=[
            pl.BlockSpec(gathered.shape, lambda z: (0, 0, 0)),
            pl.BlockSpec(fresh.shape, lambda z: (0, 0, 0, 0)),
            pl.BlockSpec((count, 1, rows, cols), lambda z: (0, z, 0, 0)),
            vmem,
            pl.BlockSpec((count, 1, fine_y, fine_x), lambda z: (0, 0, 0, 0)),
            pl.BlockSpec((count, 2, TILE, fine_x), lambda z: (0, z, 0, 0)),
            vmem,
        ],
        out_specs=[
            pl.BlockSpec((1, tiles, count * half, cols), lambda z: (z, 0, 0, 0)),
            pl.BlockSpec((tiles, 4 * TILE, fine_x), lambda z: (0, 0, 0)),
            pl.BlockSpec((2, 2 * TILE, fine_x), lambda z: (z, 0, 0)),
        ],
        out_shape=[
            jax.ShapeDtypeStruct((planes, tiles, count * half, cols), F32),
            jax.ShapeDtypeStruct((tiles, 4 * TILE, fine_x), F32),
            jax.ShapeDtypeStruct((fine_planes, 2 * TILE, fine_x), F32),
        ],
        scratch_shapes=[pltpu.VMEM((top.nz, padded, top.part), F32)],
        cost_estimate=pl.CostEstimate(
            flops=MID_FLOPS, bytes_accessed=4 * noise_middle.size, transcendentals=0
        ),
        compiler_params=pltpu.CompilerParams(vmem_limit_bytes=24 * MIB),
        name="middle",
    )(gathered, fresh, noise_middle, mid_weights, in_hbm, in_hbm,
      fine_weights)
    above = shifted(lower, "slab", -1)
    beside = shifted(south, "pencil", -1)

    deep = 64
    nz, ny = planes, fine_y // deep
    each = deep // TILE

    def block(*where):
        def index(z, y):
            at = {"z": nz - 1 - z, "y": ny - 1 - y}
            return tuple(at.get(w, 0) for w in where)

        return index

    field, zface, yface = pl.pallas_call(
        fine_kernel,
        grid=(nz, ny),
        in_specs=[
            pl.BlockSpec((1, each, count * half, cols), block("z", "y", 0, 0)),
            pl.BlockSpec((count, 2, deep, fine_x), block(0, "z", "y", 0)),
            vmem,
        ],
        out_specs=[
            pl.BlockSpec((4, 2 * deep, out_x), block("z", "y", 0)),
            pl.BlockSpec((2, 2 * deep, out_x), block("z", "y", 0)),
            pl.BlockSpec((4, deep, out_x), block("z", "y", 0)),
        ],
        out_shape=[
            jax.ShapeDtypeStruct((2 * fine_planes, 2 * fine_y, out_x), F32),
            jax.ShapeDtypeStruct((fine_planes, 2 * fine_y, out_x), F32),
            jax.ShapeDtypeStruct((2 * fine_planes, fine_y, out_x), F32),
        ],
        scratch_shapes=[
            pltpu.VMEM((ny, each, 4 * TILE, fine_x), F32),
            pltpu.VMEM((2, 2 * TILE, fine_x), F32),
        ],
        cost_estimate=pl.CostEstimate(
            flops=2 * nz * (fine_y // TILE) * fine_weights.size * fine_x,
            bytes_accessed=4 * (noise_finest.size + 16 * fine_planes * fine_y * fine_x),
            transcendentals=0,
        ),
        compiler_params=pltpu.CompilerParams(vmem_limit_bytes=24 * MIB),
        name="fine",
    )(middle, noise_finest, fine_weights)
    z_spec = pl.BlockSpec((1, 2 * fine_y, out_x), lambda i: (fine_planes - 1, 0, 0))
    y_spec = pl.BlockSpec((2 * fine_planes, TILE, out_x), lambda i: (0, fine_y // TILE - 1, 0))
    zface, yface = pl.pallas_call(
        seam_kernel,
        grid=(1,),
        in_specs=[
            pl.BlockSpec(above.shape, lambda i: (0, 0, 0)),
            pl.BlockSpec(beside.shape, lambda i: (0, 0, 0)),
            z_spec,
            y_spec,
        ],
        out_specs=[z_spec, y_spec],
        out_shape=[
            jax.ShapeDtypeStruct(zface.shape, F32),
            jax.ShapeDtypeStruct(yface.shape, F32),
        ],
        input_output_aliases={2: 0, 3: 1},
        compiler_params=pltpu.CompilerParams(vmem_limit_bytes=8 * MIB),
        name="seam",
    )(above, beside, zface, yface)
    return field, zface, yface


def solution(mesh):
    placed = (
        P(),
        P(),
        P(),
        P(),
        P("slab", None, None),
        P(None, "slab", "pencil", None),
        P(None, "slab", "pencil", None),
    )
    return jax.shard_map(
        functools.partial(shards, mesh.shape["slab"], mesh.shape["pencil"]),
        mesh=mesh,
        in_specs=placed,
        out_specs=(P("slab", "pencil", None), P("slab", "pencil", None), P("slab", "pencil", None)),
        check_vma=False,
    )
```
